8 devices in a mesh: dp: 8 (over z, y, x, core).
Axes of the slice: x: 2, y: 2, z: 1, core: 2. Of those that a mesh axis runs over, the one named last changes fastest.
Arguments:
- query: bfloat16 [256, 24, 128], P('dp')
- k_cache: bfloat16 [256, 512, 8, 128], P('dp')
- v_cache: bfloat16 [256, 512, 8, 128], P('dp')
- cache_lens: int32 [256], P('dp')
- dest_slot: int32 [256], replicated
- k_new: bfloat16 [256, 8, 128], P('dp')
- v_new: bfloat16 [256, 8, 128], P('dp')
Outputs:
- output 1: bfloat16 [256, 24, 128], P('dp')
- output 2: bfloat16 [256, 512, 8, 128], P('dp')
- output 3: bfloat16 [256, 512, 8, 128], P('dp')
- output 4: int32 [256], P('dp')
All inputs are finite; a program needn't handle non-finite values.
Results may differ from the reference program's by a relative error of at most 0.001.
Values are sent between devices in bfloat16 or wider.
A program may use at most 1 GiB of HBM per device.

```python
import jax
import jax.numpy as jnp
from jax import lax

Q_HEADS = 24
KV_HEADS = 8
HEAD_DIM = 128
CACHE_LEN = 512
SLOTS_DEV = 32
GROUP_SIZE = 8
TOTAL_SLOTS = GROUP_SIZE * SLOTS_DEV


def draw_plan(key):
    key_heavy, key_len, key_coin, key_perm = jax.random.split(key, 4)
    heavy_dev = jax.random.randint(key_heavy, (GROUP_SIZE,), 0, 2, dtype=jnp.int32)
    heavy_dev = heavy_dev.at[0].set(1).at[GROUP_SIZE - 1].set(0)
    heavy_slot = jnp.repeat(heavy_dev, SLOTS_DEV)
    len_low = jnp.where(heavy_slot == 1, CACHE_LEN // 2, CACHE_LEN // 16).astype(jnp.int32)
    len_high = jnp.where(heavy_slot == 1, CACHE_LEN, CACHE_LEN // 2).astype(jnp.int32)
    cache_lens = jax.random.randint(key_len, (TOTAL_SLOTS,), len_low, len_high, dtype=jnp.int32)
    cache_lens = cache_lens.at[0].set(CACHE_LEN - 1).at[TOTAL_SLOTS - 1].set(CACHE_LEN // 16)
    move_coin = jax.random.randint(key_coin, (TOTAL_SLOTS,), 0, 4, dtype=jnp.int32)
    moving = (heavy_slot == 1) | (move_coin == 0)
    moving = moving.at[TOTAL_SLOTS - 1].set(True)
    rand_rank = jax.random.permutation(key_perm, TOTAL_SLOTS).astype(jnp.int32)
    sort_score = jnp.where(moving, 0, TOTAL_SLOTS).astype(jnp.int32) + rand_rank
    slot_order = jnp.argsort(sort_score).astype(jnp.int32)
    move_count = jnp.sum(moving.astype(jnp.int32))
    slot_ids = jnp.arange(TOTAL_SLOTS, dtype=jnp.int32)
    next_pos = jnp.where(slot_ids < move_count, (slot_ids + 1) % jnp.maximum(move_count, 1), slot_ids)
    dest_slot = jnp.zeros((TOTAL_SLOTS,), jnp.int32).at[slot_order].set(slot_order[next_pos])
    return cache_lens, dest_slot


def setup_inputs(seed: int = 0) -> dict:
    key = jax.random.key(seed)
    key_plan, key_query, key_kcache, key_vcache, key_knew, key_vnew = jax.random.split(key, 6)
    cache_lens, dest_slot = draw_plan(key_plan)
    query = jax.random.normal(key_query, (TOTAL_SLOTS, Q_HEADS, HEAD_DIM), jnp.float32).astype(jnp.bfloat16)
    k_cache = jax.random.normal(key_kcache, (TOTAL_SLOTS, CACHE_LEN, KV_HEADS, HEAD_DIM), jnp.float32).astype(jnp.bfloat16)
    v_cache = jax.random.normal(key_vcache, (TOTAL_SLOTS, CACHE_LEN, KV_HEADS, HEAD_DIM), jnp.float32).astype(jnp.bfloat16)
    k_new = jax.random.normal(key_knew, (TOTAL_SLOTS, KV_HEADS, HEAD_DIM), jnp.float32).astype(jnp.bfloat16)
    v_new = jax.random.normal(key_vnew, (TOTAL_SLOTS, KV_HEADS, HEAD_DIM), jnp.float32).astype(jnp.bfloat16)
    return {'query': query, 'k_cache': k_cache, 'v_cache': v_cache, 'cache_lens': cache_lens, 'dest_slot': dest_slot, 'k_new': k_new, 'v_new': v_new}


def attend_one(slot_data):
    query_row, k_row, v_row, length = slot_data
    groups = Q_HEADS // KV_HEADS
    q_grp = query_row.reshape(KV_HEADS, groups, HEAD_DIM).astype(jnp.float32)
    scores = jnp.einsum('kgd,tkd->kgt', q_grp, k_row.astype(jnp.float32)) * (HEAD_DIM ** -0.5)
    positions = jnp.arange(CACHE_LEN, dtype=jnp.int32)
    scores = jnp.where((positions <= length)[None, None, :], scores, -1e30)
    score_max = jnp.max(scores, axis=-1, keepdims=True)
    weights = jnp.exp(scores - score_max)
    prob_sum = jnp.sum(weights, axis=-1, keepdims=True)
    probs = weights.astype(jnp.bfloat16).astype(jnp.float32)
    attn_acc = jnp.einsum('kgt,tkd->kgd', probs, v_row.astype(jnp.float32)) / prob_sum
    return attn_acc.astype(jnp.bfloat16).reshape(Q_HEADS, HEAD_DIM)


def reference(query, k_cache, v_cache, cache_lens, dest_slot, k_new, v_new):
    slot_ids = jnp.arange(TOTAL_SLOTS, dtype=jnp.int32)
    source = jnp.zeros((TOTAL_SLOTS,), jnp.int32).at[dest_slot].set(slot_ids)
    lens_new = cache_lens[source]
    positions = jnp.arange(CACHE_LEN, dtype=jnp.int32)
    keep_row = (positions[None, :] < lens_new[:, None])[:, :, None, None]
    at_new = (positions[None, :] == lens_new[:, None])[:, :, None, None]
    zero_val = jnp.zeros((), jnp.bfloat16)
    k_out = jnp.where(keep_row, k_cache[source], jnp.where(at_new, k_new[:, None], zero_val))
    v_out = jnp.where(keep_row, v_cache[source], jnp.where(at_new, v_new[:, None], zero_val))
    attn_out = lax.map(attend_one, (query, k_out, v_out, lens_new))
    return attn_out, k_out, v_out, lens_new + 1
```

```python
import functools

import jax
import jax.numpy as jnp
from jax import lax
from jax.experimental import pallas as pl
from jax.experimental.pallas import tpu as pltpu
from jax.sharding import PartitionSpec as P


BP = 16
NB = 32
NX = 24
A = 4
SL = 32
BL = 32
IT = 136
S0, S1, R0, R1, XS, XR = range(6)
RDY, MLEN, SRC = 6 * 2 * IT, 6 * 2 * IT + 40, 6 * 2 * IT + 80
ROUNDS, CORE = 6 * 2 * IT + 120, 6 * 2 * IT + 121
TAB = 6 * 2 * IT + 128
U_PART, U_MERGE, U_OWN, U_POST, U_XS, U_XR = 0, 2, 4, 6, 8, 9
STEP, DONE, STATE = 24, 32, 64
END = 1 << 30
bf16 = jnp.bfloat16
f32 = jnp.float32
i32 = jnp.int32


def gray(c):
    return c ^ (c >> 1)


def plan_kernel(me_ref, dest_ref, len_ref, tab, lens_out, nbv, kindv, load, dload, xload):
    me = me_ref[0]
    core = me & 1
    mychip = me >> 1
    for i in range(9):
        load[i] = 0
        dload[i] = 0
        xload[i] = 0
    tab[CORE] = core

    def first(i, _):
        n = len_ref[i]
        d = dest_ref[i]
        nb = (n + (BP - 1)) >> 4
        ra = gray(i >> 6)
        delta = (gray(d >> 6) - ra) & 3
        nbv[i] = nb
        kindv[i] = delta
        slot = jnp.where(delta == 1, ra, jnp.where(delta == 3, 4 + ra, 8))
        load[slot] = load[slot] + nb
        cross = (delta == 0) & ((i >> 5) != (d >> 5))
        xslot = jnp.where(cross, i >> 5, 8)
        xload[xslot] = xload[xslot] + nb
        mine = jnp.where((d >> 5) == me, d & 31, 32)
        tab[MLEN + mine] = n
        tab[RDY + mine] = 0
        tab[SRC + mine] = jnp.where((i >> 5) == me, i & 31, -1)
        return 0
    lax.fori_loop(0, 8 * SL, first, 0)

    def lens(j, _):
        lens_out[j] = tab[MLEN + j] + 1
        return 0
    lax.fori_loop(0, SL, lens, 0)

    def choose(i, _):
        @pl.when(kindv[i] == 2)
        def _():
            nb = nbv[i]
            ra = gray(i >> 6)
            a1, a2, b1, b2 = ra, (ra + 1) & 3, 4 + ra, 4 + ((ra - 1) & 3)
            la, lb = jnp.maximum(load[a1], load[a2]), jnp.maximum(load[b1], load[b2])
            sa, sb = load[a1] + load[a2], load[b1] + load[b2]
            cw = (la < lb) | ((la == lb) & (sa <= sb))
            x1, x2 = jnp.where(cw, a1, b1), jnp.where(cw, a2, b2)
            load[x1] = load[x1] + nb
            load[x2] = load[x2] + nb
            dload[x1] = dload[x1] + nb
            kindv[i] = jnp.where(cw, 2, 4)
        return 0
    lax.fori_loop(0, 8 * SL, choose, 0)

    def own_and_total(d, x):
        up = (x - 1) & 3 if d == 0 else (x + 1) & 3
        fwd = dload[4 * d + up]
        own = load[4 * d + x] - fwd
        start = jnp.where(fwd > 0, jnp.maximum(own, 2 * NB), own)
        return start, start + fwd

    rounds = jnp.int32(0)
    for d in range(2):
        for x in range(4):
            _, total = own_and_total(d, jnp.int32(x))
            rounds = jnp.maximum(rounds, (total + NB - 1) // NB)
    for d in range(8):
        rounds = jnp.maximum(rounds, (xload[d] + NX - 1) // NX)
    tab[ROUNDS] = (rounds + 1) & -2

    def build(lid, d, x, recv):
        base = lid * 2 * IT
        up = (x - 1) & 3 if d == 0 else (x + 1) & 3
        first_kind, direct_kind = (2, 1) if d == 0 else (4, 3)

        def scan(ring, want, mode, c0):
            chip = gray(ring)

            def body(s, c):
                k, pos, fpos = c
                i = chip * 64 + s
                nb = nbv[i]
                hit = kindv[i] == want
                dst = dest_ref[i]
                if mode == 'src':
                    code = ((s >> 5) << 16) + (s & 31) * BL
                elif mode == 'fwd_in':
                    code = (2 << 16) + pos
                elif mode == 'fwd_out':
                    code = (2 << 16) + fpos
                else:
                    code = (((dst >> 5) & 1) << 16) + (dst & 31) * BL
                    mine = hit & ((dst >> 5) == me)
                    tab[RDY + jnp.where(mine, dst & 31, 33)] = (pos + nb - 1) // NB + 2
                tab[base + 2 * k] = nb
                tab[base + 2 * k + 1] = code
                inc = jnp.where(hit, nb, 0)
                return k + jnp.where(hit, 1, 0), pos + inc, fpos + inc
            return lax.fori_loop(0, 64, body, c0)

        k, pos, _ = scan(x, first_kind, 'fwd_in' if recv else 'src', (jnp.int32(0), jnp.int32(0), jnp.int32(0)))
        k, pos, _ = scan(x, direct_kind, 'dst' if recv else 'src', (k, pos, jnp.int32(0)))
        start, _ = own_and_total(d, x)
        tab[base + 2 * k] = start - pos
        tab[base + 2 * k + 1] = 3 << 16
        k = k + jnp.where(start > pos, 1, 0)
        k, pos, _ = scan(up, first_kind, 'dst' if recv else 'fwd_out', (k, start, jnp.int32(0)))
        tab[base + 2 * k] = END
        tab[base + 2 * k + 1] = 3 << 16

    x = gray(mychip)
    build(S0, 0, x, False)
    build(S1, 1, x, False)
    build(R0, 0, (x - 1) & 3, True)
    build(R1, 1, (x + 1) & 3, True)

    def cross_list(lid, sender, receiver, recv):
        base = lid * 2 * IT

        def body(s, c):
            k, pos = c
            i = sender * SL + s
            nb = nbv[i]
            dst = dest_ref[i]
            hit = (dst >> 5) == receiver
            tab[base + 2 * k] = nb
            if recv:
                tab[base + 2 * k + 1] = (dst & 31) * BL
                tab[RDY + jnp.where(hit, dst & 31, 33)] = (pos + nb - 1) // NX + 1
            else:
                tab[base + 2 * k + 1] = s * BL
            return k + jnp.where(hit, 1, 0), pos + jnp.where(hit, nb, 0)
        k, _ = lax.fori_loop(0, SL, body, (jnp.int32(0), jnp.int32(0)))
        tab[base + 2 * k] = END
        tab[base + 2 * k + 1] = 3 << 16

    cross_list(XS, me, me ^ 1, False)
    cross_list(XR, me ^ 1, me, True)


class Mover:
    def __init__(self, tab, st_in, st):
        self.tab, self.st = tab, st
        self.core = tab[CORE]

        def cp(i, _):
            st[i] = st_in[i]
            return 0
        lax.fori_loop(0, STATE, cp, 0)

    def walk(self, lid, use, n, fn):
        tab, st = self.tab, self.st
        base = lid * 2 * IT

        def body(p, c):
            item, off, cnt = c
            width = tab[base + 2 * item]
            code = tab[base + 2 * item + 1]
            cnt = cnt + fn(p, code >> 16, (code & 0xffff) + off)
            off = off + 1
            adv = off >= width
            return jnp.where(adv, item + 1, item), jnp.where(adv, 0, off), cnt
        item, off, cnt = lax.fori_loop(0, n, body, (st[2 * use], st[2 * use + 1], jnp.int32(0)))
        st[2 * use] = item
        st[2 * use + 1] = off
        return cnt

    @staticmethod
    def drain(cnt, ref, sem):
        def body(i, _):
            pltpu.make_async_copy(ref, ref, sem).wait()
            return 0
        lax.fori_loop(0, cnt, body, 0)

    def partial(self, d, kc, vc, buf, sem):
        core = self.core

        def fn(p, kind, idx):
            mine = kind == core

            @pl.when(mine & (core == 0))
            def _():
                pltpu.make_async_copy(vc.at[idx], buf.at[d, p], sem).start()

            @pl.when(mine & (core == 1))
            def _():
                pltpu.make_async_copy(kc.at[idx], buf.at[d, p], sem).start()
            return jnp.where(mine, 1, 0)
        return self.walk(S0 + d, U_PART + d, NB, fn)

    def merge(self, d, kc, vc, pre, fwd, buf, sem):
        core = self.core

        def fn(p, kind, idx):
            mine = kind == core

            @pl.when(mine & (core == 0))
            def _():
                pltpu.make_async_copy(kc.at[idx], buf.at[d, p], sem).start()

            @pl.when(mine & (core == 1))
            def _():
                pltpu.make_async_copy(vc.at[idx], buf.at[d, p], sem).start()

            @pl.when(kind == 1 - core)
            def _():
                pltpu.make_async_copy(pre.at[d, p], buf.at[d, p], sem).start()

            if fwd is not None:
                @pl.when(kind == 2)
                def _():
                    pltpu.make_async_copy(fwd.at[idx], buf.at[d, p], sem).start()
            return jnp.where(kind < 3, 1, 0)
        return self.walk(S0 + d, U_MERGE + d, NB, fn)

    def cross_send(self, kc, vc, buf, sem):
        def fn(p, kind, idx):
            @pl.when(kind == 0)
            def _():
                pltpu.make_async_copy(kc.at[idx], buf.at[0, p], sem).start()
                pltpu.make_async_copy(vc.at[idx], buf.at[1, p], sem).start()
            return jnp.where(kind == 0, 2, 0)
        return self.walk(XS, U_XS, NX, fn)

    def cross_recv(self, n, ko, vo, buf, sem):
        def fn(p, kind, idx):
            @pl.when(kind == 0)
            def _():
                pltpu.make_async_copy(buf.at[0, p], ko.at[idx], sem).start()
                pltpu.make_async_copy(buf.at[1, p], vo.at[idx], sem).start()
            return jnp.where(kind == 0, 2, 0)
        return self.walk(XR, U_XR, n, fn)

    def unpack(self, d, use, n, flip, ko, vo, fwd, buf, sem):
        core = self.core
        plane = 1 - core if flip else core

        def fn(p, kind, idx):
            mine = kind == core

            @pl.when(mine & (plane == 0))
            def _():
                pltpu.make_async_copy(buf.at[d, p], ko.at[idx], sem).start()

            @pl.when(mine & (plane == 1))
            def _():
                pltpu.make_async_copy(buf.at[d, p], vo.at[idx], sem).start()
            cnt = jnp.where(mine, 1, 0)
            if fwd is not None:
                @pl.when(kind == 2)
                def _():
                    pltpu.make_async_copy(buf.at[d, p], fwd.at[idx], sem).start()
                cnt = cnt + jnp.where(kind == 2, 1, 0)
            return cnt
        return self.walk(R0 + d, use + d, n, fn)


def open_kernel(tab, st_in, kc, vc, st, part0, part1, dxs, vpart, vdx, sem):
    mv = Mover(tab, st_in, st)
    blk = vpart.at[0, 0, 0]
    for c, out in enumerate((part0, part1)):
        for d in range(2):
            cnt = mv.partial(d, kc, vc, vpart.at[c], sem.at[c])
            mv.drain(cnt, blk, sem.at[c])
    cnt = mv.cross_send(kc, vc, vdx, sem.at[2])
    mv.drain(cnt, blk, sem.at[2])
    outs = [pltpu.make_async_copy(vpart.at[0], part0, sem.at[0]),
            pltpu.make_async_copy(vpart.at[1], part1, sem.at[1]),
            pltpu.make_async_copy(vdx, dxs, sem.at[2])]
    for c in outs:
        c.start()
    for c in outs:
        c.wait()


def open_merge_kernel(tab, st_in, kc, vc, pre, st, send0, send1, part, vsend, vpart, sem):
    mv = Mover(tab, st_in, st)
    blk = vpart.at[0, 0]
    c0 = mv.merge(0, kc, vc, pre, None, vsend, sem.at[0])
    c1 = mv.merge(1, kc, vc, pre, None, vsend, sem.at[1])
    c2 = mv.partial(0, kc, vc, vpart, sem.at[2]) + mv.partial(1, kc, vc, vpart, sem.at[2])
    mv.drain(c0, blk, sem.at[0])
    mv.drain(c1, blk, sem.at[1])
    mv.drain(c2, blk, sem.at[2])
    outs = [pltpu.make_async_copy(vsend.at[0], send0, sem.at[0]),
            pltpu.make_async_copy(vsend.at[1], send1, sem.at[1]),
            pltpu.make_async_copy(vpart, part, sem.at[2])]
    for c in outs:
        c.start()
    for c in outs:
        c.wait()


def round_kernel(tab, st_in, kc, vc, pre, rc0, rc1, po0, po1, dxr, f0i, f1i, koi, voi,
                 st, send0, send1, part, dxs, f0, f1, ko, vo,
                 vsend, vpart, vrecv, vpost, vdxs, vdxr, sem):
    mv = Mover(tab, st_in, st)
    blk = vpart.at[0, 0]
    r = st_in[STEP]
    st[STEP] = r + 1
    ins = [pltpu.make_async_copy(rc0, vrecv.at[0], sem.at[0]),
           pltpu.make_async_copy(rc1, vrecv.at[1], sem.at[1]),
           pltpu.make_async_copy(po0, vpost.at[0], sem.at[2]),
           pltpu.make_async_copy(po1, vpost.at[1], sem.at[3]),
           pltpu.make_async_copy(dxr, vdxr, sem.at[4])]
    for c in ins:
        c.start()
    n1 = jnp.where(r >= 1, NB, 0)
    n2 = jnp.where(r >= 2, NB, 0)
    nx = jnp.where(r >= 1, NX, 0)
    cp = mv.partial(0, kc, vc, vpart, sem.at[5]) + mv.partial(1, kc, vc, vpart, sem.at[5])
    cx = mv.cross_send(kc, vc, vdxs, sem.at[6])
    ins[0].wait()
    o0 = mv.unpack(0, U_OWN, n1, False, ko, vo, f0, vrecv, sem.at[7])
    ins[1].wait()
    o1 = mv.unpack(1, U_OWN, n1, False, ko, vo, f1, vrecv, sem.at[7])
    mv.drain(o0 + o1, blk, sem.at[7])
    c0 = mv.merge(0, kc, vc, pre, f0, vsend, sem.at[8])
    c1 = mv.merge(1, kc, vc, pre, f1, vsend, sem.at[9])
    ins[2].wait()
    ins[3].wait()
    o2 = mv.unpack(0, U_POST, n2, True, ko, vo, None, vpost, sem.at[7])
    o3 = mv.unpack(1, U_POST, n2, True, ko, vo, None, vpost, sem.at[7])
    ins[4].wait()
    o4 = mv.cross_recv(nx, ko, vo, vdxr, sem.at[7])
    mv.drain(cp, blk, sem.at[5])
    mv.drain(cx, blk, sem.at[6])
    mv.drain(c0, blk, sem.at[8])
    mv.drain(c1, blk, sem.at[9])
    outs = [pltpu.make_async_copy(vsend.at[0], send0, sem.at[0]),
            pltpu.make_async_copy(vsend.at[1], send1, sem.at[1]),
            pltpu.make_async_copy(vpart, part, sem.at[2]),
            pltpu.make_async_copy(vdxs, dxs, sem.at[3])]
    for c in outs:
        c.start()
    mv.drain(o2 + o3 + o4, blk, sem.at[7])
    for c in outs:
        c.wait()


def close_kernel(last, tab, st_in, *refs):
    if last:
        (po0, po1, koi, voi, st, ko, vo, vpost, sem) = refs
    else:
        (rc0, rc1, po0, po1, dxr, koi, voi, st, ko, vo, vpost, vrecv, vdxr, sem) = refs
    mv = Mover(tab, st_in, st)
    blk = vpost.at[0, 0]
    r = st_in[STEP]
    st[STEP] = r + 1
    ins = [pltpu.make_async_copy(po0, vpost.at[0], sem.at[0]),
           pltpu.make_async_copy(po1, vpost.at[1], sem.at[1])]
    if not last:
        ins += [pltpu.make_async_copy(rc0, vrecv.at[0], sem.at[2]),
                pltpu.make_async_copy(rc1, vrecv.at[1], sem.at[3]),
                pltpu.make_async_copy(dxr, vdxr, sem.at[4])]
    for c in ins:
        c.start()
    n1 = jnp.where(r >= 1, NB, 0)
    n2 = jnp.where(r >= 2, NB, 0)
    nx = jnp.where(r >= 1, NX, 0)
    for c in ins:
        c.wait()
    cnt = mv.unpack(0, U_POST, n2, True, ko, vo, None, vpost, sem.at[5])
    cnt += mv.unpack(1, U_POST, n2, True, ko, vo, None, vpost, sem.at[5])
    if not last:
        cnt += mv.unpack(0, U_OWN, n1, False, ko, vo, None, vrecv, sem.at[5])
        cnt += mv.unpack(1, U_OWN, n1, False, ko, vo, None, vrecv, sem.at[5])
        cnt += mv.cross_recv(nx, ko, vo, vdxr, sem.at[5])
    mv.drain(cnt, blk, sem.at[5])


def attn_kernel(batches, tab, st_in, q, kn, vn, kc, vc, koi, voi, aoi, st, ko, vo, ao,
                kb, vb, ob, sel, lsem, wsem, osem):
    def cp(i, _):
        st[i] = st_in[i]
        return 0
    lax.fori_loop(0, STATE, cp, 0)
    r = st_in[STEP]
    blk = kb.at[0, 0]

    def load(a, j):
        s = tab[SRC + j]

        @pl.when(s >= 0)
        def _():
            pltpu.make_async_copy(kc.at[pl.ds(s * BL, BL)], kb.at[a], lsem.at[a]).start()
            pltpu.make_async_copy(vc.at[pl.ds(s * BL, BL)], vb.at[a], lsem.at[a]).start()

        @pl.when(s < 0)
        def _():
            pltpu.make_async_copy(ko.at[pl.ds(j * BL, BL)], kb.at[a], lsem.at[a]).start()
            pltpu.make_async_copy(vo.at[pl.ds(j * BL, BL)], vb.at[a], lsem.at[a]).start()

    def compute(a, j):
        pltpu.make_async_copy(kb.at[a], kb.at[a], lsem.at[a]).wait()
        pltpu.make_async_copy(vb.at[a], vb.at[a], lsem.at[a]).wait()
        m = tab[MLEN + j]
        s = tab[SRC + j]
        b0 = m >> 4
        row = lax.broadcasted_iota(i32, (128, 128), 0) >> 3
        for buf, new in ((kb, kn), (vb, vn)):
            x = buf[a, b0].astype(f32)
            fresh = jnp.concatenate([new[j].astype(f32)] * BP, axis=0)
            t = b0 * BP + row
            buf[a, b0] = jnp.where(t < m, x, jnp.where(t == m, fresh, 0.0)).astype(bf16)

        def wipe(b, _):
            kb[a, b] = jnp.zeros((128, 128), bf16)
            vb[a, b] = jnp.zeros((128, 128), bf16)
            return 0
        lax.fori_loop(b0 + 1, BL, wipe, 0)
        kf = kb[a].reshape(BL * 128, 128)
        vf = vb[a].reshape(BL * 128, 128)
        sc = lax.dot_general(q[j], kf, (((1,), (1,)), ((), ())), preferred_element_type=f32) * (128 ** -0.5)
        col = lax.broadcasted_iota(i32, sc.shape, 1)
        head = lax.broadcasted_iota(i32, sc.shape, 0) // 3
        ok = ((col & 7) == head) & ((col >> 3) <= m)
        sc = jnp.where(ok, sc, -1e30)
        top = jnp.max(sc, axis=1, keepdims=True)
        w = jnp.exp(sc - top)
        tot = jnp.sum(w, axis=1, keepdims=True)
        acc = lax.dot_general(w.astype(bf16), vf, (((1,), (0,)), ((), ())), preferred_element_type=f32)
        ob[a] = (acc / tot).astype(bf16)
        bw = jnp.where(s >= 0, 0, b0)

        def back(b, _):
            pltpu.make_async_copy(kb.at[a, b], ko.at[j * BL + b], wsem.at[0]).start()
            pltpu.make_async_copy(vb.at[a, b], vo.at[j * BL + b], wsem.at[0]).start()
            return 0
        lax.fori_loop(bw, BL, back, 0)
        pltpu.make_async_copy(ob.at[a], ao.at[j], osem.at[0]).start()
        return 2 * (BL - bw)

    def batch(_, c):
        def pick(j, n):
            hit = (st[DONE + j] == 0) & (tab[RDY + j] < r) & (n < A)
            sel[jnp.where(hit, n, A)] = j
            st[DONE + j] = jnp.where(hit, 1, st[DONE + j])
            return n + jnp.where(hit, 1, 0)
        n = lax.fori_loop(0, SL, pick, jnp.int32(0))

        def loads(a, _):
            load(a, sel[a])
            return 0
        lax.fori_loop(0, n, loads, 0)

        def computes(a, cnt):
            return cnt + compute(a, sel[a])
        cnt = lax.fori_loop(0, n, computes, jnp.int32(0))

        def w1(i, _):
            pltpu.make_async_copy(blk, blk, wsem.at[0]).wait()
            return 0
        lax.fori_loop(0, cnt, w1, 0)

        def w2(i, _):
            pltpu.make_async_copy(ob.at[0], ob.at[0], osem.at[0]).wait()
            return 0
        lax.fori_loop(0, n, w2, 0)
        return c
    lax.fori_loop(0, batches, batch, 0)


SMEM = pl.BlockSpec(memory_space=pltpu.SMEM)
VMEM = pl.BlockSpec(memory_space=pltpu.VMEM)
ANY = pl.BlockSpec(memory_space=pl.ANY)
BLOCK = (128, 128)


def sds(shape, dtype=bf16):
    return jax.ShapeDtypeStruct(shape, dtype)


def dma(n):
    return pltpu.SemaphoreType.DMA((n,))


def buf(*lead):
    return pltpu.VMEM(lead + BLOCK, bf16)


def cost(us):
    return pl.CostEstimate(flops=int(us * 4e6), bytes_accessed=int(us * 2e6), transcendentals=0)


ST = sds((STATE,), i32)


def solution(mesh):
    group = mesh.shape['dp']
    ring = [0, 1, 3, 2]
    cw = [(ring[k] * 2 + c, ring[(k + 1) % 4] * 2 + c) for k in range(4) for c in range(2)]
    ccw = [(b, a) for a, b in cw]
    swap = [(d, d ^ 1) for d in range(group)]

    def local(query, k_cache, v_cache, cache_lens, dest_slot, k_new, v_new):
        kc = k_cache.reshape((SL * BL,) + BLOCK)
        vc = v_cache.reshape((SL * BL,) + BLOCK)
        lens_all = lax.all_gather(cache_lens, 'dp', tiled=True)
        me = jnp.full((1,), lax.axis_index('dp'), i32)
        tab, lens_out = pl.pallas_call(
            plan_kernel, out_shape=(sds((TAB,), i32), sds((SL,), i32)), in_specs=[SMEM] * 3, out_specs=(SMEM, SMEM),
            scratch_shapes=[pltpu.SMEM((256,), i32), pltpu.SMEM((256,), i32)] + [pltpu.SMEM((16,), i32)] * 3,
            name='plan')(me, dest_slot, lens_all)

        def nothing(*refs):
            pass
        chunk, both, cross = sds((NB,) + BLOCK), sds((2, NB) + BLOCK), sds((2, NX) + BLOCK)
        cache, store = sds((SL * BL,) + BLOCK), sds((2 * SL * BL,) + BLOCK)
        ko, vo, ao, f0, f1, rc0, rc1, po0, po1, dxr = pl.pallas_call(
            nothing, out_shape=(cache, cache, sds((SL, 24, 128)), store, store, chunk, chunk, chunk, chunk, cross),
            out_specs=(ANY,) * 10, name='blank')()

        st = jnp.zeros((STATE,), i32)
        st, part0, part1, dxs = pl.pallas_call(
            open_kernel, out_shape=(ST, both, both, cross), in_specs=[SMEM, SMEM, ANY, ANY], out_specs=(SMEM, ANY, ANY, ANY),
            scratch_shapes=[buf(2, 2, NB), buf(2, NX), dma(3)], name='open')(tab, st, kc, vc)
        pre0 = lax.ppermute(part0, 'dp', swap)
        pre = lax.ppermute(part1, 'dp', swap)
        st, s0, s1, part = pl.pallas_call(
            open_merge_kernel, out_shape=(ST, chunk, chunk, both), in_specs=[SMEM, SMEM, ANY, ANY, ANY],
            out_specs=(SMEM, ANY, ANY, ANY), scratch_shapes=[buf(2, NB), buf(2, NB), dma(3)],
            name='open_merge')(tab, st, kc, vc, pre0)

        def attend(st, ko, vo, ao, batches):
            return pl.pallas_call(
                functools.partial(attn_kernel, batches),
                out_shape=(ST, cache, cache, sds((SL, 24, 128))),
                in_specs=[SMEM, SMEM, VMEM, VMEM, VMEM, ANY, ANY, ANY, ANY, ANY], out_specs=(SMEM, ANY, ANY, ANY),
                input_output_aliases={7: 1, 8: 2, 9: 3},
                scratch_shapes=[buf(A, BL), buf(A, BL), pltpu.VMEM((A, 24, 128), bf16), pltpu.SMEM((A + 1,), i32),
                                dma(A), dma(1), dma(1)],
                cost_estimate=cost(6), name='attend')(tab, st, query, k_new, v_new, kc, vc, ko, vo, ao)

        def one_round(c):
            st, s0, s1, part, dxs, pre, rc0, rc1, po0, po1, dxr, f0, f1, ko, vo, ao = c
            nrc0 = lax.ppermute(s0, 'dp', cw)
            nrc1 = lax.ppermute(s1, 'dp', ccw)
            npre = lax.ppermute(part, 'dp', swap)
            npo0 = lax.ppermute(rc0, 'dp', swap)
            npo1 = lax.ppermute(rc1, 'dp', swap)
            ndxr = lax.ppermute(dxs, 'dp', swap)
            st, s0, s1, part, dxs, f0, f1, ko, vo = pl.pallas_call(
                round_kernel, out_shape=(ST, chunk, chunk, both, cross, store, store, cache, cache),
                in_specs=[SMEM, SMEM] + [ANY] * 12, out_specs=(SMEM,) + (ANY,) * 8,
                input_output_aliases={10: 5, 11: 6, 12: 7, 13: 8},
                scratch_shapes=[buf(2, NB)] * 4 + [buf(2, NX)] * 2 + [dma(10)],
                cost_estimate=cost(10), name='round')(tab, st, kc, vc, pre, rc0, rc1, po0, po1, dxr, f0, f1, ko, vo)
            st, ko, vo, ao = attend(st, ko, vo, ao, 1)
            return st, s0, s1, part, dxs, npre, nrc0, nrc1, npo0, npo1, ndxr, f0, f1, ko, vo, ao

        rounds = tab[ROUNDS]

        def body(c):
            return (c[0] + 2,) + one_round(one_round(c[1:]))
        c = lax.while_loop(lambda c: c[0] < rounds, body,
                           (jnp.int32(0), st, s0, s1, part, dxs, pre, rc0, rc1, po0, po1, dxr, f0, f1, ko, vo, ao))
        _, st, _, _, _, _, _, rc0, rc1, po0, po1, dxr, _, _, ko, vo, ao = c

        def close(last, st, ko, vo, *ins):
            n = len(ins)
            extra = [] if last else [buf(2, NB), buf(2, NX)]
            return pl.pallas_call(
                functools.partial(close_kernel, last), out_shape=(ST, cache, cache),
                in_specs=[SMEM, SMEM] + [ANY] * (n + 2), out_specs=(SMEM, ANY, ANY),
                input_output_aliases={n + 2: 1, n + 3: 2},
                scratch_shapes=[buf(2, NB)] + extra + [dma(6)],
                name='close_last' if last else 'close')(tab, st, *ins, ko, vo)
        lpo0 = lax.ppermute(rc0, 'dp', swap)
        lpo1 = lax.ppermute(rc1, 'dp', swap)
        st, ko, vo = close(False, st, ko, vo, rc0, rc1, po0, po1, dxr)
        st, ko, vo = close(True, st, ko, vo, lpo0, lpo1)
        st, ko, vo, ao = attend(st, ko, vo, ao, SL // A)
        return ao, ko.reshape(k_cache.shape), vo.reshape(v_cache.shape), lens_out

    row_spec = P('dp')
    return jax.shard_map(local, mesh=mesh, in_specs=(row_spec, row_spec, row_spec, row_spec, P(), row_spec, row_spec),
                         out_specs=(row_spec, row_spec, row_spec, row_spec), check_vma=False)
```

```python
import functools

import jax
import jax.numpy as jnp
from jax import lax
from jax.experimental import pallas as pl
from jax.experimental.pallas import tpu as pltpu
from jax.sharding import PartitionSpec as P


BP = 16
NB = 32
NX = 24
A = 4
SL = 32
BL = 32
IT = 136
S0, S1, R0, R1, XS, XR = range(6)
RDY, MLEN, SRC = 6 * 2 * IT, 6 * 2 * IT + 40, 6 * 2 * IT + 80
ROUNDS, CORE = 6 * 2 * IT + 120, 6 * 2 * IT + 121
TAB = 6 * 2 * IT + 128
U_PART, U_MERGE, U_OWN, U_POST, U_XS, U_XR = 0, 2, 4, 6, 8, 9
STEP, DONE, STATE = 24, 32, 64
END = 1 << 30
bf16 = jnp.bfloat16
f32 = jnp.float32
i32 = jnp.int32


def gray(c):
    return c ^ (c >> 1)


def lens_kernel(x, o, bsem, ssem, rsem):
    me = lax.axis_index('dp')
    barrier = pltpu.get_barrier_semaphore()
    for k in range(1, 8):
        pl.semaphore_signal(barrier, inc=1, device_id=(lax.rem(me + k, 8),), device_id_type=pl.DeviceIdType.MESH)
    pl.semaphore_wait(barrier, 7)
    here = pltpu.make_async_copy(x, o.at[me], bsem)
    here.start()
    sends = []
    for k in range(1, 8):
        c = pltpu.make_async_remote_copy(src_ref=x, dst_ref=o.at[me], send_sem=ssem.at[k], recv_sem=rsem.at[k],
                                         device_id=(lax.rem(me + k, 8),), device_id_type=pl.DeviceIdType.MESH)
        c.start()
        sends.append(c)
    here.wait()
    for c in sends:
        c.wait()


def plan_kernel(me_ref, dest_ref, len_ref, tab, lens_out, nbv, kindv, load, dload, xload):
    me = me_ref[0]
    core = me & 1
    mychip = me >> 1
    for i in range(9):
        load[i] = 0
        dload[i] = 0
        xload[i] = 0
    tab[CORE] = core

    def first(i, _):
        n = len_ref[i >> 5, 0, i & 31]
        d = dest_ref[i]
        nb = (n + (BP - 1)) >> 4
        ra = gray(i >> 6)
        delta = (gray(d >> 6) - ra) & 3
        nbv[i] = nb
        kindv[i] = delta
        slot = jnp.where(delta == 1, ra, jnp.where(delta == 3, 4 + ra, 8))
        load[slot] = load[slot] + nb
        cross = (delta == 0) & ((i >> 5) != (d >> 5))
        xslot = jnp.where(cross, i >> 5, 8)
        xload[xslot] = xload[xslot] + nb
        mine = jnp.where((d >> 5) == me, d & 31, 32)
        tab[MLEN + mine] = n
        tab[RDY + mine] = 0
        tab[SRC + mine] = jnp.where((i >> 5) == me, i & 31, -1)
        return 0

    lax.fori_loop(0, 8 * SL, first, 0)

    def lens(j, _):
        lens_out[j] = tab[MLEN + j] + 1
        return 0

    lax.fori_loop(0, SL, lens, 0)

    def choose(i, _):
        @pl.when(kindv[i] == 2)
        def _():
            nb = nbv[i]
            ra = gray(i >> 6)
            a1, a2, b1, b2 = ra, (ra + 1) & 3, 4 + ra, 4 + ((ra - 1) & 3)
            la, lb = jnp.maximum(load[a1], load[a2]), jnp.maximum(load[b1], load[b2])
            sa, sb = load[a1] + load[a2], load[b1] + load[b2]
            cw = (la < lb) | ((la == lb) & (sa <= sb))
            x1, x2 = jnp.where(cw, a1, b1), jnp.where(cw, a2, b2)
            load[x1] = load[x1] + nb
            load[x2] = load[x2] + nb
            dload[x1] = dload[x1] + nb
            kindv[i] = jnp.where(cw, 2, 4)

        return 0

    lax.fori_loop(0, 8 * SL, choose, 0)

    def own_and_total(d, x):
        up = (x - 1) & 3 if d == 0 else (x + 1) & 3
        fwd = dload[4 * d + up]
        own = load[4 * d + x] - fwd
        start = jnp.where(fwd > 0, jnp.maximum(own, 2 * NB), own)
        return start, start + fwd

    rounds = jnp.int32(0)
    for d in range(2):
        for x in range(4):
            _, total = own_and_total(d, jnp.int32(x))
            rounds = jnp.maximum(rounds, (total + NB - 1) // NB)
    for d in range(8):
        rounds = jnp.maximum(rounds, (xload[d] + NX - 1) // NX)
    tab[ROUNDS] = (rounds + 1) & -2

    def build(lid, d, x, recv):
        base = lid * 2 * IT
        up = (x - 1) & 3 if d == 0 else (x + 1) & 3
        first_kind, direct_kind = (2, 1) if d == 0 else (4, 3)

        def scan(ring, want, mode, c0):
            chip = gray(ring)

            def body(s, c):
                k, pos, fpos = c
                i = chip * 64 + s
                nb = nbv[i]
                hit = kindv[i] == want
                dst = dest_ref[i]
                if mode == 'src':
                    code = ((s >> 5) << 16) + (s & 31) * BL
                elif mode == 'fwd_in':
                    code = (2 << 16) + pos
                elif mode == 'fwd_out':
                    code = (2 << 16) + fpos
                else:
                    code = (((dst >> 5) & 1) << 16) + (dst & 31) * BL
                    mine = hit & ((dst >> 5) == me)
                    tab[RDY + jnp.where(mine, dst & 31, 33)] = (pos + nb - 1) // NB + 2
                tab[base + 2 * k] = nb
                tab[base + 2 * k + 1] = code
                inc = jnp.where(hit, nb, 0)
                return k + jnp.where(hit, 1, 0), pos + inc, fpos + inc

            return lax.fori_loop(0, 64, body, c0)

        k, pos, _ = scan(x, first_kind, 'fwd_in' if recv else 'src', (jnp.int32(0), jnp.int32(0), jnp.int32(0)))
        k, pos, _ = scan(x, direct_kind, 'dst' if recv else 'src', (k, pos, jnp.int32(0)))
        start, _ = own_and_total(d, x)
        tab[base + 2 * k] = start - pos
        tab[base + 2 * k + 1] = 3 << 16
        k = k + jnp.where(start > pos, 1, 0)
        k, pos, _ = scan(up, first_kind, 'dst' if recv else 'fwd_out', (k, start, jnp.int32(0)))
        tab[base + 2 * k] = END
        tab[base + 2 * k + 1] = 3 << 16

    x = gray(mychip)
    build(S0, 0, x, False)
    build(S1, 1, x, False)
    build(R0, 0, (x - 1) & 3, True)
    build(R1, 1, (x + 1) & 3, True)

    def cross_list(lid, sender, receiver, recv):
        base = lid * 2 * IT

        def body(s, c):
            k, pos = c
            i = sender * SL + s
            nb = nbv[i]
            dst = dest_ref[i]
            hit = (dst >> 5) == receiver
            tab[base + 2 * k] = nb
            if recv:
                tab[base + 2 * k + 1] = (dst & 31) * BL
                tab[RDY + jnp.where(hit, dst & 31, 33)] = (pos + nb - 1) // NX + 1
            else:
                tab[base + 2 * k + 1] = s * BL
            return k + jnp.where(hit, 1, 0), pos + jnp.where(hit, nb, 0)

        k, _ = lax.fori_loop(0, SL, body, (jnp.int32(0), jnp.int32(0)))
        tab[base + 2 * k] = END
        tab[base + 2 * k + 1] = 3 << 16

    cross_list(XS, me, me ^ 1, False)
    cross_list(XR, me ^ 1, me, True)


class Mover:
    def __init__(self, tab, st_in, st):
        self.tab, self.st = tab, st
        self.core = tab[CORE]

        def cp(i, _):
            st[i] = st_in[i]
            return 0

        lax.fori_loop(0, STATE, cp, 0)

    def walk(self, lid, use, n, fn):
        tab, st = self.tab, self.st
        base = lid * 2 * IT

        def body(c):
            p, item, off, cnt = c
            width = tab[base + 2 * item]
            code = tab[base + 2 * item + 1]
            take = jnp.minimum(n - p, width - off)
            cnt = cnt + fn(p, take, code >> 16, (code & 0xffff) + off)
            off = off + take
            adv = off >= width
            return p + take, jnp.where(adv, item + 1, item), jnp.where(adv, 0, off), cnt

        c0 = (jnp.int32(0), st[2 * use], st[2 * use + 1], jnp.int32(0))
        _, item, off, cnt = lax.while_loop(lambda c: c[0] < n, body, c0)
        st[2 * use] = item
        st[2 * use + 1] = off
        return cnt

    @staticmethod
    def drain(cnt, ref, sem):
        @pl.when(cnt > 0)
        def _():
            part = ref.at[pl.ds(0, cnt)]
            pltpu.make_async_copy(part, part, sem).wait()

    def partial(self, d, kc, vc, buf, sem):
        core = self.core

        def fn(p, take, kind, idx):
            mine = kind == core

            @pl.when(mine & (core == 0))
            def _():
                pltpu.make_async_copy(vc.at[pl.ds(idx, take)], buf.at[d, pl.ds(p, take)], sem).start()

            @pl.when(mine & (core == 1))
            def _():
                pltpu.make_async_copy(kc.at[pl.ds(idx, take)], buf.at[d, pl.ds(p, take)], sem).start()

            return jnp.where(mine, take, 0)

        return self.walk(S0 + d, U_PART + d, NB, fn)

    def merge(self, d, kc, vc, pre, fwd, buf, sem):
        core = self.core

        def fn(p, take, kind, idx):
            mine = kind == core

            @pl.when(mine & (core == 0))
            def _():
                pltpu.make_async_copy(kc.at[pl.ds(idx, take)], buf.at[d, pl.ds(p, take)], sem).start()

            @pl.when(mine & (core == 1))
            def _():
                pltpu.make_async_copy(vc.at[pl.ds(idx, take)], buf.at[d, pl.ds(p, take)], sem).start()

            @pl.when(kind == 1 - core)
            def _():
                pltpu.make_async_copy(pre.at[d, pl.ds(p, take)], buf.at[d, pl.ds(p, take)], sem).start()

            if fwd is not None:
                @pl.when(kind == 2)
                def _():
                    pltpu.make_async_copy(fwd.at[pl.ds(idx, take)], buf.at[d, pl.ds(p, take)], sem).start()
            return jnp.where(kind < 3, take, 0)

        return self.walk(S0 + d, U_MERGE + d, NB, fn)

    def cross_send(self, kc, vc, buf, sem):
        def fn(p, take, kind, idx):
            @pl.when(kind == 0)
            def _():
                pltpu.make_async_copy(kc.at[pl.ds(idx, take)], buf.at[0, pl.ds(p, take)], sem).start()
                pltpu.make_async_copy(vc.at[pl.ds(idx, take)], buf.at[1, pl.ds(p, take)], sem).start()

            return jnp.where(kind == 0, 2 * take, 0)

        return self.walk(XS, U_XS, NX, fn)

    def cross_recv(self, n, ko, vo, buf, sem):
        def fn(p, take, kind, idx):
            @pl.when(kind == 0)
            def _():
                pltpu.make_async_copy(buf.at[0, pl.ds(p, take)], ko.at[pl.ds(idx, take)], sem).start()
                pltpu.make_async_copy(buf.at[1, pl.ds(p, take)], vo.at[pl.ds(idx, take)], sem).start()

            return jnp.where(kind == 0, 2 * take, 0)

        return self.walk(XR, U_XR, n, fn)

    def unpack(self, d, use, n, flip, ko, vo, fwd, buf, sem):
        core = self.core
        plane = 1 - core if flip else core

        def fn(p, take, kind, idx):
            mine = kind == core

            @pl.when(mine & (plane == 0))
            def _():
                pltpu.make_async_copy(buf.at[d, pl.ds(p, take)], ko.at[pl.ds(idx, take)], sem).start()

            @pl.when(mine & (plane == 1))
            def _():
                pltpu.make_async_copy(buf.at[d, pl.ds(p, take)], vo.at[pl.ds(idx, take)], sem).start()

            cnt = jnp.where(mine, take, 0)
            if fwd is not None:
                @pl.when(kind == 2)
                def _():
                    pltpu.make_async_copy(buf.at[d, pl.ds(p, take)], fwd.at[pl.ds(idx, take)], sem).start()

                cnt = cnt + jnp.where(kind == 2, take, 0)
            return cnt

        return self.walk(R0 + d, use + d, n, fn)


def open_kernel(tab, st_in, kc, vc, st, part0, part1, dxs, vpart, vdx, sem):
    mv = Mover(tab, st_in, st)
    outs = [pltpu.make_async_copy(vpart.at[0], part0, sem.at[0]),
            pltpu.make_async_copy(vpart.at[1], part1, sem.at[1]),
            pltpu.make_async_copy(vdx, dxs, sem.at[2])]
    cnt = [mv.partial(0, kc, vc, vpart.at[c], sem.at[c]) + mv.partial(1, kc, vc, vpart.at[c], sem.at[c]) for c in range(2)]
    cnt.append(mv.cross_send(kc, vc, vdx, sem.at[2]))
    for c in range(3):
        mv.drain(cnt[c], kc, sem.at[c])
        outs[c].start()
    for c in outs:
        c.wait()


def open_merge_kernel(tab, st_in, kc, vc, pre, st, send0, send1, part, vsend, vpart, sem):
    mv = Mover(tab, st_in, st)
    c0 = mv.merge(0, kc, vc, pre, None, vsend, sem.at[0])
    c1 = mv.merge(1, kc, vc, pre, None, vsend, sem.at[1])
    c2 = mv.partial(0, kc, vc, vpart, sem.at[2]) + mv.partial(1, kc, vc, vpart, sem.at[2])
    mv.drain(c0, kc, sem.at[0])
    mv.drain(c1, kc, sem.at[1])
    mv.drain(c2, kc, sem.at[2])
    outs = [pltpu.make_async_copy(vsend.at[0], send0, sem.at[0]),
            pltpu.make_async_copy(vsend.at[1], send1, sem.at[1]),
            pltpu.make_async_copy(vpart, part, sem.at[2])]
    for c in outs:
        c.start()
    for c in outs:
        c.wait()


def round_kernel(tab, st_in, kc, vc, pre, rc0, rc1, po0, po1, dxr, f0i, f1i, koi, voi,
                 st, send0, send1, part, dxs, f0, f1, ko, vo,
                 vsend, vpart, vrecv, vpost, vdxs, vdxr, sem):
    mv = Mover(tab, st_in, st)
    r = st_in[STEP]
    st[STEP] = r + 1
    ins = [pltpu.make_async_copy(rc0, vrecv.at[0], sem.at[0]),
           pltpu.make_async_copy(rc1, vrecv.at[1], sem.at[1]),
           pltpu.make_async_copy(po0, vpost.at[0], sem.at[2]),
           pltpu.make_async_copy(po1, vpost.at[1], sem.at[3]),
           pltpu.make_async_copy(dxr, vdxr, sem.at[4])]
    for c in ins:
        c.start()
    n1 = jnp.where(r >= 1, NB, 0)
    n2 = jnp.where(r >= 2, NB, 0)
    nx = jnp.where(r >= 1, NX, 0)
    cp = mv.partial(0, kc, vc, vpart, sem.at[5]) + mv.partial(1, kc, vc, vpart, sem.at[5])
    cx = mv.cross_send(kc, vc, vdxs, sem.at[6])
    ins[0].wait()
    o0 = mv.unpack(0, U_OWN, n1, False, ko, vo, f0, vrecv, sem.at[7])
    ins[1].wait()
    o1 = mv.unpack(1, U_OWN, n1, False, ko, vo, f1, vrecv, sem.at[7])
    mv.drain(o0 + o1, kc, sem.at[7])
    c0 = mv.merge(0, kc, vc, pre, f0, vsend, sem.at[8])
    c1 = mv.merge(1, kc, vc, pre, f1, vsend, sem.at[9])
    ins[2].wait()
    ins[3].wait()
    o2 = mv.unpack(0, U_POST, n2, True, ko, vo, None, vpost, sem.at[7])
    o3 = mv.unpack(1, U_POST, n2, True, ko, vo, None, vpost, sem.at[7])
    ins[4].wait()
    o4 = mv.cross_recv(nx, ko, vo, vdxr, sem.at[7])
    mv.drain(cp, kc, sem.at[5])
    mv.drain(cx, kc, sem.at[6])
    mv.drain(c0, kc, sem.at[8])
    mv.drain(c1, kc, sem.at[9])
    outs = [pltpu.make_async_copy(vsend.at[0], send0, sem.at[0]),
            pltpu.make_async_copy(vsend.at[1], send1, sem.at[1]),
            pltpu.make_async_copy(vpart, part, sem.at[2]),
            pltpu.make_async_copy(vdxs, dxs, sem.at[3])]
    for c in outs:
        c.start()
    mv.drain(o2 + o3 + o4, kc, sem.at[7])
    for c in outs:
        c.wait()


def close_kernel(last, tab, st_in, *refs):
    if last:
        (po0, po1, koi, voi, st, ko, vo, vpost, sem) = refs
    else:
        (rc0, rc1, po0, po1, dxr, koi, voi, st, ko, vo, vpost, vrecv, vdxr, sem) = refs
    mv = Mover(tab, st_in, st)
    r = st_in[STEP]
    st[STEP] = r + 1
    ins = [pltpu.make_async_copy(po0, vpost.at[0], sem.at[0]),
           pltpu.make_async_copy(po1, vpost.at[1], sem.at[1])]
    if not last:
        ins += [pltpu.make_async_copy(rc0, vrecv.at[0], sem.at[2]),
                pltpu.make_async_copy(rc1, vrecv.at[1], sem.at[3]),
                pltpu.make_async_copy(dxr, vdxr, sem.at[4])]
    for c in ins:
        c.start()
    n1 = jnp.where(r >= 1, NB, 0)
    n2 = jnp.where(r >= 2, NB, 0)
    nx = jnp.where(r >= 1, NX, 0)
    for c in ins:
        c.wait()
    cnt = mv.unpack(0, U_POST, n2, True, ko, vo, None, vpost, sem.at[5])
    cnt += mv.unpack(1, U_POST, n2, True, ko, vo, None, vpost, sem.at[5])
    if not last:
        cnt += mv.unpack(0, U_OWN, n1, False, ko, vo, None, vrecv, sem.at[5])
        cnt += mv.unpack(1, U_OWN, n1, False, ko, vo, None, vrecv, sem.at[5])
        cnt += mv.cross_recv(nx, ko, vo, vdxr, sem.at[5])
    mv.drain(cnt, ko, sem.at[5])


def attn_kernel(batches, tab, st_in, q, kn, vn, kc, vc, koi, voi, aoi, st, ko, vo, ao,
                kb, vb, ob, sel, lsem, wsem, osem):
    def cp(i, _):
        st[i] = st_in[i]
        return 0

    lax.fori_loop(0, STATE, cp, 0)
    r = st_in[STEP]

    def load(a, j):
        s = tab[SRC + j]

        @pl.when(s >= 0)
        def _():
            pltpu.make_async_copy(kc.at[pl.ds(s * BL, BL)], kb.at[a], lsem.at[a]).start()
            pltpu.make_async_copy(vc.at[pl.ds(s * BL, BL)], vb.at[a], lsem.at[a]).start()

        @pl.when(s < 0)
        def _():
            pltpu.make_async_copy(ko.at[pl.ds(j * BL, BL)], kb.at[a], lsem.at[a]).start()
            pltpu.make_async_copy(vo.at[pl.ds(j * BL, BL)], vb.at[a], lsem.at[a]).start()

    def compute(a, j):
        pltpu.make_async_copy(kb.at[a], kb.at[a], lsem.at[a]).wait()
        pltpu.make_async_copy(vb.at[a], vb.at[a], lsem.at[a]).wait()
        m = tab[MLEN + j]
        s = tab[SRC + j]
        b0 = m >> 4
        row = lax.broadcasted_iota(i32, (128, 128), 0) >> 3
        for buf, new in ((kb, kn), (vb, vn)):
            x = buf[a, b0].astype(f32)
            fresh = jnp.concatenate([new[j].astype(f32)] * BP, axis=0)
            t = b0 * BP + row
            buf[a, b0] = jnp.where(t < m, x, jnp.where(t == m, fresh, 0.0)).astype(bf16)

        def wipe(b, _):
            kb[a, b] = jnp.zeros((128, 128), bf16)
            vb[a, b] = jnp.zeros((128, 128), bf16)
            return 0

        lax.fori_loop(b0 + 1, BL, wipe, 0)
        kf = kb[a].reshape(BL * 128, 128)
        vf = vb[a].reshape(BL * 128, 128)
        sc = lax.dot_general(q[j], kf, (((1,), (1,)), ((), ())), preferred_element_type=f32) * (128 ** -0.5)
        col = lax.broadcasted_iota(i32, sc.shape, 1)
        head = lax.broadcasted_iota(i32, sc.shape, 0) // 3
        ok = ((col & 7) == head) & ((col >> 3) <= m)
        sc = jnp.where(ok, sc, -1e30)
        top = jnp.max(sc, axis=1, keepdims=True)
        w = jnp.exp(sc - top)
        tot = jnp.sum(w, axis=1, keepdims=True)
        acc = lax.dot_general(w.astype(bf16), vf, (((1,), (0,)), ((), ())), preferred_element_type=f32)
        ob[a] = (acc / tot).astype(bf16)
        bw = jnp.where(s >= 0, 0, b0)

        tail = pl.ds(bw, BL - bw)
        home = pl.ds(j * BL + bw, BL - bw)
        pltpu.make_async_copy(kb.at[a, tail], ko.at[home], wsem.at[0]).start()
        pltpu.make_async_copy(vb.at[a, tail], vo.at[home], wsem.at[0]).start()
        pltpu.make_async_copy(ob.at[a], ao.at[j], osem.at[0]).start()
        return 2 * (BL - bw)

    def batch(_, c):
        def pick(j, n):
            hit = (st[DONE + j] == 0) & (tab[RDY + j] < r) & (n < A)
            sel[jnp.where(hit, n, A)] = j
            st[DONE + j] = jnp.where(hit, 1, st[DONE + j])
            return n + jnp.where(hit, 1, 0)

        n = lax.fori_loop(0, SL, pick, jnp.int32(0))

        def loads(a, _):
            load(a, sel[a])
            return 0

        lax.fori_loop(0, n, loads, 0)

        def computes(a, cnt):
            return cnt + compute(a, sel[a])

        cnt = lax.fori_loop(0, n, computes, jnp.int32(0))

        @pl.when(n > 0)
        def _():
            done = ko.at[pl.ds(0, cnt)]
            pltpu.make_async_copy(done, done, wsem.at[0]).wait()
            rows = ob.at[pl.ds(0, n)]
            pltpu.make_async_copy(rows, rows, osem.at[0]).wait()

        return c

    lax.fori_loop(0, batches, batch, 0)


SMEM = pl.BlockSpec(memory_space=pltpu.SMEM)
VMEM = pl.BlockSpec(memory_space=pltpu.VMEM)
ANY = pl.BlockSpec(memory_space=pl.ANY)
BLOCK = (128, 128)


def sds(shape, dtype=bf16):
    return jax.ShapeDtypeStruct(shape, dtype)


def dma(n):
    return pltpu.SemaphoreType.DMA((n,))


def buf(*lead):
    return pltpu.VMEM(lead + BLOCK, bf16)


def cost(us):
    return pl.CostEstimate(flops=int(us * 4e6), bytes_accessed=int(us * 2e6), transcendentals=0)


ST = sds((STATE,), i32)


def solution(mesh):
    group = mesh.shape['dp']
    ring = [0, 1, 3, 2]
    cw = [(ring[k] * 2 + c, ring[(k + 1) % 4] * 2 + c) for k in range(4) for c in range(2)]
    ccw = [(b, a) for a, b in cw]
    swap = [(d, d ^ 1) for d in range(group)]

    def local(query, k_cache, v_cache, cache_lens, dest_slot, k_new, v_new):
        kc = k_cache.reshape((SL * BL,) + BLOCK)
        vc = v_cache.reshape((SL * BL,) + BLOCK)
        lens_all = pl.pallas_call(
            lens_kernel, out_shape=sds((8, 1, 128), i32), in_specs=[VMEM], out_specs=VMEM,
            scratch_shapes=[pltpu.SemaphoreType.DMA, dma(8), dma(8)],
            compiler_params=pltpu.CompilerParams(collective_id=0, has_side_effects=True),
            name='lens')(jnp.pad(cache_lens, (0, 96)).reshape(1, 128))
        me = jnp.full((1,), lax.axis_index('dp'), i32)
        tab, lens_out = pl.pallas_call(
            plan_kernel, out_shape=(sds((TAB,), i32), sds((SL,), i32)), in_specs=[SMEM] * 3, out_specs=(SMEM, SMEM),
            scratch_shapes=[pltpu.SMEM((256,), i32), pltpu.SMEM((256,), i32)] + [pltpu.SMEM((16,), i32)] * 3,
            name='plan')(me, dest_slot, lens_all)

        def nothing(*refs):
            pass

        chunk, both, cross = sds((NB,) + BLOCK), sds((2, NB) + BLOCK), sds((2, NX) + BLOCK)
        cache, store = sds((SL * BL,) + BLOCK), sds((2 * SL * BL,) + BLOCK)
        ko, vo, ao, f0, f1, rc0, rc1, po0, po1, dxr = pl.pallas_call(
            nothing, out_shape=(cache, cache, sds((SL, 24, 128)), store, store, chunk, chunk, chunk, chunk, cross),
            out_specs=(ANY,) * 10, name='blank')()

        st = jnp.zeros((STATE,), i32)
        st, part0, part1, dxs = pl.pallas_call(
            open_kernel, out_shape=(ST, both, both, cross), in_specs=[SMEM, SMEM, ANY, ANY], out_specs=(SMEM, ANY, ANY, ANY),
            scratch_shapes=[buf(2, 2, NB), buf(2, NX), dma(3)], name='open')(tab, st, kc, vc)
        pre0 = lax.ppermute(part0, 'dp', swap)
        pre = lax.ppermute(part1, 'dp', swap)
        st, s0, s1, part = pl.pallas_call(
            open_merge_kernel, out_shape=(ST, chunk, chunk, both), in_specs=[SMEM, SMEM, ANY, ANY, ANY],
            out_specs=(SMEM, ANY, ANY, ANY), scratch_shapes=[buf(2, NB), buf(2, NB), dma(3)],
            name='open_merge')(tab, st, kc, vc, pre0)

        def attend(st, ko, vo, ao, batches):
            return pl.pallas_call(
                functools.partial(attn_kernel, batches),
                out_shape=(ST, cache, cache, sds((SL, 24, 128))),
                in_specs=[SMEM, SMEM, VMEM, VMEM, VMEM, ANY, ANY, ANY, ANY, ANY], out_specs=(SMEM, ANY, ANY, ANY),
                input_output_aliases={7: 1, 8: 2, 9: 3},
                scratch_shapes=[buf(A, BL), buf(A, BL), pltpu.VMEM((A, 24, 128), bf16), pltpu.SMEM((A + 1,), i32),
                                dma(A), dma(1), dma(1)],
                cost_estimate=cost(6), name='attend')(tab, st, query, k_new, v_new, kc, vc, ko, vo, ao)

        def one_round(tag, c):
            st, s0, s1, part, dxs, pre, rc0, rc1, po0, po1, dxr, f0, f1, ko, vo, ao = c
            nrc0 = lax.ppermute(s0, 'dp', cw)
            nrc1 = lax.ppermute(s1, 'dp', ccw)
            npre = lax.ppermute(part, 'dp', swap)
            npo0 = lax.ppermute(rc0, 'dp', swap)
            npo1 = lax.ppermute(rc1, 'dp', swap)
            ndxr = lax.ppermute(dxs, 'dp', swap)
            st, s0, s1, part, dxs, f0, f1, ko, vo = pl.pallas_call(
                round_kernel, out_shape=(ST, chunk, chunk, both, cross, store, store, cache, cache),
                in_specs=[SMEM, SMEM] + [ANY] * 12, out_specs=(SMEM,) + (ANY,) * 8,
                input_output_aliases={10: 5, 11: 6, 12: 7, 13: 8},
                scratch_shapes=[buf(2, NB)] * 4 + [buf(2, NX)] * 2 + [dma(10)],
                cost_estimate=cost(10), name='round')(tab, st, kc, vc, pre, rc0, rc1, po0, po1, dxr, f0, f1, ko, vo)
            st, ko, vo, ao = attend(st, ko, vo, ao, 1)
            if tag == 'ra':
                s0, s1, npo0, npo1 = lax.optimization_barrier((s0, s1, npo0, npo1))
            return st, s0, s1, part, dxs, npre, nrc0, nrc1, npo0, npo1, ndxr, f0, f1, ko, vo, ao

        rounds = tab[ROUNDS]

        def body(c):
            return (c[0] + 2,) + one_round('rb', one_round('ra', c[1:]))

        c = lax.while_loop(lambda c: c[0] < rounds, body,
                       (jnp.int32(0), st, s0, s1, part, dxs, pre, rc0, rc1, po0, po1, dxr, f0, f1, ko, vo, ao))
        _, st, _, _, _, _, _, rc0, rc1, po0, po1, dxr, _, _, ko, vo, ao = c

        def close(last, st, ko, vo, *ins):
            n = len(ins)
            extra = [] if last else [buf(2, NB), buf(2, NX)]
            return pl.pallas_call(
                functools.partial(close_kernel, last), out_shape=(ST, cache, cache),
                in_specs=[SMEM, SMEM] + [ANY] * (n + 2), out_specs=(SMEM, ANY, ANY),
                input_output_aliases={n + 2: 1, n + 3: 2},
                scratch_shapes=[buf(2, NB)] + extra + [dma(6)],
                name='close_last' if last else 'close')(tab, st, *ins, ko, vo)

        lpo0 = lax.ppermute(rc0, 'dp', swap)
        lpo1 = lax.ppermute(rc1, 'dp', swap)
        st, ko, vo = close(False, st, ko, vo, rc0, rc1, po0, po1, dxr)
        st, ko, vo = close(True, st, ko, vo, lpo0, lpo1)
        st, ko, vo, ao = attend(st, ko, vo, ao, SL // A)
        return ao, ko.reshape(k_cache.shape), vo.reshape(v_cache.shape), lens_out

    row_spec = P('dp')
    return jax.shard_map(local, mesh=mesh, in_specs=(row_spec, row_spec, row_spec, row_spec, P(), row_spec, row_spec),
                         out_specs=(row_spec, row_spec, row_spec, row_spec), check_vma=False)
```

```python
import functools

import jax
import jax.numpy as jnp
from jax import lax
from jax.experimental import pallas as pl
from jax.experimental.pallas import tpu as pltpu
from jax.sharding import PartitionSpec as P


BP, SHIFT = 8, 3
SIZES = (64, 58, 52)
NX = 32
A = 4
SL = 32
BL = 64
WIDE = 272
S0, S1, R0, R1, XS, XR, FREE = range(7)
RDY, RDX, MLEN, SRC, ROUNDS = range(FREE * WIDE, FREE * WIDE + 200, 40)
CORE, PICK, DUMP = ROUNDS + 1, ROUNDS + 2, ROUNDS + 4
TAB = ROUNDS + 8
FWD, NONE = 2, 3
HALF = 1 << 16
FLOPS = 4000000
LOW = HALF - 1
U_PART, U_MERGE, U_OWN, U_POST, U_XS, U_XR = 0, 2, 4, 6, 8, 9
STEP, DONE, STATE = 24, 32, 64
END = HALF * HALF // 4
bf16 = jnp.bfloat16
f32 = jnp.float32
i32 = jnp.int32


def gray(c):
    return c ^ (c >> 1)


def lens_kernel(x, o, bsem, ssem, rsem):
    me = lax.axis_index('dp')
    barrier = pltpu.get_barrier_semaphore()
    for k in range(1, 8):
        pl.semaphore_signal(barrier, inc=1, device_id=(lax.rem(me + k, 8),), device_id_type=pl.DeviceIdType.MESH)
    pl.semaphore_wait(barrier, 7)
    here = pltpu.make_async_copy(x, o.at[me], bsem)
    here.start()
    sends = []
    for k in range(1, 8):
        c = pltpu.make_async_remote_copy(src_ref=x, dst_ref=o.at[me], send_sem=ssem.at[k], recv_sem=rsem.at[k],
                                         device_id=(lax.rem(me + k, 8),), device_id_type=pl.DeviceIdType.MESH)
        c.start()
        sends.append(c)
    here.wait()
    for c in sends:
        c.wait()


def plan_kernel(me_ref, dest_ref, len_ref, tab, lens_out, nbv, kindv, todo, load, hop, swap, addr, at):
    me = me_ref[0]
    zero = me * 0
    for i in range(9):
        for ref in (load, hop, swap):
            ref[i] = zero
    tab[CORE] = me & 1
    for j in range(SL):
        tab[RDY + j] = zero
        tab[RDX + j] = zero

    def first(i, n):
        size = len_ref[i >> 5, 0, i & 31]
        d = dest_ref[i]
        nb = (size + (BP - 1)) >> SHIFT
        ra = gray(i >> 6)
        delta = (gray(d >> 6) - ra) & 3
        nbv[i] = nb
        kindv[i] = delta
        slot = jnp.where(delta == 1, ra, jnp.where(delta == 3, 4 + ra, 8))
        load[slot] = load[slot] + nb + HALF
        todo[n] = i
        cross = (delta == 0) & ((i >> 5) != (d >> 5))
        xslot = jnp.where(cross, i >> 5, 8)
        swap[xslot] = swap[xslot] + nb
        mine = jnp.where((d >> 5) == me, d & 31, SL)
        tab[MLEN + mine] = size
        tab[SRC + mine] = jnp.where((i >> 5) == me, i & 31, -1)
        return n + jnp.where(delta == 2, 1, 0)

    far = lax.fori_loop(0, 8 * SL, first, zero, unroll=4)

    def lens(j, c):
        lens_out[j] = tab[MLEN + j] + 1
        return c

    lax.fori_loop(0, SL, lens, 0, unroll=8)

    def choose(n, c):
        i = todo[n]
        nb = nbv[i]
        ra = gray(i >> 6)
        a1, a2, b1, b2 = ra, (ra + 1) & 3, 4 + ra, 4 + ((ra - 1) & 3)
        la1, la2, lb1, lb2 = load[a1] & LOW, load[a2] & LOW, load[b1] & LOW, load[b2] & LOW
        la, lb = jnp.maximum(la1, la2), jnp.maximum(lb1, lb2)
        cw = (la < lb) | ((la == lb) & (la1 + la2 <= lb1 + lb2))
        x1, x2 = jnp.where(cw, a1, b1), jnp.where(cw, a2, b2)
        load[x1] = load[x1] + nb + HALF
        load[x2] = load[x2] + nb + HALF
        hop[x1] = hop[x1] + nb + HALF
        kindv[i] = jnp.where(cw, 2, 4)
        return c

    lax.fori_loop(0, far, choose, 0)

    def link(d, x, size):
        fwd = hop[4 * d + ((x - 1 + 2 * d) & 3)]
        own = load[4 * d + x] - fwd
        start = jnp.where(fwd > 0, jnp.maximum(own & LOW, 2 * size), own & LOW)
        return own, fwd, start

    cross = zero
    for d in range(8):
        cross = jnp.maximum(cross, (swap[d] + NX - 1) // NX)
    best, pick, turns, chunk = zero + END, zero, zero, zero
    for o, size in enumerate(SIZES):
        longest = zero
        for d in range(2):
            for x in range(4):
                _, fwd, start = link(d, x, size)
                longest = jnp.maximum(longest, start + (fwd & LOW))
        rounds = (jnp.maximum((longest + size - 1) // size, cross) + 1) & -2
        price = rounds * (size + BP // 2)
        better = price < best
        best, pick, turns, chunk = [jnp.where(better, n, o) for n, o in (
            (price, best), (o, pick), (rounds, turns), (size, chunk))]
    tab[ROUNDS] = turns
    tab[PICK] = pick

    x0 = gray(me >> 1)
    left, right, opposite = (x0 - 1) & 3, (x0 + 1) & 3, (x0 + 2) & 3
    for lid, d, x in ((S0, 0, x0), (S1, 1, x0), (R0, 0, left), (R1, 1, right)):
        own, fwd, start = link(d, x, chunk)
        near = hop[4 * d + x]
        base = lid * WIDE
        pad = base + 2 * (own >> 16)
        last = pad + 2 + 2 * (fwd >> 16)
        tab[pad] = start - (own & LOW)
        tab[last] = zero + END
        for a in (pad, last):
            tab[a + 1] = zero + NONE * HALF
        for k, (where, pos) in enumerate(((base, 0), (base + 2 * (near >> 16), near & LOW), (pad + 2, start))):
            addr[3 * lid + k] = zero + where
            at[3 * lid + k] = zero + pos
    addr[12] = zero + DUMP
    at[12] = zero

    def append(seg, hit, nb, code):
        seg = jnp.where(hit, seg, 12)
        a, p = addr[seg], at[seg]
        tab[a] = nb
        tab[a + 1] = code
        addr[seg] = a + jnp.where(hit, 2, 0)
        at[seg] = p + nb
        return p + nb

    def source(s, c):
        i = (me >> 1) * 2 * SL + s
        kind = kindv[i]
        seg = jnp.where(kind < 3, 2 - kind, 7 - kind)
        append(seg, kind > 0, nbv[i], ((s >> 5) << 16) + (s & 31) * BL)
        return c

    lax.fori_loop(0, 2 * SL, source, 0, unroll=4)

    def arrive(seg, hit, i):
        dst = dest_ref[i]
        end = append(seg, hit, nbv[i], (((dst >> 5) & 1) << 16) + (dst & 31) * BL)
        mine = hit & ((dst >> 5) == me)
        tab[RDY + jnp.where(mine, dst & 31, SL)] = end

    for d, x in ((0, left), (1, right)):
        def upstream(s, c):
            i = gray(x) * 2 * SL + s
            kind = kindv[i]
            hit = kind == 2 + 2 * d
            code = FWD * HALF + at[6 + 3 * d]
            append(6 + 3 * d, hit, nbv[i], code)
            append(2 + 3 * d, hit, nbv[i], code)
            arrive(7 + 3 * d, kind == 1 + 2 * d, i)
            return c

        lax.fori_loop(0, 2 * SL, upstream, 0, unroll=2)

    def across(s, c):
        i = gray(opposite) * 2 * SL + s
        kind = kindv[i]
        arrive(jnp.where(kind == 2, 8, 11), (kind == FWD) | (kind == 4), i)
        return c

    lax.fori_loop(0, 2 * SL, across, 0, unroll=2)

    for lid, sender, receiver in ((XS, me, me ^ 1), (XR, me ^ 1, me)):
        def cross_list(s, c):
            a, pos = c
            i = sender * SL + s
            nb = nbv[i]
            dst = dest_ref[i]
            hit = (dst >> 5) == receiver
            tab[a] = nb
            tab[a + 1] = (s if lid == XS else dst & 31) * BL
            pos = pos + jnp.where(hit, nb, 0)
            if lid == XR:
                tab[RDX + jnp.where(hit, dst & 31, SL)] = pos
            return a + jnp.where(hit, 2, 0), pos

        a, _ = lax.fori_loop(0, SL, cross_list, (zero + lid * WIDE, zero), unroll=2)
        tab[a] = zero + END
        tab[a + 1] = zero + NONE * HALF


class Mover:
    def __init__(self, tab, st_in, st, size):
        self.tab, self.st, self.size = tab, st, size
        self.core = tab[CORE]

        def cp(i, _):
            st[i] = st_in[i]
            return 0

        lax.fori_loop(0, STATE, cp, 0)

    def walk(self, lid, use, n, fn):
        tab, st = self.tab, self.st
        base = lid * WIDE

        def body(c):
            p, item, off, cnt = c
            width = tab[base + 2 * item]
            code = tab[base + 2 * item + 1]
            take = jnp.minimum(n - p, width - off)
            cnt = cnt + fn(p, take, code >> 16, (code & LOW) + off)
            off = off + take
            adv = off >= width
            return p + take, jnp.where(adv, item + 1, item), jnp.where(adv, 0, off), cnt

        c0 = (jnp.int32(0), st[2 * use], st[2 * use + 1], jnp.int32(0))
        _, item, off, cnt = lax.while_loop(lambda c: c[0] < n, body, c0)
        st[2 * use] = item
        st[2 * use + 1] = off
        return cnt

    @staticmethod
    def drain(cnt, ref, sem):
        @pl.when(cnt > 0)
        def _():
            part = ref.at[pl.ds(0, cnt)]
            pltpu.make_async_copy(part, part, sem).wait()

    def partial(self, d, kc, vc, buf, sem):
        core = self.core

        def fn(p, take, kind, idx):
            mine = kind == core

            @pl.when(mine & (core == 0))
            def _():
                pltpu.make_async_copy(vc.at[pl.ds(idx, take)], buf.at[d, pl.ds(p, take)], sem).start()

            @pl.when(mine & (core == 1))
            def _():
                pltpu.make_async_copy(kc.at[pl.ds(idx, take)], buf.at[d, pl.ds(p, take)], sem).start()

            return jnp.where(mine, take, 0)

        return self.walk(S0 + d, U_PART + d, self.size, fn)

    def merge(self, d, kc, vc, pre, fwd, buf, sem):
        core = self.core

        def fn(p, take, kind, idx):
            mine = kind == core

            @pl.when(mine & (core == 0))
            def _():
                pltpu.make_async_copy(kc.at[pl.ds(idx, take)], buf.at[d, pl.ds(p, take)], sem).start()

            @pl.when(mine & (core == 1))
            def _():
                pltpu.make_async_copy(vc.at[pl.ds(idx, take)], buf.at[d, pl.ds(p, take)], sem).start()

            @pl.when(kind == 1 - core)
            def _():
                pltpu.make_async_copy(pre.at[d, pl.ds(p, take)], buf.at[d, pl.ds(p, take)], sem).start()

            if fwd is not None:
                @pl.when(kind == FWD)
                def _():
                    pltpu.make_async_copy(fwd.at[pl.ds(idx, take)], buf.at[d, pl.ds(p, take)], sem).start()
            return jnp.where(kind < NONE, take, 0)

        return self.walk(S0 + d, U_MERGE + d, self.size, fn)

    def cross_send(self, kc, vc, buf, sem):
        def fn(p, take, kind, idx):
            @pl.when(kind == 0)
            def _():
                pltpu.make_async_copy(kc.at[pl.ds(idx, take)], buf.at[0, pl.ds(p, take)], sem).start()
                pltpu.make_async_copy(vc.at[pl.ds(idx, take)], buf.at[1, pl.ds(p, take)], sem).start()

            return jnp.where(kind == 0, 2 * take, 0)

        return self.walk(XS, U_XS, NX, fn)

    def cross_recv(self, n, ko, vo, buf, sem):
        def fn(p, take, kind, idx):
            @pl.when(kind == 0)
            def _():
                pltpu.make_async_copy(buf.at[0, pl.ds(p, take)], ko.at[pl.ds(idx, take)], sem).start()
                pltpu.make_async_copy(buf.at[1, pl.ds(p, take)], vo.at[pl.ds(idx, take)], sem).start()

            return jnp.where(kind == 0, 2 * take, 0)

        return self.walk(XR, U_XR, n, fn)

    def unpack(self, d, use, n, flip, ko, vo, fwd, buf, sem):
        core = self.core
        plane = 1 - core if flip else core

        def fn(p, take, kind, idx):
            mine = kind == core

            @pl.when(mine & (plane == 0))
            def _():
                pltpu.make_async_copy(buf.at[d, pl.ds(p, take)], ko.at[pl.ds(idx, take)], sem).start()

            @pl.when(mine & (plane == 1))
            def _():
                pltpu.make_async_copy(buf.at[d, pl.ds(p, take)], vo.at[pl.ds(idx, take)], sem).start()

            cnt = jnp.where(mine, take, 0)
            if fwd is not None:
                @pl.when(kind == FWD)
                def _():
                    pltpu.make_async_copy(buf.at[d, pl.ds(p, take)], fwd.at[pl.ds(idx, take)], sem).start()

                cnt = cnt + jnp.where(kind == FWD, take, 0)
            return cnt

        return self.walk(R0 + d, use + d, n, fn)


def open_kernel(NB, tab, st_in, kc, vc, st, part0, part1, dxs, vpart, vdx, sem):
    mv = Mover(tab, st_in, st, NB)
    outs = [pltpu.make_async_copy(vpart.at[0], part0, sem.at[0]),
            pltpu.make_async_copy(vpart.at[1], part1, sem.at[1]),
            pltpu.make_async_copy(vdx, dxs, sem.at[2])]
    cnt = [mv.partial(0, kc, vc, vpart.at[c], sem.at[c]) + mv.partial(1, kc, vc, vpart.at[c], sem.at[c]) for c in range(2)]
    cnt.append(mv.cross_send(kc, vc, vdx, sem.at[2]))
    for c in range(3):
        mv.drain(cnt[c], kc, sem.at[c])
        outs[c].start()
    for c in outs:
        c.wait()


def open_merge_kernel(NB, tab, st_in, kc, vc, pre, st, send0, send1, part, vsend, vpart, sem):
    mv = Mover(tab, st_in, st, NB)
    c0 = mv.merge(0, kc, vc, pre, None, vsend, sem.at[0])
    c1 = mv.merge(1, kc, vc, pre, None, vsend, sem.at[1])
    c2 = mv.partial(0, kc, vc, vpart, sem.at[2]) + mv.partial(1, kc, vc, vpart, sem.at[2])
    mv.drain(c0, kc, sem.at[0])
    mv.drain(c1, kc, sem.at[1])
    mv.drain(c2, kc, sem.at[2])
    outs = [pltpu.make_async_copy(vsend.at[0], send0, sem.at[0]),
            pltpu.make_async_copy(vsend.at[1], send1, sem.at[1]),
            pltpu.make_async_copy(vpart, part, sem.at[2])]
    for c in outs:
        c.start()
    for c in outs:
        c.wait()


def round_kernel(NB, tab, st_in, kc, vc, pre, rc0, rc1, po0, po1, dxr, f0i, f1i, koi, voi,
                 st, send0, send1, part, dxs, f0, f1, ko, vo,
                 vsend, vpart, vrecv, vpost, vdxs, vdxr, sem):
    mv = Mover(tab, st_in, st, NB)
    r = st_in[STEP]
    st[STEP] = r + 1
    ins = [pltpu.make_async_copy(rc0, vrecv.at[0], sem.at[0]),
           pltpu.make_async_copy(rc1, vrecv.at[1], sem.at[1]),
           pltpu.make_async_copy(po0, vpost.at[0], sem.at[2]),
           pltpu.make_async_copy(po1, vpost.at[1], sem.at[3]),
           pltpu.make_async_copy(dxr, vdxr, sem.at[4])]
    for c in ins:
        c.start()
    n1 = jnp.where(r >= 1, NB, 0)
    n2 = jnp.where(r >= 2, NB, 0)
    nx = jnp.where(r >= 1, NX, 0)
    cp = mv.partial(0, kc, vc, vpart, sem.at[5]) + mv.partial(1, kc, vc, vpart, sem.at[5])
    cx = mv.cross_send(kc, vc, vdxs, sem.at[6])
    ins[0].wait()
    o0 = mv.unpack(0, U_OWN, n1, False, ko, vo, f0, vrecv, sem.at[7])
    ins[1].wait()
    o1 = mv.unpack(1, U_OWN, n1, False, ko, vo, f1, vrecv, sem.at[7])
    mv.drain(o0 + o1, kc, sem.at[7])
    c0 = mv.merge(0, kc, vc, pre, f0, vsend, sem.at[8])
    c1 = mv.merge(1, kc, vc, pre, f1, vsend, sem.at[9])
    ins[2].wait()
    ins[3].wait()
    o2 = mv.unpack(0, U_POST, n2, True, ko, vo, None, vpost, sem.at[7])
    o3 = mv.unpack(1, U_POST, n2, True, ko, vo, None, vpost, sem.at[7])
    ins[4].wait()
    o4 = mv.cross_recv(nx, ko, vo, vdxr, sem.at[7])
    mv.drain(cp, kc, sem.at[5])
    mv.drain(cx, kc, sem.at[6])
    mv.drain(c0, kc, sem.at[8])
    mv.drain(c1, kc, sem.at[9])
    outs = [pltpu.make_async_copy(vsend.at[0], send0, sem.at[0]),
            pltpu.make_async_copy(vsend.at[1], send1, sem.at[1]),
            pltpu.make_async_copy(vpart, part, sem.at[2]),
            pltpu.make_async_copy(vdxs, dxs, sem.at[3])]
    for c in outs:
        c.start()
    mv.drain(o2 + o3 + o4, kc, sem.at[7])
    for c in outs:
        c.wait()


def close_kernel(NB, last, tab, st_in, *refs):
    if last:
        (po0, po1, koi, voi, st, ko, vo, vpost, sem) = refs
    else:
        (rc0, rc1, po0, po1, dxr, koi, voi, st, ko, vo, vpost, vrecv, vdxr, sem) = refs
    mv = Mover(tab, st_in, st, NB)
    r = st_in[STEP]
    st[STEP] = r + 1
    ins = [pltpu.make_async_copy(po0, vpost.at[0], sem.at[0]),
           pltpu.make_async_copy(po1, vpost.at[1], sem.at[1])]
    if not last:
        ins += [pltpu.make_async_copy(rc0, vrecv.at[0], sem.at[2]),
                pltpu.make_async_copy(rc1, vrecv.at[1], sem.at[3]),
                pltpu.make_async_copy(dxr, vdxr, sem.at[4])]
    for c in ins:
        c.start()
    n1 = jnp.where(r >= 1, NB, 0)
    n2 = jnp.where(r >= 2, NB, 0)
    nx = jnp.where(r >= 1, NX, 0)
    for c in ins:
        c.wait()
    cnt = mv.unpack(0, U_POST, n2, True, ko, vo, None, vpost, sem.at[5])
    cnt += mv.unpack(1, U_POST, n2, True, ko, vo, None, vpost, sem.at[5])
    if not last:
        cnt += mv.unpack(0, U_OWN, n1, False, ko, vo, None, vrecv, sem.at[5])
        cnt += mv.unpack(1, U_OWN, n1, False, ko, vo, None, vrecv, sem.at[5])
        cnt += mv.cross_recv(nx, ko, vo, vdxr, sem.at[5])
    mv.drain(cnt, ko, sem.at[5])


def attn_kernel(NB, batches, tab, st_in, q, kn, vn, kc, vc, koi, voi, aoi, st, ko, vo, ao,
                kb, vb, ob, sel, lsem, wsem, osem):
    def cp(i, _):
        st[i] = st_in[i]
        return 0

    lax.fori_loop(0, STATE, cp, 0)
    link_end = jnp.maximum((st_in[STEP] - 2) * NB, 0)
    swap_end = jnp.maximum((st_in[STEP] - 1) * NX, 0)

    def load(a, j):
        s = tab[SRC + j]

        @pl.when(s >= 0)
        def _():
            pltpu.make_async_copy(kc.at[pl.ds(s * BL, BL)], kb.at[a], lsem.at[a]).start()
            pltpu.make_async_copy(vc.at[pl.ds(s * BL, BL)], vb.at[a], lsem.at[a]).start()

        @pl.when(s < 0)
        def _():
            pltpu.make_async_copy(ko.at[pl.ds(j * BL, BL)], kb.at[a], lsem.at[a]).start()
            pltpu.make_async_copy(vo.at[pl.ds(j * BL, BL)], vb.at[a], lsem.at[a]).start()

    def compute(a, j):
        pltpu.make_async_copy(kb.at[a], kb.at[a], lsem.at[a]).wait()
        pltpu.make_async_copy(vb.at[a], vb.at[a], lsem.at[a]).wait()
        m = tab[MLEN + j]
        s = tab[SRC + j]
        b0 = m >> SHIFT
        row = lax.broadcasted_iota(i32, BLOCK, 0) >> 3
        for buf, new in ((kb, kn), (vb, vn)):
            x = buf[a, b0].astype(f32)
            fresh = jnp.concatenate([new[j].astype(f32)] * BP, axis=0)
            t = b0 * BP + row
            buf[a, b0] = jnp.where(t < m, x, jnp.where(t == m, fresh, 0.0)).astype(bf16)

        def wipe(b, _):
            kb[a, b] = jnp.zeros(BLOCK, bf16)
            vb[a, b] = jnp.zeros(BLOCK, bf16)
            return 0

        lax.fori_loop(b0 + 1, BL, wipe, 0)
        kf = kb[a].reshape(-1, 128)
        vf = vb[a].reshape(-1, 128)
        sc = lax.dot_general(q[j], kf, (((1,), (1,)), ((), ())), preferred_element_type=f32) * (128 ** -0.5)
        col = lax.broadcasted_iota(i32, sc.shape, 1)
        head = lax.broadcasted_iota(i32, sc.shape, 0) // 3
        ok = ((col & 7) == head) & ((col >> 3) <= m)
        sc = jnp.where(ok, sc, -1e30)
        top = jnp.max(sc, axis=1, keepdims=True)
        w = jnp.exp(sc - top)
        tot = jnp.sum(w, axis=1, keepdims=True)
        acc = lax.dot_general(w.astype(bf16), vf, (((1,), (0,)), ((), ())), preferred_element_type=f32)
        ob[a] = (acc / tot).astype(bf16)
        bw = jnp.where(s >= 0, 0, b0)

        tail = pl.ds(bw, BL - bw)
        home = pl.ds(j * BL + bw, BL - bw)
        pltpu.make_async_copy(kb.at[a, tail], ko.at[home], wsem.at[0]).start()
        pltpu.make_async_copy(vb.at[a, tail], vo.at[home], wsem.at[0]).start()
        pltpu.make_async_copy(ob.at[a], ao.at[j], osem.at[0]).start()
        return 2 * (BL - bw)

    def batch(_, c):
        def pick(j, n):
            hit = (st[DONE + j] == 0) & (tab[RDY + j] <= link_end) & (tab[RDX + j] <= swap_end) & (n < A)
            sel[jnp.where(hit, n, A)] = j
            st[DONE + j] = jnp.where(hit, 1, st[DONE + j])
            return n + jnp.where(hit, 1, 0)

        n = lax.fori_loop(0, SL, pick, jnp.int32(0))

        def loads(a, _):
            load(a, sel[a])
            return 0

        lax.fori_loop(0, n, loads, 0)

        def computes(a, cnt):
            return cnt + compute(a, sel[a])

        cnt = lax.fori_loop(0, n, computes, jnp.int32(0))

        @pl.when(n > 0)
        def _():
            done = ko.at[pl.ds(0, cnt)]
            pltpu.make_async_copy(done, done, wsem.at[0]).wait()
            rows = ob.at[pl.ds(0, n)]
            pltpu.make_async_copy(rows, rows, osem.at[0]).wait()

        return c

    lax.fori_loop(0, batches, batch, 0)


SMEM = pl.BlockSpec(memory_space=pltpu.SMEM)
VMEM = pl.BlockSpec(memory_space=pltpu.VMEM)
ANY = pl.BlockSpec(memory_space=pl.ANY)
BLOCK = (8 * BP, 128)


def sds(shape, dtype=bf16):
    return jax.ShapeDtypeStruct(shape, dtype)


def dma(n):
    return pltpu.SemaphoreType.DMA((n,))


def buf(*lead):
    return pltpu.VMEM(lead + BLOCK, bf16)


def cost(us):
    return pl.CostEstimate(flops=us * FLOPS, bytes_accessed=us * FLOPS, transcendentals=0)


ST = sds((STATE,), i32)


def solution(mesh):
    group = mesh.shape['dp']
    ring = [0, 1, 3, 2]
    cw = [(ring[k] * 2 + c, ring[(k + 1) % 4] * 2 + c) for k in range(4) for c in range(2)]
    ccw = [(b, a) for a, b in cw]
    swap = [(d, d ^ 1) for d in range(group)]

    def local(query, k_cache, v_cache, cache_lens, dest_slot, k_new, v_new):
        kc = k_cache.reshape((SL * BL,) + BLOCK)
        vc = v_cache.reshape((SL * BL,) + BLOCK)
        lens_all = pl.pallas_call(
            lens_kernel, out_shape=sds((8, 1, SL), i32), in_specs=[VMEM], out_specs=VMEM,
            scratch_shapes=[pltpu.SemaphoreType.DMA, dma(8), dma(8)],
            compiler_params=pltpu.CompilerParams(collective_id=0, has_side_effects=True),
            name='lens')(cache_lens.reshape(1, SL))
        me = jnp.full((1,), lax.axis_index('dp'), i32)
        tab, lens_out = pl.pallas_call(
            plan_kernel, out_shape=(sds((TAB,), i32), sds((SL,), i32)), in_specs=[SMEM] * 3, out_specs=(SMEM, SMEM),
            scratch_shapes=[pltpu.SMEM((8 * SL + 1,), i32)] * 3 + [pltpu.SMEM((16,), i32)] * 5,
            name='plan')(me, dest_slot, lens_all)

        def run(NB):
            def nothing(*refs):
                pass

            chunk, both, cross = sds((NB,) + BLOCK), sds((2, NB) + BLOCK), sds((2, NX) + BLOCK)
            cache, store = sds((SL * BL,) + BLOCK), sds((2 * SL * BL,) + BLOCK)
            ko, vo, ao, f0, f1, rc0, rc1, po0, po1, dxr = pl.pallas_call(
                nothing, out_shape=(cache, cache, sds((SL, 24, 128)), store, store, chunk, chunk, chunk, chunk, cross),
                out_specs=(ANY,) * 10, name='blank')()

            st = jnp.zeros((STATE,), i32)
            st, part0, part1, dxs = pl.pallas_call(
                functools.partial(open_kernel, NB), out_shape=(ST, both, both, cross), in_specs=[SMEM, SMEM, ANY, ANY], out_specs=(SMEM, ANY, ANY, ANY),
                scratch_shapes=[buf(2, 2, NB), buf(2, NX), dma(3)], name='open')(tab, st, kc, vc)
            pre0 = lax.ppermute(part0, 'dp', swap)
            pre = lax.ppermute(part1, 'dp', swap)
            st, s0, s1, part = pl.pallas_call(
                functools.partial(open_merge_kernel, NB), out_shape=(ST, chunk, chunk, both), in_specs=[SMEM, SMEM, ANY, ANY, ANY],
                out_specs=(SMEM, ANY, ANY, ANY), scratch_shapes=[buf(2, NB), buf(2, NB), dma(3)],
                name='open_merge')(tab, st, kc, vc, pre0)

            def attend(st, ko, vo, ao, batches):
                return pl.pallas_call(
                    functools.partial(attn_kernel, NB, batches),
                    out_shape=(ST, cache, cache, sds((SL, 24, 128))),
                    in_specs=[SMEM, SMEM, VMEM, VMEM, VMEM, ANY, ANY, ANY, ANY, ANY], out_specs=(SMEM, ANY, ANY, ANY),
                    input_output_aliases={7: 1, 8: 2, 9: 3},
                    scratch_shapes=[buf(A, BL), buf(A, BL), pltpu.VMEM((A, 24, 128), bf16), pltpu.SMEM((A + 1,), i32),
                                    dma(A), dma(1), dma(1)],
                    cost_estimate=cost(6), name='attend')(tab, st, query, k_new, v_new, kc, vc, ko, vo, ao)

            def one_round(tag, c):
                st, s0, s1, part, dxs, pre, rc0, rc1, po0, po1, dxr, f0, f1, ko, vo, ao = c
                nrc0 = lax.ppermute(s0, 'dp', cw)
                nrc1 = lax.ppermute(s1, 'dp', ccw)
                npre = lax.ppermute(part, 'dp', swap)
                npo0 = lax.ppermute(rc0, 'dp', swap)
                npo1 = lax.ppermute(rc1, 'dp', swap)
                ndxr = lax.ppermute(dxs, 'dp', swap)
                st, s0, s1, part, dxs, f0, f1, ko, vo = pl.pallas_call(
                    functools.partial(round_kernel, NB), out_shape=(ST, chunk, chunk, both, cross, store, store, cache, cache),
                    in_specs=[SMEM, SMEM] + [ANY] * 12, out_specs=(SMEM,) + (ANY,) * 8,
                    input_output_aliases={10: 5, 11: 6, 12: 7, 13: 8},
                    scratch_shapes=[buf(2, NB)] * 4 + [buf(2, NX)] * 2 + [dma(10)],
                    cost_estimate=cost(10), name='round')(tab, st, kc, vc, pre, rc0, rc1, po0, po1, dxr, f0, f1, ko, vo)
                st, ko, vo, ao = attend(st, ko, vo, ao, 1)
                if tag == 'ra':
                    s0, s1, npo0, npo1 = lax.optimization_barrier((s0, s1, npo0, npo1))
                return st, s0, s1, part, dxs, npre, nrc0, nrc1, npo0, npo1, ndxr, f0, f1, ko, vo, ao

            rounds = tab[ROUNDS]

            def body(c):
                return (c[0] + 2,) + one_round('rb', one_round('ra', c[1:]))

            c = lax.while_loop(lambda c: c[0] < rounds, body,
                           (jnp.int32(0), st, s0, s1, part, dxs, pre, rc0, rc1, po0, po1, dxr, f0, f1, ko, vo, ao))
            _, st, _, _, _, _, _, rc0, rc1, po0, po1, dxr, _, _, ko, vo, ao = c

            def close(last, st, ko, vo, *ins):
                n = len(ins)
                extra = [] if last else [buf(2, NB), buf(2, NX)]
                return pl.pallas_call(
                    functools.partial(close_kernel, NB, last), out_shape=(ST, cache, cache),
                    in_specs=[SMEM, SMEM] + [ANY] * (n + 2), out_specs=(SMEM, ANY, ANY),
                    input_output_aliases={n + 2: 1, n + 3: 2},
                    scratch_shapes=[buf(2, NB)] + extra + [dma(6)],
                    name='close_last' if last else 'close')(tab, st, *ins, ko, vo)

            lpo0 = lax.ppermute(rc0, 'dp', swap)
            lpo1 = lax.ppermute(rc1, 'dp', swap)
            st, ko, vo = close(False, st, ko, vo, rc0, rc1, po0, po1, dxr)
            st, ko, vo = close(True, st, ko, vo, lpo0, lpo1)
            st, ko, vo, ao = attend(st, ko, vo, ao, SL // A)
            return ao, ko, vo

        ao, ko, vo = lax.switch(tab[PICK], [functools.partial(run, size) for size in SIZES])
        return ao, ko.reshape(k_cache.shape), vo.reshape(v_cache.shape), lens_out

    row_spec = P('dp')
    return jax.shard_map(local, mesh=mesh, in_specs=(row_spec, row_spec, row_spec, row_spec, P(), row_spec, row_spec),
                         out_specs=(row_spec, row_spec, row_spec, row_spec), check_vma=False)
```

```python
import functools

import jax
import jax.numpy as jnp
from jax import lax
from jax.experimental import pallas as pl
from jax.experimental.pallas import tpu as pltpu
from jax.sharding import PartitionSpec as P


BP, SHIFT = 8, 3
SIZES = (66, 60, 54, 48)
NX = 32
A = 4
SL = 32
BL = 64
WIDE = 400
S0, S1, R0, R1, XS, XR, FREE = range(7)
RDY, RDX, MLEN, SRC, ROUNDS = range(FREE * WIDE, FREE * WIDE + 200, 40)
CORE, PICK, DUMP = ROUNDS + 1, ROUNDS + 2, ROUNDS + 4
TAB = ROUNDS + 8
FWD, NONE = 2, 3
TURN = 4
SEGS = 6
IDLE = 4 * SEGS
HALF = 1 << 16
FLOPS = 4000000
LOW = HALF - 1
U_PART, U_MERGE, U_OWN, U_POST, U_XS, U_XR = 0, 2, 4, 6, 8, 9
STEP, DONE, STATE = 24, 32, 64
END = HALF * HALF // 4
bf16 = jnp.bfloat16
f32 = jnp.float32
i32 = jnp.int32


def gray(c):
    return c ^ (c >> 1)


def lens_kernel(x, o, bsem, ssem, rsem):
    me = lax.axis_index('dp')
    barrier = pltpu.get_barrier_semaphore()
    for k in range(1, 8):
        pl.semaphore_signal(barrier, inc=1, device_id=(lax.rem(me + k, 8),), device_id_type=pl.DeviceIdType.MESH)
    pl.semaphore_wait(barrier, 7)
    here = pltpu.make_async_copy(x, o.at[me], bsem)
    here.start()
    sends = []
    for k in range(1, 8):
        c = pltpu.make_async_remote_copy(src_ref=x, dst_ref=o.at[me], send_sem=ssem.at[k], recv_sem=rsem.at[k],
                                         device_id=(lax.rem(me + k, 8),), device_id_type=pl.DeviceIdType.MESH)
        c.start()
        sends.append(c)
    here.wait()
    for c in sends:
        c.wait()


def plan_kernel(me_ref, dest_ref, len_ref, tab, lens_out, nbv, kindv, todo, near, load, one, two, three, swap, addr, at):
    me = me_ref[0]
    zero = me - me
    for i in range(9):
        for ref in (load, one, two, three, swap):
            ref[i] = zero
    tab[CORE] = me & 1
    for j in range(SL):
        tab[RDY + j] = zero
        tab[RDX + j] = zero

    def first(i, c):
        size = len_ref[i >> 5, 0, i & 31]
        d = dest_ref[i]
        nb = (size + (BP - 1)) >> SHIFT
        ra = gray(i >> 6)
        delta = (gray(d >> 6) - ra) & 3
        nbv[i] = nb
        beside = (delta & 1) == 1
        ccw = delta == 3
        kindv[i] = jnp.where(beside, jnp.where(ccw, 4, 1), 0)
        slot = jnp.where(beside, jnp.where(ccw, 4, 0) + ra, 8)
        one[slot] = one[slot] + nb + HALF
        load[slot] = load[slot] + nb
        todo[c[0]] = i
        near[c[1]] = i
        cross = (delta == 0) & ((i >> 5) != (d >> 5))
        xslot = jnp.where(cross, i >> 5, 8)
        swap[xslot] = swap[xslot] + nb
        mine = jnp.where((d >> 5) == me, d & 31, SL)
        tab[MLEN + mine] = size
        tab[SRC + mine] = jnp.where((i >> 5) == me, i & 31, -1)
        return c[0] + jnp.where(delta == 2, 1, 0), c[1] + jnp.where(beside, 1, 0)

    far, side = lax.fori_loop(0, 8 * SL, first, (zero, zero), unroll=4)

    def lens(j, c):
        lens_out[j] = tab[MLEN + j] + 1
        return c

    lax.fori_loop(0, SL, lens, 0, unroll=8)

    def hops(x):
        return (x, (x + 1) & 3, (x + 2) & 3), (4 + x, 4 + ((x - 1) & 3), 4 + ((x + 2) & 3))

    def choose(n, c):
        i = todo[n]
        nb = nbv[i]
        (a1, a2, _), (b1, b2, _) = hops(gray(i >> 6))
        la1, la2, lb1, lb2 = load[a1], load[a2], load[b1], load[b2]
        la, lb = jnp.maximum(la1, la2), jnp.maximum(lb1, lb2)
        cw = (la < lb) | ((la == lb) & (la1 + la2 <= lb1 + lb2))
        x1, x2 = jnp.where(cw, a1, b1), jnp.where(cw, a2, b2)
        load[x1] = load[x1] + nb
        load[x2] = load[x2] + nb
        two[x1] = two[x1] + nb + HALF
        kindv[i] = jnp.where(cw, 2, 5)
        return c

    lax.fori_loop(0, far, choose, 0)

    def detour(n, c):
        i = near[n]
        nb = nbv[i]
        cws, ccws = hops(gray(i >> 6))
        cw = kindv[i] == 1
        a = jnp.where(cw, cws[0], ccws[0])
        b = [jnp.where(cw, y, x) for x, y in zip(cws, ccws)]
        lb = [load[x] for x in b]
        la = load[a]
        top = functools.reduce(jnp.maximum, [load[x] for x in range(8)])

        @pl.when((la - nb >= functools.reduce(jnp.maximum, lb) + nb) & (la * 10 >= top * 9))
        def _():
            load[a] = la - nb
            one[a] = one[a] - nb - HALF
            for x, l in zip(b, lb):
                load[x] = l + nb
            three[b[0]] = three[b[0]] + nb + HALF
            kindv[i] = jnp.where(cw, 6, 3)

        return c

    lax.fori_loop(0, side, detour, 0)

    def again(n, c):
        i = todo[n]
        nb = nbv[i]
        cws, ccws = hops(gray(i >> 6))
        cw = kindv[i] == 2
        a = [jnp.where(cw, x, y) for x, y in zip(cws[:2], ccws)]
        b = [jnp.where(cw, y, x) for x, y in zip(cws[:2], ccws)]
        la, lb = [load[x] for x in a], [load[x] for x in b]

        @pl.when(jnp.maximum(*lb) + nb < jnp.maximum(*la))
        def _():
            for x, l in zip(a + b, [l - nb for l in la] + [l + nb for l in lb]):
                load[x] = l
            two[a[0]] = two[a[0]] - nb - HALF
            two[b[0]] = two[b[0]] + nb + HALF
            kindv[i] = jnp.where(cw, 5, 2)

        return c

    lax.fori_loop(0, far, again, 0)

    def back(d, x, n):
        return 4 * d + ((x + (2 * d - 1) * n) & 3)

    def own_of(d, x):
        x = back(d, x, 0)
        return one[x] + two[x] + three[x]

    def link(d, x, size):
        up, up2 = back(d, x, 1), back(d, x, 2)
        own = own_of(d, x)
        fwd, fwd2 = two[up] + three[up], three[up2]
        start = jnp.maximum(own & LOW, jnp.where(fwd > 0, 2 * size, 0))
        own_up = own_of(d, up & 3)
        start_up = jnp.maximum(own_up & LOW, jnp.where(two[up2] + three[up2] > 0, 2 * size, 0))
        start2 = jnp.maximum(start + (fwd & LOW), jnp.where(fwd2 > 0, start_up + 2 * size, 0))
        return own, fwd, fwd2, start, start_up, start2

    cross = zero
    for d in range(8):
        cross = jnp.maximum(cross, (swap[d] + NX - 1) // NX)
    best, pick, turns, chunk = zero + END, zero, zero, zero
    for o, size in enumerate(SIZES):
        longest = zero
        for d in range(2):
            for x in range(4):
                _, _, fwd2, _, _, start2 = link(d, x, size)
                longest = jnp.maximum(longest, start2 + (fwd2 & LOW))
        trips = (jnp.maximum((longest + size - 1) // size, cross) + TURN - 1) // TURN
        price = trips * (TURN * size + 12)
        better = price < best
        best, pick, turns, chunk = [jnp.where(better, n, o) for n, o in (
            (price, best), (o, pick), (trips * TURN, turns), (size, chunk))]
    tab[ROUNDS] = turns
    tab[PICK] = pick

    x0 = gray(me >> 1)
    left, right, opposite = (x0 - 1) & 3, (x0 + 1) & 3, (x0 + 2) & 3
    shift = []
    for lid, d, x in ((S0, 0, x0), (S1, 1, x0), (R0, 0, left), (R1, 1, right)):
        own, fwd, fwd2, start, _, start2 = link(d, x, chunk)
        here, up = back(d, x, 0), back(d, x, 1)
        base = zero + lid * WIDE
        wide = 2 * (three[here] >> 16)
        pad = base + 2 * (own >> 16)
        pad2 = pad + 2 + 2 * (fwd >> 16)
        tab[pad] = start - (own & LOW)
        tab[pad2] = start2 - start - (fwd & LOW)
        last = pad2 + 2 + 2 * (fwd2 >> 16)
        tab[last] = zero + END
        for a in (pad, pad2, last):
            tab[a + 1] = zero + NONE * HALF
        hop3, hop2 = three[here], two[here]
        segs = ((base, zero), (base + wide, hop3 & LOW), (base + wide + 2 * (hop2 >> 16), (hop3 + hop2) & LOW),
                (pad + 2, start), (pad + 2 + 2 * (three[up] >> 16), start + (three[up] & LOW)), (pad2 + 2, start2))
        for k, (where, pos) in enumerate(segs):
            addr[SEGS * lid + k] = where
            at[SEGS * lid + k] = pos
        shift.append(((hop3 + hop2) & LOW) - start)
    addr[IDLE] = zero + DUMP
    at[IDLE] = zero

    def append(seg, hit, nb, code):
        seg = jnp.where(hit, seg, IDLE)
        a, p = addr[seg], at[seg]
        tab[a] = nb
        tab[a + 1] = code
        addr[seg] = a + jnp.where(hit, 2, 0)
        at[seg] = p + nb
        return p + nb

    def source(s, c):
        i = (me >> 1) * 2 * SL + s
        kind = kindv[i]
        seg = jnp.where(kind > 3, SEGS + 6, 3) - kind
        append(seg, kind > 0, nbv[i], ((s >> 5) << 16) + (s & 31) * BL)
        return c

    lax.fori_loop(0, 2 * SL, source, 0, unroll=4)

    def visit(i, hit, seg, goes_on, seg_on, ahead):
        nb = nbv[i]
        dst = dest_ref[i]
        code = jnp.where(goes_on, FWD * HALF + at[seg] + ahead, (((dst >> 5) & 1) << 16) + (dst & 31) * BL)
        end = append(seg, hit, nb, code)
        append(seg_on, goes_on, nb, code)
        mine = hit & ((dst >> 5) == me) & jnp.logical_not(goes_on)
        tab[RDY + jnp.where(mine, dst & 31, SL)] = end

    for d, x in ((0, left), (1, right)):
        def beside(s, c):
            i = gray(x) * 2 * SL + s
            kind = kindv[i]
            h = kind - 3 * d
            along = (h > 0) & (h <= 3)
            about = kind == 6 - 3 * d
            seg = jnp.where(along, SEGS * (R0 + d) + 3 - h, SEGS * (R1 - d) + 5)
            visit(i, along | about, seg, along & (h > 1), SEGS * d + 6 - h, 0)
            return c

        lax.fori_loop(0, 2 * SL, beside, 0, unroll=2)

    def across(s, c):
        i = gray(opposite) * 2 * SL + s
        kind = kindv[i]
        d = jnp.where(kind > 3, 1, 0)
        h = kind - 3 * d
        seg = SEGS * (R0 + d) + jnp.where(h == 3, 3, 4)
        visit(i, h > 1, seg, h == 3, SEGS * d + 5, jnp.where(d == 0, shift[R0], shift[R1]))
        return c

    lax.fori_loop(0, 2 * SL, across, 0, unroll=2)

    for lid, sender, receiver in ((XS, me, me ^ 1), (XR, me ^ 1, me)):
        def cross_list(s, c):
            a, pos = c
            i = sender * SL + s
            nb = nbv[i]
            dst = dest_ref[i]
            hit = (dst >> 5) == receiver
            tab[a] = nb
            tab[a + 1] = (s if lid == XS else dst & 31) * BL
            pos = pos + jnp.where(hit, nb, 0)
            if lid == XR:
                tab[RDX + jnp.where(hit, dst & 31, SL)] = pos
            return a + jnp.where(hit, 2, 0), pos

        a, _ = lax.fori_loop(0, SL, cross_list, (zero + lid * WIDE, zero), unroll=2)
        tab[a] = zero + END
        tab[a + 1] = zero + NONE * HALF


class Mover:
    def __init__(self, tab, st_in, st, size):
        self.tab, self.st, self.size = tab, st, size
        self.core = tab[CORE]

        def cp(i, _):
            st[i] = st_in[i]
            return 0

        lax.fori_loop(0, STATE, cp, 0)

    def walk(self, lid, use, n, fn):
        tab, st = self.tab, self.st
        base = lid * WIDE

        def body(c):
            p, item, off, cnt = c
            width = tab[base + 2 * item]
            code = tab[base + 2 * item + 1]
            take = jnp.minimum(n - p, width - off)
            cnt = cnt + fn(p, take, code >> 16, (code & LOW) + off)
            off = off + take
            adv = off >= width
            return p + take, jnp.where(adv, item + 1, item), jnp.where(adv, 0, off), cnt

        c0 = (jnp.int32(0), st[2 * use], st[2 * use + 1], jnp.int32(0))
        _, item, off, cnt = lax.while_loop(lambda c: c[0] < n, body, c0)
        st[2 * use] = item
        st[2 * use + 1] = off
        return cnt

    @staticmethod
    def drain(cnt, ref, sem):
        @pl.when(cnt > 0)
        def _():
            part = ref.at[pl.ds(0, cnt)]
            pltpu.make_async_copy(part, part, sem).wait()

    def partial(self, d, kc, vc, buf, sem):
        core = self.core

        def fn(p, take, kind, idx):
            mine = kind == core

            @pl.when(mine & (core == 0))
            def _():
                pltpu.make_async_copy(vc.at[pl.ds(idx, take)], buf.at[d, pl.ds(p, take)], sem).start()

            @pl.when(mine & (core == 1))
            def _():
                pltpu.make_async_copy(kc.at[pl.ds(idx, take)], buf.at[d, pl.ds(p, take)], sem).start()

            return jnp.where(mine, take, 0)

        return self.walk(S0 + d, U_PART + d, self.size, fn)

    def merge(self, d, kc, vc, pre, fwd, buf, sem):
        core = self.core

        def fn(p, take, kind, idx):
            mine = kind == core

            @pl.when(mine & (core == 0))
            def _():
                pltpu.make_async_copy(kc.at[pl.ds(idx, take)], buf.at[d, pl.ds(p, take)], sem).start()

            @pl.when(mine & (core == 1))
            def _():
                pltpu.make_async_copy(vc.at[pl.ds(idx, take)], buf.at[d, pl.ds(p, take)], sem).start()

            @pl.when(kind == 1 - core)
            def _():
                pltpu.make_async_copy(pre.at[d, pl.ds(p, take)], buf.at[d, pl.ds(p, take)], sem).start()

            if fwd is not None:
                @pl.when(kind == FWD)
                def _():
                    pltpu.make_async_copy(fwd.at[pl.ds(idx, take)], buf.at[d, pl.ds(p, take)], sem).start()
            return jnp.where(kind < NONE, take, 0)

        return self.walk(S0 + d, U_MERGE + d, self.size, fn)

    def cross_send(self, kc, vc, buf, sem):
        def fn(p, take, kind, idx):
            @pl.when(kind == 0)
            def _():
                pltpu.make_async_copy(kc.at[pl.ds(idx, take)], buf.at[0, pl.ds(p, take)], sem).start()
                pltpu.make_async_copy(vc.at[pl.ds(idx, take)], buf.at[1, pl.ds(p, take)], sem).start()

            return jnp.where(kind == 0, 2 * take, 0)

        return self.walk(XS, U_XS, NX, fn)

    def cross_recv(self, n, ko, vo, buf, sem):
        def fn(p, take, kind, idx):
            @pl.when(kind == 0)
            def _():
                pltpu.make_async_copy(buf.at[0, pl.ds(p, take)], ko.at[pl.ds(idx, take)], sem).start()
                pltpu.make_async_copy(buf.at[1, pl.ds(p, take)], vo.at[pl.ds(idx, take)], sem).start()

            return jnp.where(kind == 0, 2 * take, 0)

        return self.walk(XR, U_XR, n, fn)

    def unpack(self, d, use, n, flip, ko, vo, fwd, buf, sem):
        core = self.core
        plane = 1 - core if flip else core

        def fn(p, take, kind, idx):
            mine = kind == core

            @pl.when(mine & (plane == 0))
            def _():
                pltpu.make_async_copy(buf.at[d, pl.ds(p, take)], ko.at[pl.ds(idx, take)], sem).start()

            @pl.when(mine & (plane == 1))
            def _():
                pltpu.make_async_copy(buf.at[d, pl.ds(p, take)], vo.at[pl.ds(idx, take)], sem).start()

            cnt = jnp.where(mine, take, 0)
            if fwd is not None:
                @pl.when(kind == FWD)
                def _():
                    pltpu.make_async_copy(buf.at[d, pl.ds(p, take)], fwd.at[pl.ds(idx, take)], sem).start()

                cnt = cnt + jnp.where(kind == FWD, take, 0)
            return cnt

        return self.walk(R0 + d, use + d, n, fn)


def copies(pairs, sems):
    made = [pltpu.make_async_copy(src, dst, sem) for (src, dst), sem in zip(pairs, sems)]
    for c in made:
        c.start()
    return made


def halves(ref):
    return [ref.at[d] for d in range(2)]


def finish(made):
    for c in made:
        c.wait()


def open_kernel(NB, tab, st_in, kc, vc, st, part, vpart, sem):
    mv = Mover(tab, st_in, st, NB)
    mv.drain(sum(mv.partial(d, kc, vc, vpart, sem) for d in range(2)), kc, sem)
    finish(copies([(vpart, part)], [sem]))


def open_more_kernel(NB, tab, st_in, kc, vc, st, part1, part2, dxs, vpart, vdx, *sems):
    mv = Mover(tab, st_in, st, NB)
    cnt = [sum(mv.partial(d, kc, vc, buf, sem) for d in range(2)) for buf, sem in zip(halves(vpart), sems)]
    cnt.append(mv.cross_send(kc, vc, vdx, sems[-1]))
    made = []
    for n, sem, pair in zip(cnt, sems, zip(halves(vpart) + [vdx], (part1, part2, dxs))):
        mv.drain(n, kc, sem)
        made += copies([pair], [sem])
    finish(made)


def open_merge_kernel(NB, tab, st_in, kc, vc, pre, st, send0, send1, vsend, *sems):
    mv = Mover(tab, st_in, st, NB)
    cnt = [mv.merge(d, kc, vc, pre, None, vsend, sem) for d, sem in enumerate(sems)]
    made = []
    for n, sem, pair in zip(cnt, sems, zip(halves(vsend), (send0, send1))):
        mv.drain(n, kc, sem)
        made += copies([pair], [sem])
    finish(made)


def round_kernel(NB, tab, st_in, kc, vc, pre, rc0, rc1, po0, po1, dxr, f0i, f1i, koi, voi,
                 st, send0, send1, part, dxs, f0, f1, ko, vo,
                 vsend, vpart, vrecv, vpost, vdxs, vdxr, *sems):
    mv = Mover(tab, st_in, st, NB)
    part_sem, cross_sem, out_sem, post_sem, *sems = sems
    r = st_in[STEP]
    st[STEP] = r + 1
    ins = copies(zip([rc0, rc1, po0, po1, dxr], halves(vrecv) + halves(vpost) + [vdxr]), sems)
    n1, n2, nx = [jnp.where(r >= back, n, 0) for back, n in ((1, NB), (2, NB), (1, NX))]
    cp = sum(mv.partial(d, kc, vc, vpart, part_sem) for d in range(2))
    cx = mv.cross_send(kc, vc, vdxs, cross_sem)
    fwd = (f0, f1)
    cnt = []
    for d in range(2):
        ins[d].wait()
        cnt.append(mv.unpack(d, U_OWN, n1, False, ko, vo, fwd[d], vrecv, out_sem))
    mv.drain(sum(cnt), kc, out_sem)
    merged = [mv.merge(d, kc, vc, pre, fwd[d], vsend, sem) for d, sem in enumerate(sems[:2])]
    finish(ins[2:])
    cnt = sum(mv.unpack(d, U_POST, n2, True, ko, vo, None, vpost, post_sem) for d in range(2))
    cnt += mv.cross_recv(nx, ko, vo, vdxr, post_sem)
    outs = []
    for n, sem, pair in zip(merged + [cp, cx], sems[:2] + [part_sem, cross_sem],
                            zip(halves(vsend) + [vpart, vdxs], (send0, send1, part, dxs))):
        mv.drain(n, kc, sem)
        outs += copies([pair], [sem])
    mv.drain(cnt, kc, post_sem)
    finish(outs)


def close_kernel(NB, last, tab, st_in, *refs):
    if last:
        (po0, po1, koi, voi, st, ko, vo, vpost, *sems) = refs
        pairs = zip((po0, po1), halves(vpost))
    else:
        (rc0, rc1, po0, po1, dxr, koi, voi, st, ko, vo, vpost, vrecv, vdxr, *sems) = refs
        pairs = zip((po0, po1, rc0, rc1, dxr), halves(vpost) + halves(vrecv) + [vdxr])
    mv = Mover(tab, st_in, st, NB)
    sem = sems[-1]
    r = st_in[STEP]
    st[STEP] = r + 1
    finish(copies(pairs, sems))
    n1, n2, nx = [jnp.where(r >= back, n, 0) for back, n in ((1, NB), (2, NB), (1, NX))]
    cnt = sum(mv.unpack(d, U_POST, n2, True, ko, vo, None, vpost, sem) for d in range(2))
    if not last:
        cnt += sum(mv.unpack(d, U_OWN, n1, False, ko, vo, None, vrecv, sem) for d in range(2))
        cnt += mv.cross_recv(nx, ko, vo, vdxr, sem)
    mv.drain(cnt, ko, sem)


def attn_kernel(NB, batches, tab, st_in, q, kn, vn, kc, vc, koi, voi, aoi, st, ko, vo, ao,
                kb, vb, ob, sel, lsem, wsem, osem):
    def cp(i, _):
        st[i] = st_in[i]
        return 0

    lax.fori_loop(0, STATE, cp, 0)
    link_end = jnp.maximum((st_in[STEP] - 2) * NB, 0)
    swap_end = jnp.maximum((st_in[STEP] - 1) * NX, 0)

    def load(a, j):
        s = tab[SRC + j]

        @pl.when(s >= 0)
        def _():
            pltpu.make_async_copy(kc.at[pl.ds(s * BL, BL)], kb.at[a], lsem.at[a]).start()
            pltpu.make_async_copy(vc.at[pl.ds(s * BL, BL)], vb.at[a], lsem.at[a]).start()

        @pl.when(s < 0)
        def _():
            pltpu.make_async_copy(ko.at[pl.ds(j * BL, BL)], kb.at[a], lsem.at[a]).start()
            pltpu.make_async_copy(vo.at[pl.ds(j * BL, BL)], vb.at[a], lsem.at[a]).start()

    def compute(a, j):
        pltpu.make_async_copy(kb.at[a], kb.at[a], lsem.at[a]).wait()
        pltpu.make_async_copy(vb.at[a], vb.at[a], lsem.at[a]).wait()
        m = tab[MLEN + j]
        s = tab[SRC + j]
        b0 = m >> SHIFT
        row = lax.broadcasted_iota(i32, BLOCK, 0) >> 3
        for buf, new in ((kb, kn), (vb, vn)):
            x = buf[a, b0].astype(f32)
            fresh = jnp.concatenate([new[j].astype(f32)] * BP, axis=0)
            t = b0 * BP + row
            buf[a, b0] = jnp.where(t < m, x, jnp.where(t == m, fresh, 0.0)).astype(bf16)

        def wipe(b, _):
            kb[a, b] = jnp.zeros(BLOCK, bf16)
            vb[a, b] = jnp.zeros(BLOCK, bf16)
            return 0

        lax.fori_loop(b0 + 1, BL, wipe, 0)
        kf = kb[a].reshape(-1, 128)
        vf = vb[a].reshape(-1, 128)
        sc = lax.dot_general(q[j], kf, (((1,), (1,)), ((), ())), preferred_element_type=f32) * (128 ** -0.5)
        col = lax.broadcasted_iota(i32, sc.shape, 1)
        head = lax.broadcasted_iota(i32, sc.shape, 0) // 3
        ok = ((col & 7) == head) & ((col >> 3) <= m)
        sc = jnp.where(ok, sc, -1e30)
        top = jnp.max(sc, axis=1, keepdims=True)
        w = jnp.exp(sc - top)
        tot = jnp.sum(w, axis=1, keepdims=True)
        acc = lax.dot_general(w.astype(bf16), vf, (((1,), (0,)), ((), ())), preferred_element_type=f32)
        ob[a] = (acc / tot).astype(bf16)
        bw = jnp.where(s >= 0, 0, b0)

        tail = pl.ds(bw, BL - bw)
        home = pl.ds(j * BL + bw, BL - bw)
        pltpu.make_async_copy(kb.at[a, tail], ko.at[home], wsem.at[0]).start()
        pltpu.make_async_copy(vb.at[a, tail], vo.at[home], wsem.at[0]).start()
        pltpu.make_async_copy(ob.at[a], ao.at[j], osem.at[0]).start()
        return 2 * (BL - bw)

    def batch(_, c):
        def pick(j, n):
            hit = (st[DONE + j] == 0) & (tab[RDY + j] <= link_end) & (tab[RDX + j] <= swap_end) & (n < A)
            sel[jnp.where(hit, n, A)] = j
            st[DONE + j] = jnp.where(hit, 1, st[DONE + j])
            return n + jnp.where(hit, 1, 0)

        n = lax.fori_loop(0, SL, pick, jnp.int32(0))

        def loads(a, _):
            load(a, sel[a])
            return 0

        lax.fori_loop(0, n, loads, 0)

        def computes(a, cnt):
            return cnt + compute(a, sel[a])

        cnt = lax.fori_loop(0, n, computes, jnp.int32(0))

        @pl.when(n > 0)
        def _():
            done = ko.at[pl.ds(0, cnt)]
            pltpu.make_async_copy(done, done, wsem.at[0]).wait()
            rows = ob.at[pl.ds(0, n)]
            pltpu.make_async_copy(rows, rows, osem.at[0]).wait()

        return c

    lax.fori_loop(0, batches, batch, 0)


SMEM = pl.BlockSpec(memory_space=pltpu.SMEM)
VMEM = pl.BlockSpec(memory_space=pltpu.VMEM)
ANY = pl.BlockSpec(memory_space=pl.ANY)
BLOCK = (8 * BP, 128)


def sds(shape, dtype=bf16):
    return jax.ShapeDtypeStruct(shape, dtype)


def dma(n):
    return pltpu.SemaphoreType.DMA((n,))


def buf(*lead):
    return pltpu.VMEM(lead + BLOCK, bf16)


def cost(us):
    return pl.CostEstimate(flops=us * FLOPS, bytes_accessed=us * FLOPS, transcendentals=0)


ST = sds((STATE,), i32)
DMA = [pltpu.SemaphoreType.DMA]
TAGS = ('ra', 'rb', 'rc', 'rd')


def solution(mesh):
    group = mesh.shape['dp']
    ring = [0, 1, 3, 2]
    cw = [(ring[k] * 2 + c, ring[(k + 1) % 4] * 2 + c) for k in range(4) for c in range(2)]
    ccw = [(b, a) for a, b in cw]
    swap = [(d, d ^ 1) for d in range(group)]

    def local(query, k_cache, v_cache, cache_lens, dest_slot, k_new, v_new):
        kc = k_cache.reshape((SL * BL,) + BLOCK)
        vc = v_cache.reshape((SL * BL,) + BLOCK)
        lens_all = pl.pallas_call(
            lens_kernel, out_shape=sds((8, 1, SL), i32), in_specs=[VMEM], out_specs=VMEM,
            scratch_shapes=[pltpu.SemaphoreType.DMA, dma(8), dma(8)],
            compiler_params=pltpu.CompilerParams(collective_id=0, has_side_effects=True),
            name='lens')(cache_lens.reshape(1, SL))
        me = jnp.full((1,), lax.axis_index('dp'), i32)
        tab, lens_out = pl.pallas_call(
            plan_kernel, out_shape=(sds((TAB,), i32), sds((SL,), i32)), in_specs=[SMEM] * 3, out_specs=(SMEM, SMEM),
            scratch_shapes=[pltpu.SMEM((8 * SL + 1,), i32)] * 4 + [pltpu.SMEM((IDLE + 1,), i32)] * 7,
            name='plan')(me, dest_slot, lens_all)

        def run(NB):
            def nothing(*refs):
                pass

            chunk, both, cross = sds((NB,) + BLOCK), sds((2, NB) + BLOCK), sds((2, NX) + BLOCK)
            cache, store = sds((SL * BL,) + BLOCK), sds((4 * SL * BL,) + BLOCK)
            ko, vo, ao, f0, f1, rc0, rc1, po0, po1, dxr = pl.pallas_call(
                nothing, out_shape=(cache, cache, sds((SL, 24, 128)), store, store, chunk, chunk, chunk, chunk, cross),
                out_specs=(ANY,) * 10, name='blank')()

            st = jnp.zeros((STATE,), i32)
            caches = [SMEM, SMEM, ANY, ANY]
            st, part = pl.pallas_call(
                functools.partial(open_kernel, NB), out_shape=(ST, both), in_specs=caches, out_specs=(SMEM, ANY),
                scratch_shapes=[buf(2, NB)] + DMA, name='open')(tab, st, kc, vc)
            pre = lax.ppermute(part, 'dp', swap)
            st, part1, part, dxs = pl.pallas_call(
                functools.partial(open_more_kernel, NB), out_shape=(ST, both, both, cross), in_specs=caches,
                out_specs=(SMEM,) + (ANY,) * 3, scratch_shapes=[buf(2, 2, NB), buf(2, NX)] + DMA * 3,
                name='open_more')(tab, st, kc, vc)
            pre1 = lax.ppermute(part1, 'dp', swap)
            st, s0, s1 = pl.pallas_call(
                functools.partial(open_merge_kernel, NB), out_shape=(ST, chunk, chunk), in_specs=caches + [VMEM],
                out_specs=(SMEM, ANY, ANY), scratch_shapes=[buf(2, NB)] + DMA * 2,
                name='open_merge')(tab, st, kc, vc, pre)
            pre = pre1

            def attend(st, ko, vo, ao, batches):
                return pl.pallas_call(
                    functools.partial(attn_kernel, NB, batches),
                    out_shape=(ST, cache, cache, sds((SL, 24, 128))),
                    in_specs=[SMEM, SMEM, VMEM, VMEM, VMEM, ANY, ANY, ANY, ANY, ANY], out_specs=(SMEM, ANY, ANY, ANY),
                    input_output_aliases={7: 1, 8: 2, 9: 3},
                    scratch_shapes=[buf(A, BL), buf(A, BL), pltpu.VMEM((A, 24, 128), bf16), pltpu.SMEM((A + 1,), i32),
                                    dma(A), dma(1), dma(1)],
                    cost_estimate=cost(6), name='attend')(tab, st, query, k_new, v_new, kc, vc, ko, vo, ao)

            def one_round(tag, c):
                st, s0, s1, part, dxs, pre, rc0, rc1, po0, po1, dxr, f0, f1, ko, vo, ao = c
                nrc0 = lax.ppermute(s0, 'dp', cw)
                nrc1 = lax.ppermute(s1, 'dp', ccw)
                npre = lax.ppermute(part, 'dp', swap)
                npo0 = lax.ppermute(rc0, 'dp', swap)
                npo1 = lax.ppermute(rc1, 'dp', swap)
                ndxr = lax.ppermute(dxs, 'dp', swap)
                st, s0, s1, part, dxs, f0, f1, ko, vo = pl.pallas_call(
                    functools.partial(round_kernel, NB), out_shape=(ST, chunk, chunk, both, cross, store, store, cache, cache),
                    in_specs=caches + [VMEM] + [ANY] * 9, out_specs=(SMEM,) + (ANY,) * 8,
                    input_output_aliases={10: 5, 11: 6, 12: 7, 13: 8},
                    scratch_shapes=[buf(2, NB)] * 4 + [buf(2, NX)] * 2 + DMA * 9,
                    cost_estimate=cost(10), name='round')(tab, st, kc, vc, pre, rc0, rc1, po0, po1, dxr, f0, f1, ko, vo)
                st, ko, vo, ao = attend(st, ko, vo, ao, 1)
                if tag != TAGS[-1]:
                    s0, s1, npo0, npo1 = lax.optimization_barrier((s0, s1, npo0, npo1))
                return st, s0, s1, part, dxs, npre, nrc0, nrc1, npo0, npo1, ndxr, f0, f1, ko, vo, ao

            rounds = tab[ROUNDS]

            def body(c):
                return (c[0] + TURN,) + functools.reduce(lambda c, tag: one_round(tag, c), TAGS, c[1:])

            c = lax.while_loop(lambda c: c[0] < rounds, body,
                           (jnp.int32(0), st, s0, s1, part, dxs, pre, rc0, rc1, po0, po1, dxr, f0, f1, ko, vo, ao))
            _, st, _, _, _, _, _, rc0, rc1, po0, po1, dxr, _, _, ko, vo, ao = c

            def close(last, st, ko, vo, *ins):
                n = len(ins)
                extra = [] if last else [buf(2, NB), buf(2, NX)]
                return pl.pallas_call(
                    functools.partial(close_kernel, NB, last), out_shape=(ST, cache, cache),
                    in_specs=[SMEM, SMEM] + [VMEM if last else ANY] * n + [ANY] * 2, out_specs=(SMEM, ANY, ANY),
                    input_output_aliases={n + 2: 1, n + 3: 2},
                    scratch_shapes=[buf(2, NB)] + extra + DMA * 6,
                    name='close_last' if last else 'close')(tab, st, *ins, ko, vo)

            lpo0 = lax.ppermute(rc0, 'dp', swap)
            lpo1 = lax.ppermute(rc1, 'dp', swap)
            st, ko, vo = close(False, st, ko, vo, rc0, rc1, po0, po1, dxr)
            st, ko, vo = close(True, st, ko, vo, lpo0, lpo1)
            st, ko, vo, ao = attend(st, ko, vo, ao, SL // A)
            return ao, ko, vo

        ao, ko, vo = lax.switch(tab[PICK], [functools.partial(run, size) for size in SIZES])
        return ao, ko.reshape(k_cache.shape), vo.reshape(v_cache.shape), lens_out

    row_spec = P('dp')
    return jax.shard_map(local, mesh=mesh, in_specs=(row_spec, row_spec, row_spec, row_spec, P(), row_spec, row_spec),
                         out_specs=(row_spec, row_spec, row_spec, row_spec), check_vma=False)
```

```python
import functools

import jax
import jax.numpy as jnp
from jax import lax
from jax.experimental import pallas as pl
from jax.experimental.pallas import tpu as pltpu
from jax.sharding import PartitionSpec as P


BP, SHIFT = 8, 3
SIZES = (66, 60, 54, 48)
NX = 32
A = 4
SL = 32
BL = 64
WIDE = 400
S0, S1, R0, R1, XS, XR, FREE = range(7)
RDY, RDX, MLEN, SRC, ROUNDS = range(FREE * WIDE, FREE * WIDE + 200, 40)
CORE, PICK, SHARE, DUMP = range(ROUNDS + 1, ROUNDS + 5)
TAB = ROUNDS + 8
FWD, NONE = 2, 3
TURN = 4
SEGS = 6
IDLE = 4 * SEGS
HALF = 1 << 16
FLOPS = 4000000
LOW = HALF - 1
U_PART, U_MERGE, U_OWN, U_POST, U_XS, U_XR = 0, 2, 4, 6, 8, 9
STEP, DONE, STATE = 24, 32, 64
END = HALF * HALF // 4
bf16 = jnp.bfloat16
f32 = jnp.float32
i32 = jnp.int32


def gray(c):
    return c ^ (c >> 1)


def lens_kernel(x, o, bsem, ssem, rsem):
    me = lax.axis_index('dp')
    barrier = pltpu.get_barrier_semaphore()
    for k in range(1, 8):
        pl.semaphore_signal(barrier, inc=1, device_id=(lax.rem(me + k, 8),), device_id_type=pl.DeviceIdType.MESH)
    pl.semaphore_wait(barrier, 7)
    here = pltpu.make_async_copy(x, o.at[me], bsem)
    here.start()
    sends = []
    for k in range(1, 8):
        c = pltpu.make_async_remote_copy(src_ref=x, dst_ref=o.at[me], send_sem=ssem.at[k], recv_sem=rsem.at[k],
                                         device_id=(lax.rem(me + k, 8),), device_id_type=pl.DeviceIdType.MESH)
        c.start()
        sends.append(c)
    here.wait()
    for c in sends:
        c.wait()


def plan_kernel(me_ref, dest_ref, len_ref, tab, lens_out, nbv, kindv, todo, near, load, one, two, three, swap, addr, at):
    me = me_ref[0]
    zero = me - me
    for i in range(9):
        for ref in (load, one, two, three, swap):
            ref[i] = zero
    tab[CORE] = me & 1
    for j in range(SL):
        tab[RDY + j] = zero
        tab[RDX + j] = zero

    def first(i, c):
        size = len_ref[i >> 5, 0, i & 31]
        d = dest_ref[i]
        nb = (size + (BP - 1)) >> SHIFT
        ra = gray(i >> 6)
        delta = (gray(d >> 6) - ra) & 3
        nbv[i] = nb
        beside = (delta & 1) == 1
        ccw = delta == 3
        kindv[i] = jnp.where(beside, jnp.where(ccw, 4, 1), 0)
        slot = jnp.where(beside, jnp.where(ccw, 4, 0) + ra, 8)
        one[slot] = one[slot] + nb + HALF
        load[slot] = load[slot] + nb
        todo[c[0]] = i
        near[c[1]] = i
        cross = (delta == 0) & ((i >> 5) != (d >> 5))
        xslot = jnp.where(cross, i >> 5, 8)
        swap[xslot] = swap[xslot] + nb
        mine = jnp.where((d >> 5) == me, d & 31, SL)
        tab[MLEN + mine] = size
        tab[SRC + mine] = jnp.where((i >> 5) == me, i & 31, -1)
        return c[0] + jnp.where(delta == 2, 1, 0), c[1] + jnp.where(beside, 1, 0)

    far, side = lax.fori_loop(0, 8 * SL, first, (zero, zero), unroll=4)

    def lens(j, c):
        lens_out[j] = tab[MLEN + j] + 1
        return c

    lax.fori_loop(0, SL, lens, 0, unroll=8)

    def hops(x):
        return (x, (x + 1) & 3, (x + 2) & 3), (4 + x, 4 + ((x - 1) & 3), 4 + ((x + 2) & 3))

    def choose(n, c):
        i = todo[n]
        nb = nbv[i]
        (a1, a2, _), (b1, b2, _) = hops(gray(i >> 6))
        la1, la2, lb1, lb2 = load[a1], load[a2], load[b1], load[b2]
        la, lb = jnp.maximum(la1, la2), jnp.maximum(lb1, lb2)
        cw = (la < lb) | ((la == lb) & (la1 + la2 <= lb1 + lb2))
        x1, x2 = jnp.where(cw, a1, b1), jnp.where(cw, a2, b2)
        load[x1] = load[x1] + nb
        load[x2] = load[x2] + nb
        two[x1] = two[x1] + nb + HALF
        kindv[i] = jnp.where(cw, 2, 5)
        return c

    lax.fori_loop(0, far, choose, 0)

    def detour(n, c):
        i = near[n]
        nb = nbv[i]
        cws, ccws = hops(gray(i >> 6))
        cw = kindv[i] == 1
        a = jnp.where(cw, cws[0], ccws[0])
        b = [jnp.where(cw, y, x) for x, y in zip(cws, ccws)]
        lb = [load[x] for x in b]
        la = load[a]
        top = functools.reduce(jnp.maximum, [load[x] for x in range(8)])

        @pl.when((la - nb >= functools.reduce(jnp.maximum, lb) + nb) & (la * 10 >= top * 9))
        def _():
            load[a] = la - nb
            one[a] = one[a] - nb - HALF
            for x, l in zip(b, lb):
                load[x] = l + nb
            three[b[0]] = three[b[0]] + nb + HALF
            kindv[i] = jnp.where(cw, 6, 3)

        return c

    lax.fori_loop(0, side, detour, 0)

    def again(n, c):
        i = todo[n]
        nb = nbv[i]
        cws, ccws = hops(gray(i >> 6))
        cw = kindv[i] == 2
        a = [jnp.where(cw, x, y) for x, y in zip(cws[:2], ccws)]
        b = [jnp.where(cw, y, x) for x, y in zip(cws[:2], ccws)]
        la, lb = [load[x] for x in a], [load[x] for x in b]

        @pl.when(jnp.maximum(*lb) + nb < jnp.maximum(*la))
        def _():
            for x, l in zip(a + b, [l - nb for l in la] + [l + nb for l in lb]):
                load[x] = l
            two[a[0]] = two[a[0]] - nb - HALF
            two[b[0]] = two[b[0]] + nb + HALF
            kindv[i] = jnp.where(cw, 5, 2)

        return c

    lax.fori_loop(0, far, again, 0)

    def back(d, x, n):
        return 4 * d + ((x + (2 * d - 1) * n) & 3)

    def own_of(d, x):
        x = back(d, x, 0)
        return one[x] + two[x] + three[x]

    def link(d, x, size):
        up, up2 = back(d, x, 1), back(d, x, 2)
        own = own_of(d, x)
        fwd, fwd2 = two[up] + three[up], three[up2]
        start = jnp.maximum(own & LOW, jnp.where(fwd > 0, 2 * size, 0))
        own_up = own_of(d, up & 3)
        start_up = jnp.maximum(own_up & LOW, jnp.where(two[up2] + three[up2] > 0, 2 * size, 0))
        start2 = jnp.maximum(start + (fwd & LOW), jnp.where(fwd2 > 0, start_up + 2 * size, 0))
        return own, fwd, fwd2, start, start_up, start2

    cross = zero
    for d in range(8):
        cross = jnp.maximum(cross, (swap[d] + NX - 1) // NX)
    best, pick, turns, chunk = zero + END, zero, zero, zero
    for o, size in enumerate(SIZES):
        longest = zero
        for d in range(2):
            for x in range(4):
                _, _, fwd2, _, _, start2 = link(d, x, size)
                longest = jnp.maximum(longest, start2 + (fwd2 & LOW))
        trips = (jnp.maximum((longest + size - 1) // size, cross) + TURN - 1) // TURN
        price = trips * (TURN * size + 12)
        better = price < best
        best, pick, turns, chunk = [jnp.where(better, n, o) for n, o in (
            (price, best), (o, pick), (trips * TURN, turns), (size, chunk))]
    tab[ROUNDS] = turns
    tab[PICK] = pick
    tab[SHARE] = jnp.minimum(SL // jnp.maximum(turns - TURN, 1) + 1, A)

    x0 = gray(me >> 1)
    left, right, opposite = (x0 - 1) & 3, (x0 + 1) & 3, (x0 + 2) & 3
    shift = []
    for lid, d, x in ((S0, 0, x0), (S1, 1, x0), (R0, 0, left), (R1, 1, right)):
        own, fwd, fwd2, start, _, start2 = link(d, x, chunk)
        here, up = back(d, x, 0), back(d, x, 1)
        base = zero + lid * WIDE
        wide = 2 * (three[here] >> 16)
        pad = base + 2 * (own >> 16)
        pad2 = pad + 2 + 2 * (fwd >> 16)
        tab[pad] = start - (own & LOW)
        tab[pad2] = start2 - start - (fwd & LOW)
        last = pad2 + 2 + 2 * (fwd2 >> 16)
        tab[last] = zero + END
        for a in (pad, pad2, last):
            tab[a + 1] = zero + NONE * HALF
        hop3, hop2 = three[here], two[here]
        segs = ((base, zero), (base + wide, hop3 & LOW), (base + wide + 2 * (hop2 >> 16), (hop3 + hop2) & LOW),
                (pad + 2, start), (pad + 2 + 2 * (three[up] >> 16), start + (three[up] & LOW)), (pad2 + 2, start2))
        for k, (where, pos) in enumerate(segs):
            addr[SEGS * lid + k] = where
            at[SEGS * lid + k] = pos
        shift.append(((hop3 + hop2) & LOW) - start)
    addr[IDLE] = zero + DUMP
    at[IDLE] = zero

    def append(seg, hit, nb, code):
        seg = jnp.where(hit, seg, IDLE)
        a, p = addr[seg], at[seg]
        tab[a] = nb
        tab[a + 1] = code
        addr[seg] = a + jnp.where(hit, 2, 0)
        at[seg] = p + nb
        return p + nb

    def source(s, c):
        i = (me >> 1) * 2 * SL + s
        kind = kindv[i]
        seg = jnp.where(kind > 3, SEGS + 6, 3) - kind
        append(seg, kind > 0, nbv[i], ((s >> 5) << 16) + (s & 31) * BL)
        return c

    lax.fori_loop(0, 2 * SL, source, 0, unroll=4)

    def visit(i, hit, seg, goes_on, seg_on, ahead):
        nb = nbv[i]
        dst = dest_ref[i]
        code = jnp.where(goes_on, FWD * HALF + at[seg] + ahead, (((dst >> 5) & 1) << 16) + (dst & 31) * BL)
        end = append(seg, hit, nb, code)
        append(seg_on, goes_on, nb, code)
        mine = hit & ((dst >> 5) == me) & jnp.logical_not(goes_on)
        tab[RDY + jnp.where(mine, dst & 31, SL)] = end

    for d, x in ((0, left), (1, right)):
        def beside(s, c):
            i = gray(x) * 2 * SL + s
            kind = kindv[i]
            h = kind - 3 * d
            along = (h > 0) & (h <= 3)
            about = kind == 6 - 3 * d
            seg = jnp.where(along, SEGS * (R0 + d) + 3 - h, SEGS * (R1 - d) + 5)
            visit(i, along | about, seg, along & (h > 1), SEGS * d + 6 - h, 0)
            return c

        lax.fori_loop(0, 2 * SL, beside, 0, unroll=2)

    def across(s, c):
        i = gray(opposite) * 2 * SL + s
        kind = kindv[i]
        d = jnp.where(kind > 3, 1, 0)
        h = kind - 3 * d
        seg = SEGS * (R0 + d) + jnp.where(h == 3, 3, 4)
        visit(i, h > 1, seg, h == 3, SEGS * d + 5, jnp.where(d == 0, shift[R0], shift[R1]))
        return c

    lax.fori_loop(0, 2 * SL, across, 0, unroll=2)

    for lid, sender, receiver in ((XS, me, me ^ 1), (XR, me ^ 1, me)):
        def cross_list(s, c):
            a, pos = c
            i = sender * SL + s
            nb = nbv[i]
            dst = dest_ref[i]
            hit = (dst >> 5) == receiver
            tab[a] = nb
            tab[a + 1] = (s if lid == XS else dst & 31) * BL
            pos = pos + jnp.where(hit, nb, 0)
            if lid == XR:
                tab[RDX + jnp.where(hit, dst & 31, SL)] = pos
            return a + jnp.where(hit, 2, 0), pos

        a, _ = lax.fori_loop(0, SL, cross_list, (zero + lid * WIDE, zero), unroll=2)
        tab[a] = zero + END
        tab[a + 1] = zero + NONE * HALF


class Mover:
    def __init__(self, tab, st_in, st, size):
        self.tab, self.st, self.size = tab, st, size
        self.core = tab[CORE]

        def cp(i, _):
            st[i] = st_in[i]
            return 0

        lax.fori_loop(0, STATE, cp, 0)

    def walk(self, lid, use, n, fn):
        tab, st = self.tab, self.st
        base = lid * WIDE

        def body(c):
            p, item, off, cnt = c
            width = tab[base + 2 * item]
            code = tab[base + 2 * item + 1]
            take = jnp.minimum(n - p, width - off)
            cnt = cnt + fn(p, take, code >> 16, (code & LOW) + off)
            off = off + take
            adv = off >= width
            return p + take, jnp.where(adv, item + 1, item), jnp.where(adv, 0, off), cnt

        c0 = (jnp.int32(0), st[2 * use], st[2 * use + 1], jnp.int32(0))
        _, item, off, cnt = lax.while_loop(lambda c: c[0] < n, body, c0)
        st[2 * use] = item
        st[2 * use + 1] = off
        return cnt

    @staticmethod
    def drain(cnt, ref, sem):
        @pl.when(cnt > 0)
        def _():
            part = ref.at[pl.ds(0, cnt)]
            pltpu.make_async_copy(part, part, sem).wait()

    def partial(self, d, kc, vc, buf, sem):
        core = self.core

        def fn(p, take, kind, idx):
            mine = kind == core

            @pl.when(mine & (core == 0))
            def _():
                pltpu.make_async_copy(vc.at[pl.ds(idx, take)], buf.at[pl.ds(p, take)], sem).start()

            @pl.when(mine & (core == 1))
            def _():
                pltpu.make_async_copy(kc.at[pl.ds(idx, take)], buf.at[pl.ds(p, take)], sem).start()

            return jnp.where(mine, take, 0)

        return self.walk(S0 + d, U_PART + d, self.size, fn)

    def merge(self, d, kc, vc, pre, fwd, buf, sem):
        core = self.core

        def fn(p, take, kind, idx):
            mine = kind == core

            @pl.when(mine & (core == 0))
            def _():
                pltpu.make_async_copy(kc.at[pl.ds(idx, take)], buf.at[pl.ds(p, take)], sem).start()

            @pl.when(mine & (core == 1))
            def _():
                pltpu.make_async_copy(vc.at[pl.ds(idx, take)], buf.at[pl.ds(p, take)], sem).start()

            @pl.when(kind == 1 - core)
            def _():
                pltpu.make_async_copy(pre.at[d, pl.ds(p, take)], buf.at[pl.ds(p, take)], sem).start()

            if fwd is not None:
                @pl.when(kind == FWD)
                def _():
                    pltpu.make_async_copy(fwd.at[pl.ds(idx, take)], buf.at[pl.ds(p, take)], sem).start()
            return jnp.where(kind < NONE, take, 0)

        return self.walk(S0 + d, U_MERGE + d, self.size, fn)

    def cross_send(self, kc, vc, buf, sem):
        def fn(p, take, kind, idx):
            @pl.when(kind == 0)
            def _():
                pltpu.make_async_copy(kc.at[pl.ds(idx, take)], buf.at[0, pl.ds(p, take)], sem).start()
                pltpu.make_async_copy(vc.at[pl.ds(idx, take)], buf.at[1, pl.ds(p, take)], sem).start()

            return jnp.where(kind == 0, 2 * take, 0)

        return self.walk(XS, U_XS, NX, fn)

    def cross_recv(self, n, ko, vo, buf, sem):
        def fn(p, take, kind, idx):
            @pl.when(kind == 0)
            def _():
                pltpu.make_async_copy(buf.at[0, pl.ds(p, take)], ko.at[pl.ds(idx, take)], sem).start()
                pltpu.make_async_copy(buf.at[1, pl.ds(p, take)], vo.at[pl.ds(idx, take)], sem).start()

            return jnp.where(kind == 0, 2 * take, 0)

        return self.walk(XR, U_XR, n, fn)

    def unpack(self, d, use, n, flip, ko, vo, fwd, buf, sem):
        core = self.core
        plane = 1 - core if flip else core

        def fn(p, take, kind, idx):
            mine = kind == core

            @pl.when(mine & (plane == 0))
            def _():
                pltpu.make_async_copy(buf.at[pl.ds(p, take)], ko.at[pl.ds(idx, take)], sem).start()

            @pl.when(mine & (plane == 1))
            def _():
                pltpu.make_async_copy(buf.at[pl.ds(p, take)], vo.at[pl.ds(idx, take)], sem).start()

            cnt = jnp.where(mine, take, 0)
            if fwd is not None:
                @pl.when(kind == FWD)
                def _():
                    pltpu.make_async_copy(buf.at[pl.ds(p, take)], fwd.at[pl.ds(idx, take)], sem).start()

                cnt = cnt + jnp.where(kind == FWD, take, 0)
            return cnt

        return self.walk(R0 + d, use + d, n, fn)


def open_kernel(NB, tab, st_in, kc, vc, st, part, sem):
    mv = Mover(tab, st_in, st, NB)
    mv.drain(sum(mv.partial(d, kc, vc, part.at[d], sem) for d in range(2)), kc, sem)


def open_more_kernel(NB, tab, st_in, kc, vc, st, part1, part2, dxs, sem):
    mv = Mover(tab, st_in, st, NB)
    cnt = sum(mv.partial(d, kc, vc, part.at[d], sem) for part in (part1, part2) for d in range(2))
    mv.drain(cnt + mv.cross_send(kc, vc, dxs, sem), kc, sem)


def open_merge_kernel(NB, tab, st_in, kc, vc, pre, st, send0, send1, sem):
    mv = Mover(tab, st_in, st, NB)
    mv.drain(sum(mv.merge(d, kc, vc, pre, None, buf, sem) for d, buf in enumerate((send0, send1))), kc, sem)


def stages(r, NB):
    return [jnp.where(r >= back, n, 0) for back, n in ((1, NB), (2, NB), (1, NX))]


def round_kernel(NB, tab, st_in, kc, vc, pre, rc0, rc1, po0, po1, dxr, f0i, f1i, koi, voi,
                 st, send0, send1, part, dxs, f0, f1, ko, vo, in_sem, out_sem, post_sem):
    mv = Mover(tab, st_in, st, NB)
    r = st_in[STEP]
    st[STEP] = r + 1
    n1, n2, nx = stages(r, NB)
    links = ((0, rc0, po0, f0, send0), (1, rc1, po1, f1, send1))
    mv.drain(sum(mv.unpack(d, U_OWN, n1, False, ko, vo, fwd, rc, out_sem) for d, rc, _, fwd, _ in links), kc, out_sem)
    cnt = sum(mv.merge(d, kc, vc, pre, fwd, send, in_sem) for d, _, _, fwd, send in links)
    late = sum(mv.unpack(d, U_POST, n2, True, ko, vo, None, po, post_sem) for d, _, po, _, _ in links)
    cnt += sum(mv.partial(d, kc, vc, part.at[d], in_sem) for d in range(2)) + mv.cross_send(kc, vc, dxs, in_sem)
    late += mv.cross_recv(nx, ko, vo, dxr, post_sem)
    mv.drain(cnt, kc, in_sem)
    mv.drain(late, kc, post_sem)


def close_kernel(NB, last, tab, st_in, *refs):
    if last:
        (po0, po1, koi, voi, st, ko, vo, sem) = refs
    else:
        (rc0, rc1, po0, po1, dxr, koi, voi, st, ko, vo, sem) = refs
    mv = Mover(tab, st_in, st, NB)
    r = st_in[STEP]
    st[STEP] = r + 1
    n1, n2, nx = stages(r, NB)
    cnt = sum(mv.unpack(d, U_POST, n2, True, ko, vo, None, po, sem) for d, po in enumerate((po0, po1)))
    if not last:
        cnt += sum(mv.unpack(d, U_OWN, n1, False, ko, vo, None, rc, sem) for d, rc in enumerate((rc0, rc1)))
        cnt += mv.cross_recv(nx, ko, vo, dxr, sem)
    mv.drain(cnt, ko, sem)


def attn_kernel(NB, batches, tab, st_in, q, kn, vn, kc, vc, koi, voi, aoi, st, ko, vo, ao,
                kb, vb, ob, sel, lsem, wsem, osem):
    def cp(i, _):
        st[i] = st_in[i]
        return 0

    lax.fori_loop(0, STATE, cp, 0)
    link_end = jnp.maximum((st_in[STEP] - 2) * NB, 0)
    swap_end = jnp.maximum((st_in[STEP] - 1) * NX, 0)

    def load(a, j):
        s = tab[SRC + j]

        @pl.when(s >= 0)
        def _():
            pltpu.make_async_copy(kc.at[pl.ds(s * BL, BL)], kb.at[a], lsem.at[a]).start()
            pltpu.make_async_copy(vc.at[pl.ds(s * BL, BL)], vb.at[a], lsem.at[a]).start()

        @pl.when(s < 0)
        def _():
            pltpu.make_async_copy(ko.at[pl.ds(j * BL, BL)], kb.at[a], lsem.at[a]).start()
            pltpu.make_async_copy(vo.at[pl.ds(j * BL, BL)], vb.at[a], lsem.at[a]).start()

    def compute(a, j):
        pltpu.make_async_copy(kb.at[a], kb.at[a], lsem.at[a]).wait()
        pltpu.make_async_copy(vb.at[a], vb.at[a], lsem.at[a]).wait()
        m = tab[MLEN + j]
        s = tab[SRC + j]
        b0 = m >> SHIFT
        row = lax.broadcasted_iota(i32, BLOCK, 0) >> 3
        for buf, new in ((kb, kn), (vb, vn)):
            x = buf[a, b0].astype(f32)
            fresh = jnp.concatenate([new[j].astype(f32)] * BP, axis=0)
            t = b0 * BP + row
            buf[a, b0] = jnp.where(t < m, x, jnp.where(t == m, fresh, 0.0)).astype(bf16)

        def wipe(b, _):
            kb[a, b] = jnp.zeros(BLOCK, bf16)
            vb[a, b] = jnp.zeros(BLOCK, bf16)
            return 0

        lax.fori_loop(b0 + 1, BL, wipe, 0)
        kf = kb[a].reshape(-1, 128)
        vf = vb[a].reshape(-1, 128)
        sc = lax.dot_general(q[j], kf, (((1,), (1,)), ((), ())), preferred_element_type=f32) * (128 ** -0.5)
        col = lax.broadcasted_iota(i32, sc.shape, 1)
        head = lax.broadcasted_iota(i32, sc.shape, 0) // 3
        ok = ((col & 7) == head) & ((col >> 3) <= m)
        sc = jnp.where(ok, sc, -1e30)
        top = jnp.max(sc, axis=1, keepdims=True)
        w = jnp.exp(sc - top)
        tot = jnp.sum(w, axis=1, keepdims=True)
        acc = lax.dot_general(w.astype(bf16), vf, (((1,), (0,)), ((), ())), preferred_element_type=f32)
        ob[a] = (acc / tot).astype(bf16)
        bw = jnp.where(s >= 0, 0, b0)

        tail = pl.ds(bw, BL - bw)
        home = pl.ds(j * BL + bw, BL - bw)
        pltpu.make_async_copy(kb.at[a, tail], ko.at[home], wsem.at[0]).start()
        pltpu.make_async_copy(vb.at[a, tail], vo.at[home], wsem.at[0]).start()
        pltpu.make_async_copy(ob.at[a], ao.at[j], osem.at[0]).start()
        return 2 * (BL - bw)

    share = tab[SHARE] if batches == 1 else A

    def batch(_, c):
        def pick(j, n):
            hit = (st[DONE + j] == 0) & (tab[RDY + j] <= link_end) & (tab[RDX + j] <= swap_end) & (n < share)
            sel[jnp.where(hit, n, A)] = j
            st[DONE + j] = jnp.where(hit, 1, st[DONE + j])
            return n + jnp.where(hit, 1, 0)

        n = lax.fori_loop(0, SL, pick, jnp.int32(0))

        def loads(a, _):
            load(a, sel[a])
            return 0

        lax.fori_loop(0, n, loads, 0)

        def computes(a, cnt):
            return cnt + compute(a, sel[a])

        cnt = lax.fori_loop(0, n, computes, jnp.int32(0))

        @pl.when(n > 0)
        def _():
            done = ko.at[pl.ds(0, cnt)]
            pltpu.make_async_copy(done, done, wsem.at[0]).wait()
            rows = ob.at[pl.ds(0, n)]
            pltpu.make_async_copy(rows, rows, osem.at[0]).wait()

        return c

    lax.fori_loop(0, batches, batch, 0)


SMEM = pl.BlockSpec(memory_space=pltpu.SMEM)
VMEM = pl.BlockSpec(memory_space=pltpu.VMEM)
ANY = pl.BlockSpec(memory_space=pl.ANY)
BLOCK = (8 * BP, 128)


def sds(shape, dtype=bf16):
    return jax.ShapeDtypeStruct(shape, dtype)


def dma(n):
    return pltpu.SemaphoreType.DMA((n,))


def buf(*lead):
    return pltpu.VMEM(lead + BLOCK, bf16)


def cost(us):
    return pl.CostEstimate(flops=us * FLOPS, bytes_accessed=us * FLOPS, transcendentals=0)


ST = sds((STATE,), i32)
DMA = [pltpu.SemaphoreType.DMA]
TAGS = ('ra', 'rb', 'rc', 'rd')


def solution(mesh):
    group = mesh.shape['dp']
    ring = [0, 1, 3, 2]
    cw = [(ring[k] * 2 + c, ring[(k + 1) % 4] * 2 + c) for k in range(4) for c in range(2)]
    ccw = [(b, a) for a, b in cw]
    swap = [(d, d ^ 1) for d in range(group)]

    def local(query, k_cache, v_cache, cache_lens, dest_slot, k_new, v_new):
        kc = k_cache.reshape((SL * BL,) + BLOCK)
        vc = v_cache.reshape((SL * BL,) + BLOCK)
        lens_all = pl.pallas_call(
            lens_kernel, out_shape=sds((8, 1, SL), i32), in_specs=[VMEM], out_specs=VMEM,
            scratch_shapes=[pltpu.SemaphoreType.DMA, dma(8), dma(8)],
            compiler_params=pltpu.CompilerParams(collective_id=0, has_side_effects=True),
            name='lens')(cache_lens.reshape(1, SL))
        me = jnp.full((1,), lax.axis_index('dp'), i32)
        tab, lens_out = pl.pallas_call(
            plan_kernel, out_shape=(sds((TAB,), i32), sds((SL,), i32)), in_specs=[SMEM] * 3, out_specs=(SMEM, SMEM),
            scratch_shapes=[pltpu.SMEM((8 * SL + 1,), i32)] * 4 + [pltpu.SMEM((IDLE + 1,), i32)] * 7,
            name='plan')(me, dest_slot, lens_all)

        def run(NB):
            def nothing(*refs):
                pass

            chunk, both, cross = sds((NB,) + BLOCK), sds((2, NB) + BLOCK), sds((2, NX) + BLOCK)
            cache, store = sds((SL * BL,) + BLOCK), sds((4 * SL * BL,) + BLOCK)
            ko, vo, ao, f0, f1, rc0, rc1, po0, po1, dxr = pl.pallas_call(
                nothing, out_shape=(cache, cache, sds((SL, 24, 128)), store, store, chunk, chunk, chunk, chunk, cross),
                out_specs=(ANY,) * 10, name='blank')()

            st = jnp.zeros((STATE,), i32)
            caches = [SMEM, SMEM, ANY, ANY]
            st, part = pl.pallas_call(
                functools.partial(open_kernel, NB), out_shape=(ST, both), in_specs=caches, out_specs=(SMEM, VMEM),
                scratch_shapes=DMA, name='open')(tab, st, kc, vc)
            pre = lax.ppermute(part, 'dp', swap)
            st, part1, part, dxs = pl.pallas_call(
                functools.partial(open_more_kernel, NB), out_shape=(ST, both, both, cross), in_specs=caches,
                out_specs=(SMEM,) + (VMEM,) * 3, scratch_shapes=DMA,
                name='open_more')(tab, st, kc, vc)
            pre1 = lax.ppermute(part1, 'dp', swap)
            st, s0, s1 = pl.pallas_call(
                functools.partial(open_merge_kernel, NB), out_shape=(ST, chunk, chunk), in_specs=caches + [VMEM],
                out_specs=(SMEM, VMEM, VMEM), scratch_shapes=DMA,
                name='open_merge')(tab, st, kc, vc, pre)
            pre = pre1

            def attend(st, ko, vo, ao, batches):
                return pl.pallas_call(
                    functools.partial(attn_kernel, NB, batches),
                    out_shape=(ST, cache, cache, sds((SL, 24, 128))),
                    in_specs=[SMEM, SMEM, VMEM, VMEM, VMEM, ANY, ANY, ANY, ANY, ANY], out_specs=(SMEM, ANY, ANY, ANY),
                    input_output_aliases={7: 1, 8: 2, 9: 3},
                    scratch_shapes=[buf(A, BL), buf(A, BL), pltpu.VMEM((A, 24, 128), bf16), pltpu.SMEM((A + 1,), i32),
                                    dma(A), dma(1), dma(1)],
                    cost_estimate=cost(6), name='attend')(tab, st, query, k_new, v_new, kc, vc, ko, vo, ao)

            def one_round(tag, c):
                st, s0, s1, part, dxs, pre, rc0, rc1, po0, po1, dxr, f0, f1, ko, vo, ao = c
                nrc0 = lax.ppermute(s0, 'dp', cw)
                nrc1 = lax.ppermute(s1, 'dp', ccw)
                npre = lax.ppermute(part, 'dp', swap)
                npo0 = lax.ppermute(rc0, 'dp', swap)
                npo1 = lax.ppermute(rc1, 'dp', swap)
                ndxr = lax.ppermute(dxs, 'dp', swap)
                st, s0, s1, part, dxs, f0, f1, ko, vo = pl.pallas_call(
                    functools.partial(round_kernel, NB), out_shape=(ST, chunk, chunk, both, cross, store, store, cache, cache),
                    in_specs=caches + [VMEM] * 6 + [ANY] * 4, out_specs=(SMEM,) + (VMEM,) * 4 + (ANY,) * 4,
                    input_output_aliases={10: 5, 11: 6, 12: 7, 13: 8},
                    scratch_shapes=DMA * 3,
                    cost_estimate=cost(10), name='round')(tab, st, kc, vc, pre, rc0, rc1, po0, po1, dxr, f0, f1, ko, vo)
                st, ko, vo, ao = attend(st, ko, vo, ao, 1)
                if tag != TAGS[-1]:
                    s0, s1, npo0, npo1 = lax.optimization_barrier((s0, s1, npo0, npo1))
                return st, s0, s1, part, dxs, npre, nrc0, nrc1, npo0, npo1, ndxr, f0, f1, ko, vo, ao

            rounds = tab[ROUNDS]

            def body(c):
                return (c[0] + TURN,) + functools.reduce(lambda c, tag: one_round(tag, c), TAGS, c[1:])

            c = lax.while_loop(lambda c: c[0] < rounds, body,
                           (jnp.int32(0), st, s0, s1, part, dxs, pre, rc0, rc1, po0, po1, dxr, f0, f1, ko, vo, ao))
            _, st, _, _, _, _, _, rc0, rc1, po0, po1, dxr, _, _, ko, vo, ao = c

            def close(last, st, ko, vo, *ins):
                n = len(ins)
                return pl.pallas_call(
                    functools.partial(close_kernel, NB, last), out_shape=(ST, cache, cache),
                    in_specs=[SMEM, SMEM] + [VMEM] * n + [ANY] * 2, out_specs=(SMEM, ANY, ANY),
                    input_output_aliases={n + 2: 1, n + 3: 2},
                    scratch_shapes=DMA,
                    name='close_last' if last else 'close')(tab, st, *ins, ko, vo)

            lpo0 = lax.ppermute(rc0, 'dp', swap)
            lpo1 = lax.ppermute(rc1, 'dp', swap)
            st, ko, vo = close(False, st, ko, vo, rc0, rc1, po0, po1, dxr)
            st, ko, vo = close(True, st, ko, vo, lpo0, lpo1)
            st, ko, vo, ao = attend(st, ko, vo, ao, SL // A)
            return ao, ko, vo

        ao, ko, vo = lax.switch(tab[PICK], [functools.partial(run, size) for size in SIZES])
        return ao, ko.reshape(k_cache.shape), vo.reshape(v_cache.shape), lens_out

    row_spec = P('dp')
    return jax.shard_map(local, mesh=mesh, in_specs=(row_spec, row_spec, row_spec, row_spec, P(), row_spec, row_spec),
                         out_specs=(row_spec, row_spec, row_spec, row_spec), check_vma=False)
```

```python
import functools

import jax
import jax.numpy as jnp
from jax import lax
from jax.experimental import pallas as pl
from jax.experimental.pallas import tpu as pltpu
from jax.sharding import PartitionSpec as P


BP, SHIFT = 8, 3
SIZES = range(84, 56, -4)
NX = 32
A = 4
SL = 32
BL = 64
WIDE = 400
S0, S1, R0, R1, XS, XR, FREE = range(7)
RDY, RDX, MLEN, SRC, ROUNDS = range(FREE * WIDE, FREE * WIDE + 200, 40)
CORE, PICK, SHARE, DUMP = range(ROUNDS + 1, ROUNDS + 5)
TAB = ROUNDS + 8
FWD, NONE = 2, 3
TURN = 2
SEGS = 6
IDLE = 4 * SEGS
HALF = 1 << 16
FLOPS = 4000000
LOW = HALF - 1
U_PART, U_MERGE, U_OWN, U_POST, U_XS, U_XR = 0, 2, 4, 6, 8, 9
STEP, DONE, STATE = 24, 32, 64
END = HALF * HALF // 4
bf16 = jnp.bfloat16
f32 = jnp.float32
i32 = jnp.int32


def gray(c):
    return c ^ (c >> 1)


def lens_kernel(x, o, bsem, ssem, rsem):
    me = lax.axis_index('dp')
    barrier = pltpu.get_barrier_semaphore()
    for k in range(1, 8):
        pl.semaphore_signal(barrier, inc=1, device_id=(lax.rem(me + k, 8),), device_id_type=pl.DeviceIdType.MESH)
    pl.semaphore_wait(barrier, 7)
    here = pltpu.make_async_copy(x, o.at[me], bsem)
    here.start()
    sends = []
    for k in range(1, 8):
        c = pltpu.make_async_remote_copy(src_ref=x, dst_ref=o.at[me], send_sem=ssem.at[k], recv_sem=rsem.at[k],
                                         device_id=(lax.rem(me + k, 8),), device_id_type=pl.DeviceIdType.MESH)
        c.start()
        sends.append(c)
    here.wait()
    for c in sends:
        c.wait()


def plan_kernel(me_ref, dest_ref, len_ref, tab, lens_out, nbv, kindv, todo, near, load, one, two, three, swap, addr, at):
    me = me_ref[0]
    zero = me - me
    for i in range(9):
        for ref in (load, one, two, three, swap):
            ref[i] = zero
    tab[CORE] = me & 1
    for j in range(SL):
        tab[RDY + j] = zero
        tab[RDX + j] = zero

    def first(i, c):
        size = len_ref[i >> 5, 0, i & 31]
        d = dest_ref[i]
        nb = (size + (BP - 1)) >> SHIFT
        ra = gray(i >> 6)
        delta = (gray(d >> 6) - ra) & 3
        nbv[i] = nb
        beside = (delta & 1) == 1
        ccw = delta == 3
        kindv[i] = jnp.where(beside, jnp.where(ccw, 4, 1), 0)
        slot = jnp.where(beside, jnp.where(ccw, 4, 0) + ra, 8)
        one[slot] = one[slot] + nb + HALF
        load[slot] = load[slot] + nb
        todo[c[0]] = i
        near[c[1]] = i
        cross = (delta == 0) & ((i >> 5) != (d >> 5))
        xslot = jnp.where(cross, i >> 5, 8)
        swap[xslot] = swap[xslot] + nb
        mine = jnp.where((d >> 5) == me, d & 31, SL)
        tab[MLEN + mine] = size
        tab[SRC + mine] = jnp.where((i >> 5) == me, i & 31, -1)
        return c[0] + jnp.where(delta == 2, 1, 0), c[1] + jnp.where(beside, 1, 0)

    far, side = lax.fori_loop(0, 8 * SL, first, (zero, zero), unroll=4)

    def lens(j, c):
        lens_out[j] = tab[MLEN + j] + 1
        return c

    lax.fori_loop(0, SL, lens, 0, unroll=8)

    def hops(x):
        return (x, (x + 1) & 3, (x + 2) & 3), (4 + x, 4 + ((x - 1) & 3), 4 + ((x + 2) & 3))

    def choose(n, c):
        i = todo[n]
        nb = nbv[i]
        (a1, a2, _), (b1, b2, _) = hops(gray(i >> 6))
        la1, la2, lb1, lb2 = load[a1], load[a2], load[b1], load[b2]
        la, lb = jnp.maximum(la1, la2), jnp.maximum(lb1, lb2)
        cw = (la < lb) | ((la == lb) & (la1 + la2 <= lb1 + lb2))
        x1, x2 = jnp.where(cw, a1, b1), jnp.where(cw, a2, b2)
        load[x1] = load[x1] + nb
        load[x2] = load[x2] + nb
        two[x1] = two[x1] + nb + HALF
        kindv[i] = jnp.where(cw, 2, 5)
        return c

    lax.fori_loop(0, far, choose, 0)

    def largest():
        return functools.reduce(jnp.maximum, [load[x] for x in range(8)])

    at[0] = largest()

    def detour(n, c):
        i = near[n]
        nb = nbv[i]
        cws, ccws = hops(gray(i >> 6))
        cw = kindv[i] == 1
        a = jnp.where(cw, cws[0], ccws[0])
        b = [jnp.where(cw, y, x) for x, y in zip(cws, ccws)]
        lb = [load[x] for x in b]
        la = load[a]

        @pl.when((la - nb >= functools.reduce(jnp.maximum, lb) + nb) & (la * 10 >= at[0] * 9))
        def _():
            load[a] = la - nb
            one[a] = one[a] - nb - HALF
            for x, l in zip(b, lb):
                load[x] = l + nb
            three[b[0]] = three[b[0]] + nb + HALF
            kindv[i] = jnp.where(cw, 6, 3)
            at[0] = largest()

        return c

    lax.fori_loop(0, side, detour, 0)

    def again(n, c):
        i = todo[n]
        nb = nbv[i]
        cws, ccws = hops(gray(i >> 6))
        cw = kindv[i] == 2
        a = [jnp.where(cw, x, y) for x, y in zip(cws[:2], ccws)]
        b = [jnp.where(cw, y, x) for x, y in zip(cws[:2], ccws)]
        la, lb = [load[x] for x in a], [load[x] for x in b]

        @pl.when(jnp.maximum(*lb) + nb < jnp.maximum(*la))
        def _():
            for x, l in zip(a + b, [l - nb for l in la] + [l + nb for l in lb]):
                load[x] = l
            two[a[0]] = two[a[0]] - nb - HALF
            two[b[0]] = two[b[0]] + nb + HALF
            kindv[i] = jnp.where(cw, 5, 2)

        return c

    lax.fori_loop(0, far, again, 0)

    def back(d, x, n):
        return 4 * d + ((x + (2 * d - 1) * n) & 3)

    def own_of(d, x):
        x = back(d, x, 0)
        return one[x] + two[x] + three[x]

    def link(d, x, size):
        up, up2 = back(d, x, 1), back(d, x, 2)
        own = own_of(d, x)
        fwd, fwd2 = two[up] + three[up], three[up2]
        start = jnp.maximum(own & LOW, jnp.where(fwd > 0, 2 * size, 0))
        own_up = own_of(d, up & 3)
        start_up = jnp.maximum(own_up & LOW, jnp.where(two[up2] + three[up2] > 0, 2 * size, 0))
        start2 = jnp.maximum(start + (fwd & LOW), jnp.where(fwd2 > 0, start_up + 2 * size, 0))
        return own, fwd, fwd2, start, start_up, start2

    cross = zero
    for d in range(8):
        cross = jnp.maximum(cross, (swap[d] + NX - 1) // NX)
    best, pick, turns, chunk = zero + END, zero, zero, zero
    all_links = [(two[x] + three[x], three[x], one[x] + two[x] + three[x]) for x in range(8)]
    parts = []
    for d in range(2):
        ring = all_links[4 * d:][:4][::1 - 2 * d]
        for x in range(4):
            (_, _, own), (fwd, _, own_up), (fwd_up, fwd2, _) = ring[x], ring[x - 1], ring[x - 2]
            parts.append([n & LOW for n in (own, fwd, own_up, fwd_up, fwd2)])
    for o, size in enumerate(SIZES):
        longest = zero
        for own, fwd, own_up, fwd_up, fwd2 in parts:
            wait, wait_up = jnp.where(fwd > 0, 2 * size, 0), jnp.where(fwd_up > 0, 2 * size, 0)
            total = jnp.maximum(own, wait) + fwd
            late = jnp.maximum(own_up, wait_up) + 2 * size
            longest = jnp.maximum(longest, jnp.where(fwd2 > 0, jnp.maximum(total, late) + fwd2, total))
        trips = (jnp.maximum((longest + size - 1) // size, cross) + TURN - 1) // TURN
        price = trips * (TURN * size + 7)
        better = price < best
        best, pick, turns, chunk = [jnp.where(better, n, o) for n, o in (
            (price, best), (o, pick), (trips * TURN, turns), (size, chunk))]
    tab[ROUNDS] = turns
    tab[PICK] = pick
    tab[SHARE] = jnp.minimum(SL // jnp.maximum(turns - TURN, 1) + 1, A)

    x0 = gray(me >> 1)
    left, right, opposite = (x0 - 1) & 3, (x0 + 1) & 3, (x0 + 2) & 3
    shift = []
    for lid, d, x in ((S0, 0, x0), (S1, 1, x0), (R0, 0, left), (R1, 1, right)):
        own, fwd, fwd2, start, _, start2 = link(d, x, chunk)
        here, up = back(d, x, 0), back(d, x, 1)
        base = zero + lid * WIDE
        wide = 2 * (three[here] >> 16)
        pad = base + 2 * (own >> 16)
        pad2 = pad + 2 + 2 * (fwd >> 16)
        tab[pad] = start - (own & LOW)
        tab[pad2] = start2 - start - (fwd & LOW)
        last = pad2 + 2 + 2 * (fwd2 >> 16)
        tab[last] = zero + END
        for a in (pad, pad2, last):
            tab[a + 1] = zero + NONE * HALF
        hop3, hop2 = three[here], two[here]
        segs = ((base, zero), (base + wide, hop3 & LOW), (base + wide + 2 * (hop2 >> 16), (hop3 + hop2) & LOW),
                (pad + 2, start), (pad + 2 + 2 * (three[up] >> 16), start + (three[up] & LOW)), (pad2 + 2, start2))
        for k, (where, pos) in enumerate(segs):
            addr[SEGS * lid + k] = where
            at[SEGS * lid + k] = pos
        shift.append(((hop3 + hop2) & LOW) - start)
    addr[IDLE] = zero + DUMP
    at[IDLE] = zero

    def append(seg, hit, nb, code):
        seg = jnp.where(hit, seg, IDLE)
        a, p = addr[seg], at[seg]
        tab[a] = nb
        tab[a + 1] = code
        addr[seg] = a + jnp.where(hit, 2, 0)
        at[seg] = p + nb
        return p + nb

    def source(s, c):
        i = (me >> 1) * 2 * SL + s
        kind = kindv[i]
        seg = jnp.where(kind > 3, SEGS + 6, 3) - kind
        append(seg, kind > 0, nbv[i], ((s >> 5) << 16) + (s & 31) * BL)
        return c

    lax.fori_loop(0, 2 * SL, source, 0, unroll=4)

    def visit(i, hit, seg, goes_on, seg_on, ahead):
        nb = nbv[i]
        dst = dest_ref[i]
        code = jnp.where(goes_on, FWD * HALF + at[seg] + ahead, (((dst >> 5) & 1) << 16) + (dst & 31) * BL)
        end = append(seg, hit, nb, code)
        append(seg_on, goes_on, nb, code)
        mine = hit & ((dst >> 5) == me) & jnp.logical_not(goes_on)
        tab[RDY + jnp.where(mine, dst & 31, SL)] = end

    for d, x in ((0, left), (1, right)):
        def beside(s, c):
            i = gray(x) * 2 * SL + s
            kind = kindv[i]
            h = kind - 3 * d
            along = (h > 0) & (h <= 3)
            about = kind == 6 - 3 * d
            seg = jnp.where(along, SEGS * (R0 + d) + 3 - h, SEGS * (R1 - d) + 5)
            visit(i, along | about, seg, along & (h > 1), SEGS * d + 6 - h, 0)
            return c

        lax.fori_loop(0, 2 * SL, beside, 0, unroll=2)

    def across(s, c):
        i = gray(opposite) * 2 * SL + s
        kind = kindv[i]
        d = jnp.where(kind > 3, 1, 0)
        h = kind - 3 * d
        seg = SEGS * (R0 + d) + jnp.where(h == 3, 3, 4)
        visit(i, h > 1, seg, h == 3, SEGS * d + 5, jnp.where(d == 0, shift[R0], shift[R1]))
        return c

    lax.fori_loop(0, 2 * SL, across, 0, unroll=2)

    for lid, sender, receiver in ((XS, me, me ^ 1), (XR, me ^ 1, me)):
        def cross_list(s, c):
            a, pos = c
            i = sender * SL + s
            nb = nbv[i]
            dst = dest_ref[i]
            hit = (dst >> 5) == receiver
            tab[a] = nb
            tab[a + 1] = (s if lid == XS else dst & 31) * BL
            pos = pos + jnp.where(hit, nb, 0)
            if lid == XR:
                tab[RDX + jnp.where(hit, dst & 31, SL)] = pos
            return a + jnp.where(hit, 2, 0), pos

        a, _ = lax.fori_loop(0, SL, cross_list, (zero + lid * WIDE, zero), unroll=2)
        tab[a] = zero + END
        tab[a + 1] = zero + NONE * HALF


class Mover:
    def __init__(self, tab, st_in, st, size):
        self.tab, self.st, self.size = tab, st, size
        self.core = tab[CORE]

        def cp(i, _):
            st[i] = st_in[i]
            return 0

        lax.fori_loop(0, STATE, cp, 0)

    def walk(self, lid, use, n, fn):
        tab, st = self.tab, self.st
        base = lid * WIDE

        def body(c):
            p, item, off, cnt = c
            width = tab[base + 2 * item]
            code = tab[base + 2 * item + 1]
            take = jnp.minimum(n - p, width - off)
            cnt = cnt + fn(p, take, code >> 16, (code & LOW) + off)
            off = off + take
            adv = off >= width
            return p + take, jnp.where(adv, item + 1, item), jnp.where(adv, 0, off), cnt

        c0 = (jnp.int32(0), st[2 * use], st[2 * use + 1], jnp.int32(0))
        _, item, off, cnt = lax.while_loop(lambda c: c[0] < n, body, c0)
        st[2 * use] = item
        st[2 * use + 1] = off
        return cnt

    @staticmethod
    def drain(cnt, ref, sem):
        @pl.when(cnt > 0)
        def _():
            part = ref.at[pl.ds(0, cnt)]
            pltpu.make_async_copy(part, part, sem).wait()

    def partial(self, d, kc, vc, buf, sem):
        core = self.core

        def fn(p, take, kind, idx):
            mine = kind == core

            @pl.when(mine & (core == 0))
            def _():
                pltpu.make_async_copy(vc.at[pl.ds(idx, take)], buf.at[pl.ds(p, take)], sem).start()

            @pl.when(mine & (core == 1))
            def _():
                pltpu.make_async_copy(kc.at[pl.ds(idx, take)], buf.at[pl.ds(p, take)], sem).start()

            return jnp.where(mine, take, 0)

        return self.walk(S0 + d, U_PART + d, self.size, fn)

    def merge(self, d, kc, vc, pre, fwd, buf, sem):
        core = self.core

        def fn(p, take, kind, idx):
            mine = kind == core

            @pl.when(mine & (core == 0))
            def _():
                pltpu.make_async_copy(kc.at[pl.ds(idx, take)], buf.at[pl.ds(p, take)], sem).start()

            @pl.when(mine & (core == 1))
            def _():
                pltpu.make_async_copy(vc.at[pl.ds(idx, take)], buf.at[pl.ds(p, take)], sem).start()

            @pl.when(kind == 1 - core)
            def _():
                pltpu.make_async_copy(pre.at[d, pl.ds(p, take)], buf.at[pl.ds(p, take)], sem).start()

            if fwd is not None:
                @pl.when(kind == FWD)
                def _():
                    pltpu.make_async_copy(fwd.at[pl.ds(idx, take)], buf.at[pl.ds(p, take)], sem).start()
            return jnp.where(kind < NONE, take, 0)

        return self.walk(S0 + d, U_MERGE + d, self.size, fn)

    def cross_send(self, kc, vc, buf, sem):
        def fn(p, take, kind, idx):
            @pl.when(kind == 0)
            def _():
                pltpu.make_async_copy(kc.at[pl.ds(idx, take)], buf.at[0, pl.ds(p, take)], sem).start()
                pltpu.make_async_copy(vc.at[pl.ds(idx, take)], buf.at[1, pl.ds(p, take)], sem).start()

            return jnp.where(kind == 0, 2 * take, 0)

        return self.walk(XS, U_XS, NX, fn)

    def cross_recv(self, n, ko, vo, buf, sem):
        def fn(p, take, kind, idx):
            @pl.when(kind == 0)
            def _():
                pltpu.make_async_copy(buf.at[0, pl.ds(p, take)], ko.at[pl.ds(idx, take)], sem).start()
                pltpu.make_async_copy(buf.at[1, pl.ds(p, take)], vo.at[pl.ds(idx, take)], sem).start()

            return jnp.where(kind == 0, 2 * take, 0)

        return self.walk(XR, U_XR, n, fn)

    def unpack(self, d, use, n, flip, ko, vo, fwd, buf, sem):
        core = self.core
        plane = 1 - core if flip else core

        def fn(p, take, kind, idx):
            mine = kind == core

            @pl.when(mine & (plane == 0))
            def _():
                pltpu.make_async_copy(buf.at[pl.ds(p, take)], ko.at[pl.ds(idx, take)], sem).start()

            @pl.when(mine & (plane == 1))
            def _():
                pltpu.make_async_copy(buf.at[pl.ds(p, take)], vo.at[pl.ds(idx, take)], sem).start()

            cnt = jnp.where(mine, take, 0)
            if fwd is not None:
                @pl.when(kind == FWD)
                def _():
                    pltpu.make_async_copy(buf.at[pl.ds(p, take)], fwd.at[pl.ds(idx, take)], sem).start()

                cnt = cnt + jnp.where(kind == FWD, take, 0)
            return cnt

        return self.walk(R0 + d, use + d, n, fn)


def open_kernel(NB, tab, st_in, kc, vc, st, part, sem):
    mv = Mover(tab, st_in, st, NB)
    mv.drain(sum(mv.partial(d, kc, vc, part.at[d], sem) for d in range(2)), kc, sem)


def open_more_kernel(NB, tab, st_in, kc, vc, st, part1, part2, dxs, sem):
    mv = Mover(tab, st_in, st, NB)
    cnt = sum(mv.partial(d, kc, vc, part.at[d], sem) for part in (part1, part2) for d in range(2))
    mv.drain(cnt + mv.cross_send(kc, vc, dxs, sem), kc, sem)


def open_merge_kernel(NB, tab, st_in, kc, vc, pre, st, send0, send1, sem):
    mv = Mover(tab, st_in, st, NB)
    mv.drain(sum(mv.merge(d, kc, vc, pre, None, buf, sem) for d, buf in enumerate((send0, send1))), kc, sem)


def stages(r, NB):
    return [jnp.where(r >= back, n, 0) for back, n in ((1, NB), (2, NB), (1, NX))]


def round_kernel(NB, tab, st_in, kc, vc, pre, rc0, rc1, po0, po1, dxr, f0i, f1i, koi, voi,
                 st, send0, send1, part, dxs, f0, f1, ko, vo, in_sem, out_sem, post_sem):
    mv = Mover(tab, st_in, st, NB)
    r = st_in[STEP]
    st[STEP] = r + 1
    n1, n2, nx = stages(r, NB)
    links = ((0, rc0, po0, f0, send0), (1, rc1, po1, f1, send1))
    mv.drain(sum(mv.unpack(d, U_OWN, n1, False, ko, vo, fwd, rc, out_sem) for d, rc, _, fwd, _ in links), kc, out_sem)
    cnt = sum(mv.merge(d, kc, vc, pre, fwd, send, in_sem) for d, _, _, fwd, send in links)
    late = sum(mv.unpack(d, U_POST, n2, True, ko, vo, None, po, post_sem) for d, _, po, _, _ in links)
    cnt += sum(mv.partial(d, kc, vc, part.at[d], in_sem) for d in range(2)) + mv.cross_send(kc, vc, dxs, in_sem)
    late += mv.cross_recv(nx, ko, vo, dxr, post_sem)
    mv.drain(cnt, kc, in_sem)
    mv.drain(late, kc, post_sem)


def close_kernel(NB, last, tab, st_in, *refs):
    if last:
        (po0, po1, koi, voi, st, ko, vo, sem) = refs
    else:
        (rc0, rc1, po0, po1, dxr, koi, voi, st, ko, vo, sem) = refs
    mv = Mover(tab, st_in, st, NB)
    r = st_in[STEP]
    st[STEP] = r + 1
    n1, n2, nx = stages(r, NB)
    cnt = sum(mv.unpack(d, U_POST, n2, True, ko, vo, None, po, sem) for d, po in enumerate((po0, po1)))
    if not last:
        cnt += sum(mv.unpack(d, U_OWN, n1, False, ko, vo, None, rc, sem) for d, rc in enumerate((rc0, rc1)))
        cnt += mv.cross_recv(nx, ko, vo, dxr, sem)
    mv.drain(cnt, ko, sem)


def attn_kernel(NB, batches, tab, st_in, q, kn, vn, kc, vc, koi, voi, aoi, st, ko, vo, ao,
                kb, vb, ob, sel, lsem, wsem, osem):
    def cp(i, _):
        st[i] = st_in[i]
        return 0

    lax.fori_loop(0, STATE, cp, 0)
    link_end = jnp.maximum((st_in[STEP] - 2) * NB, 0)
    swap_end = jnp.maximum((st_in[STEP] - 1) * NX, 0)

    def load(a, j):
        s = tab[SRC + j]

        @pl.when(s >= 0)
        def _():
            pltpu.make_async_copy(kc.at[pl.ds(s * BL, BL)], kb.at[a], lsem.at[a]).start()
            pltpu.make_async_copy(vc.at[pl.ds(s * BL, BL)], vb.at[a], lsem.at[a]).start()

        @pl.when(s < 0)
        def _():
            pltpu.make_async_copy(ko.at[pl.ds(j * BL, BL)], kb.at[a], lsem.at[a]).start()
            pltpu.make_async_copy(vo.at[pl.ds(j * BL, BL)], vb.at[a], lsem.at[a]).start()

    def compute(a, j):
        pltpu.make_async_copy(kb.at[a], kb.at[a], lsem.at[a]).wait()
        pltpu.make_async_copy(vb.at[a], vb.at[a], lsem.at[a]).wait()
        m = tab[MLEN + j]
        s = tab[SRC + j]
        b0 = m >> SHIFT
        row = lax.broadcasted_iota(i32, BLOCK, 0) >> 3
        for buf, new in ((kb, kn), (vb, vn)):
            x = buf[a, b0].astype(f32)
            fresh = jnp.concatenate([new[j].astype(f32)] * BP, axis=0)
            t = b0 * BP + row
            buf[a, b0] = jnp.where(t < m, x, jnp.where(t == m, fresh, 0.0)).astype(bf16)

        def wipe(b, _):
            kb[a, b] = jnp.zeros(BLOCK, bf16)
            vb[a, b] = jnp.zeros(BLOCK, bf16)
            return 0

        lax.fori_loop(b0 + 1, BL, wipe, 0)
        kf = kb[a].reshape(-1, 128)
        vf = vb[a].reshape(-1, 128)
        sc = lax.dot_general(q[j], kf, (((1,), (1,)), ((), ())), preferred_element_type=f32) * (128 ** -0.5)
        col = lax.broadcasted_iota(i32, sc.shape, 1)
        head = lax.broadcasted_iota(i32, sc.shape, 0) // 3
        ok = ((col & 7) == head) & ((col >> 3) <= m)
        sc = jnp.where(ok, sc, -1e30)
        top = jnp.max(sc, axis=1, keepdims=True)
        w = jnp.exp(sc - top)
        tot = jnp.sum(w, axis=1, keepdims=True)
        acc = lax.dot_general(w.astype(bf16), vf, (((1,), (0,)), ((), ())), preferred_element_type=f32)
        ob[a] = (acc / tot).astype(bf16)
        bw = jnp.where(s >= 0, 0, b0)

        tail = pl.ds(bw, BL - bw)
        home = pl.ds(j * BL + bw, BL - bw)
        pltpu.make_async_copy(kb.at[a, tail], ko.at[home], wsem.at[0]).start()
        pltpu.make_async_copy(vb.at[a, tail], vo.at[home], wsem.at[0]).start()
        pltpu.make_async_copy(ob.at[a], ao.at[j], osem.at[0]).start()
        return 2 * (BL - bw)

    share = tab[SHARE] if batches == 1 else A

    def batch(_, c):
        def pick(j, n):
            hit = (st[DONE + j] == 0) & (tab[RDY + j] <= link_end) & (tab[RDX + j] <= swap_end) & (n < share)
            sel[jnp.where(hit, n, A)] = j
            st[DONE + j] = jnp.where(hit, 1, st[DONE + j])
            return n + jnp.where(hit, 1, 0)

        n = lax.fori_loop(0, SL, pick, jnp.int32(0))

        def loads(a, _):
            load(a, sel[a])
            return 0

        lax.fori_loop(0, n, loads, 0)

        def computes(a, cnt):
            return cnt + compute(a, sel[a])

        cnt = lax.fori_loop(0, n, computes, jnp.int32(0))

        @pl.when(n > 0)
        def _():
            done = ko.at[pl.ds(0, cnt)]
            pltpu.make_async_copy(done, done, wsem.at[0]).wait()
            rows = ob.at[pl.ds(0, n)]
            pltpu.make_async_copy(rows, rows, osem.at[0]).wait()

        return c

    lax.fori_loop(0, batches, batch, 0)


SMEM = pl.BlockSpec(memory_space=pltpu.SMEM)
VMEM = pl.BlockSpec(memory_space=pltpu.VMEM)
ANY = pl.BlockSpec(memory_space=pl.ANY)
BLOCK = (8 * BP, 128)


def sds(shape, dtype=bf16):
    return jax.ShapeDtypeStruct(shape, dtype)


def dma(n):
    return pltpu.SemaphoreType.DMA((n,))


def buf(*lead):
    return pltpu.VMEM(lead + BLOCK, bf16)


def cost(us):
    return pl.CostEstimate(flops=us * FLOPS, bytes_accessed=us * FLOPS, transcendentals=0)


ST = sds((STATE,), i32)
DMA = [pltpu.SemaphoreType.DMA]
TAGS = ('ra', 'rb')


def solution(mesh):
    group = mesh.shape['dp']
    ring = [0, 1, 3, 2]
    cw = [(ring[k] * 2 + c, ring[(k + 1) % 4] * 2 + c) for k in range(4) for c in range(2)]
    ccw = [(b, a) for a, b in cw]
    swap = [(d, d ^ 1) for d in range(group)]

    def local(query, k_cache, v_cache, cache_lens, dest_slot, k_new, v_new):
        kc = k_cache.reshape((SL * BL,) + BLOCK)
        vc = v_cache.reshape((SL * BL,) + BLOCK)
        lens_all = pl.pallas_call(
            lens_kernel, out_shape=sds((8, 1, SL), i32), in_specs=[VMEM], out_specs=VMEM,
            scratch_shapes=[pltpu.SemaphoreType.DMA, dma(8), dma(8)],
            compiler_params=pltpu.CompilerParams(collective_id=0, has_side_effects=True),
            name='lens')(cache_lens.reshape(1, SL))
        me = jnp.full((1,), lax.axis_index('dp'), i32)
        tab, lens_out = pl.pallas_call(
            plan_kernel, out_shape=(sds((TAB,), i32), sds((SL,), i32)), in_specs=[SMEM] * 3, out_specs=(SMEM, SMEM),
            scratch_shapes=[pltpu.SMEM((8 * SL + 1,), i32)] * 4 + [pltpu.SMEM((IDLE + 1,), i32)] * 7,
            name='plan')(me, dest_slot, lens_all)

        def run(NB):
            def nothing(*refs):
                pass

            chunk, both, cross = sds((NB,) + BLOCK), sds((2, NB) + BLOCK), sds((2, NX) + BLOCK)
            cache, store = sds((SL * BL,) + BLOCK), sds((4 * SL * BL,) + BLOCK)
            ko, vo, ao, f0, f1, rc0, rc1, po0, po1, dxr = pl.pallas_call(
                nothing, out_shape=(cache, cache, sds((SL, 24, 128)), store, store, chunk, chunk, chunk, chunk, cross),
                out_specs=(ANY,) * 10, name='blank')()

            st = jnp.zeros((STATE,), i32)
            caches = [SMEM, SMEM, ANY, ANY]
            st, part = pl.pallas_call(
                functools.partial(open_kernel, NB), out_shape=(ST, both), in_specs=caches, out_specs=(SMEM, VMEM),
                scratch_shapes=DMA, name='open')(tab, st, kc, vc)
            pre = lax.ppermute(part, 'dp', swap)
            st, part1, part, dxs = pl.pallas_call(
                functools.partial(open_more_kernel, NB), out_shape=(ST, both, both, cross), in_specs=caches,
                out_specs=(SMEM,) + (VMEM,) * 3, scratch_shapes=DMA,
                name='open_more')(tab, st, kc, vc)
            pre1 = lax.ppermute(part1, 'dp', swap)
            st, s0, s1 = pl.pallas_call(
                functools.partial(open_merge_kernel, NB), out_shape=(ST, chunk, chunk), in_specs=caches + [VMEM],
                out_specs=(SMEM, VMEM, VMEM), scratch_shapes=DMA,
                name='open_merge')(tab, st, kc, vc, pre)
            pre = pre1

            def attend(st, ko, vo, ao, batches):
                return pl.pallas_call(
                    functools.partial(attn_kernel, NB, batches),
                    out_shape=(ST, cache, cache, sds((SL, 24, 128))),
                    in_specs=[SMEM, SMEM, VMEM, VMEM, VMEM, ANY, ANY, ANY, ANY, ANY], out_specs=(SMEM, ANY, ANY, ANY),
                    input_output_aliases={7: 1, 8: 2, 9: 3},
                    scratch_shapes=[buf(A, BL), buf(A, BL), pltpu.VMEM((A, 24, 128), bf16), pltpu.SMEM((A + 1,), i32),
                                    dma(A), dma(1), dma(1)],
                    cost_estimate=cost(6), name='attend')(tab, st, query, k_new, v_new, kc, vc, ko, vo, ao)

            def one_round(tag, c):
                st, s0, s1, part, dxs, pre, rc0, rc1, po0, po1, dxr, f0, f1, ko, vo, ao = c
                nrc0 = lax.ppermute(s0, 'dp', cw)
                nrc1 = lax.ppermute(s1, 'dp', ccw)
                npre = lax.ppermute(part, 'dp', swap)
                npo0 = lax.ppermute(rc0, 'dp', swap)
                npo1 = lax.ppermute(rc1, 'dp', swap)
                ndxr = lax.ppermute(dxs, 'dp', swap)
                st, s0, s1, part, dxs, f0, f1, ko, vo = pl.pallas_call(
                    functools.partial(round_kernel, NB), out_shape=(ST, chunk, chunk, both, cross, store, store, cache, cache),
                    in_specs=caches + [VMEM] * 6 + [ANY] * 4, out_specs=(SMEM,) + (VMEM,) * 4 + (ANY,) * 4,
                    input_output_aliases={10: 5, 11: 6, 12: 7, 13: 8},
                    scratch_shapes=DMA * 3,
                    cost_estimate=cost(10), name='round')(tab, st, kc, vc, pre, rc0, rc1, po0, po1, dxr, f0, f1, ko, vo)
                st, ko, vo, ao = attend(st, ko, vo, ao, 1)
                if tag != TAGS[-1]:
                    s0, s1, npo0, npo1 = lax.optimization_barrier((s0, s1, npo0, npo1))
                return st, s0, s1, part, dxs, npre, nrc0, nrc1, npo0, npo1, ndxr, f0, f1, ko, vo, ao

            rounds = tab[ROUNDS]

            def body(c):
                return (c[0] + TURN,) + functools.reduce(lambda c, tag: one_round(tag, c), TAGS, c[1:])

            c = lax.while_loop(lambda c: c[0] < rounds, body,
                           (jnp.int32(0), st, s0, s1, part, dxs, pre, rc0, rc1, po0, po1, dxr, f0, f1, ko, vo, ao))
            _, st, _, _, _, _, _, rc0, rc1, po0, po1, dxr, _, _, ko, vo, ao = c

            def close(last, st, ko, vo, *ins):
                n = len(ins)
                return pl.pallas_call(
                    functools.partial(close_kernel, NB, last), out_shape=(ST, cache, cache),
                    in_specs=[SMEM, SMEM] + [VMEM] * n + [ANY] * 2, out_specs=(SMEM, ANY, ANY),
                    input_output_aliases={n + 2: 1, n + 3: 2},
                    scratch_shapes=DMA,
                    name='close_last' if last else 'close')(tab, st, *ins, ko, vo)

            lpo0 = lax.ppermute(rc0, 'dp', swap)
            lpo1 = lax.ppermute(rc1, 'dp', swap)
            st, ko, vo = close(False, st, ko, vo, rc0, rc1, po0, po1, dxr)
            st, ko, vo = close(True, st, ko, vo, lpo0, lpo1)
            st, ko, vo, ao = attend(st, ko, vo, ao, SL // A)
            return ao, ko, vo

        ao, ko, vo = lax.switch(tab[PICK], [functools.partial(run, size) for size in SIZES])
        return ao, ko.reshape(k_cache.shape), vo.reshape(v_cache.shape), lens_out

    row_spec = P('dp')
    return jax.shard_map(local, mesh=mesh, in_specs=(row_spec, row_spec, row_spec, row_spec, P(), row_spec, row_spec),
                         out_specs=(row_spec, row_spec, row_spec, row_spec), check_vma=False)
```

```python
import functools

import jax
import jax.numpy as jnp
from jax import lax
from jax.experimental import pallas as pl
from jax.experimental.pallas import tpu as pltpu
from jax.sharding import PartitionSpec as P


BP, SHIFT = 8, 3
SIZES = range(84, 56, -4)
NX = 32
A = 4
SL = 32
BL = 64
WIDE = 400
S0, S1, R0, R1, XS, XR, FREE = range(7)
RDY, RDX, MLEN, SRC, ROUNDS = range(FREE * WIDE, FREE * WIDE + 200, 40)
CORE, PICK, SHARE, DUMP = range(ROUNDS + 1, ROUNDS + 5)
TAB = ROUNDS + 8
FWD, NONE = 2, 3
TURN = 2
SEGS = 6
IDLE = 4 * SEGS
HALF = 1 << 16
FLOPS = 4000000
LOW = HALF - 1
U_PART, U_MERGE, U_OWN, U_POST, U_XS, U_XR = 0, 2, 4, 6, 8, 9
STEP, DONE, STATE = 24, 32, 64
END = HALF * HALF // 4
bf16 = jnp.bfloat16
f32 = jnp.float32
i32 = jnp.int32


def gray(c):
    return c ^ (c >> 1)


def lens_kernel(x, o, bsem, ssem, rsem):
    me = lax.axis_index('dp')
    barrier = pltpu.get_barrier_semaphore()
    for k in range(1, 8):
        pl.semaphore_signal(barrier, inc=1, device_id=(lax.rem(me + k, 8),), device_id_type=pl.DeviceIdType.MESH)
    pl.semaphore_wait(barrier, 7)
    here = pltpu.make_async_copy(x, o.at[me], bsem)
    here.start()
    sends = []
    for k in range(1, 8):
        c = pltpu.make_async_remote_copy(src_ref=x, dst_ref=o.at[me], send_sem=ssem.at[k], recv_sem=rsem.at[k],
                                         device_id=(lax.rem(me + k, 8),), device_id_type=pl.DeviceIdType.MESH)
        c.start()
        sends.append(c)
    here.wait()
    for c in sends:
        c.wait()


def plan_kernel(me_ref, dest_ref, len_ref, tab, lens_out, nbv, kindv, todo, near, load, one, two, three, addr, at):
    me = me_ref[0]
    zero = me - me
    for i in range(17):
        for ref in (one, two, three):
            ref[i] = zero
    tab[CORE] = me & 1
    for j in range(SL):
        tab[RDY + j] = zero
        tab[RDX + j] = zero

    def first(i, c):
        size = len_ref[i >> 5, 0, i & 31]
        d = dest_ref[i]
        nb = (size + (BP - 1)) >> SHIFT
        ra = gray(i >> 6)
        delta = (gray(d >> 6) - ra) & 3
        nbv[i] = nb
        beside = (delta & 1) == 1
        ccw = delta == 3
        kindv[i] = jnp.where(beside, jnp.where(ccw, 4, 1), 0)
        todo[c[0]] = i
        near[c[1]] = i
        cross = (delta == 0) & ((i >> 5) != (d >> 5))
        slot = jnp.where(beside, jnp.where(ccw, 4, 0) + ra, jnp.where(cross, 9 + (i >> 5), 8))
        one[slot] = one[slot] + nb + HALF
        mine = jnp.where((d >> 5) == me, d & 31, SL)
        tab[MLEN + mine] = size
        tab[SRC + mine] = jnp.where((i >> 5) == me, i & 31, -1)
        return c[0] + jnp.where(delta == 2, 1, 0), c[1] + jnp.where(beside, 1, 0)

    far, side = lax.fori_loop(0, 8 * SL, first, (zero, zero), unroll=8)
    for i in range(8):
        load[i] = one[i] & LOW

    def lens(j, c):
        lens_out[j] = tab[MLEN + j] + 1
        return c

    lax.fori_loop(0, SL, lens, 0, unroll=8)

    def hops(x):
        return (x, (x + 1) & 3, (x + 2) & 3), (4 + x, 4 + ((x - 1) & 3), 4 + ((x + 2) & 3))

    def choose(n, c):
        i = todo[n]
        nb = nbv[i]
        (a1, a2, _), (b1, b2, _) = hops(gray(i >> 6))
        la1, la2, lb1, lb2 = load[a1], load[a2], load[b1], load[b2]
        la, lb = jnp.maximum(la1, la2), jnp.maximum(lb1, lb2)
        cw = (la < lb) | ((la == lb) & (la1 + la2 <= lb1 + lb2))
        x1, x2 = jnp.where(cw, a1, b1), jnp.where(cw, a2, b2)
        load[x1] = load[x1] + nb
        load[x2] = load[x2] + nb
        two[x1] = two[x1] + nb + HALF
        kindv[i] = jnp.where(cw, 2, 5)
        return c

    lax.fori_loop(0, far, choose, 0)

    def largest():
        return functools.reduce(jnp.maximum, [load[x] for x in range(8)])

    at[0] = largest()

    def detour(n, c):
        i = near[n]
        nb = nbv[i]
        cws, ccws = hops(gray(i >> 6))
        cw = kindv[i] == 1
        a = jnp.where(cw, cws[0], ccws[0])
        b = [jnp.where(cw, y, x) for x, y in zip(cws, ccws)]
        lb = [load[x] for x in b]
        la = load[a]

        @pl.when((la - nb >= functools.reduce(jnp.maximum, lb) + nb) & (la * 10 >= at[0] * 9))
        def _():
            load[a] = la - nb
            one[a] = one[a] - nb - HALF
            for x, l in zip(b, lb):
                load[x] = l + nb
            three[b[0]] = three[b[0]] + nb + HALF
            kindv[i] = jnp.where(cw, 6, 3)
            at[0] = largest()

        return c

    lax.fori_loop(0, side, detour, 0)

    def again(n, c):
        i = todo[n]
        nb = nbv[i]
        cws, ccws = hops(gray(i >> 6))
        cw = kindv[i] == 2
        a = [jnp.where(cw, x, y) for x, y in zip(cws[:2], ccws)]
        b = [jnp.where(cw, y, x) for x, y in zip(cws[:2], ccws)]
        la, lb = [load[x] for x in a], [load[x] for x in b]

        @pl.when(jnp.maximum(*lb) + nb < jnp.maximum(*la))
        def _():
            for x, l in zip(a + b, [l - nb for l in la] + [l + nb for l in lb]):
                load[x] = l
            two[a[0]] = two[a[0]] - nb - HALF
            two[b[0]] = two[b[0]] + nb + HALF
            kindv[i] = jnp.where(cw, 5, 2)

        return c

    lax.fori_loop(0, far, again, 0)

    def back(d, x, n):
        return 4 * d + ((x + (2 * d - 1) * n) & 3)

    def own_of(d, x):
        x = back(d, x, 0)
        return one[x] + two[x] + three[x]

    def link(d, x, size):
        up, up2 = back(d, x, 1), back(d, x, 2)
        own = own_of(d, x)
        fwd, fwd2 = two[up] + three[up], three[up2]
        start = jnp.maximum(own & LOW, jnp.where(fwd > 0, 2 * size, 0))
        own_up = own_of(d, up & 3)
        start_up = jnp.maximum(own_up & LOW, jnp.where(two[up2] + three[up2] > 0, 2 * size, 0))
        start2 = jnp.maximum(start + (fwd & LOW), jnp.where(fwd2 > 0, start_up + 2 * size, 0))
        return own, fwd, fwd2, start, start_up, start2

    cross = zero
    for d in range(8):
        cross = jnp.maximum(cross, ((one[9 + d] & LOW) + NX - 1) // NX)
    best, pick, turns, chunk = zero + END, zero, zero, zero
    all_links = [(two[x] + three[x], three[x], one[x] + two[x] + three[x]) for x in range(8)]
    parts = []
    for d in range(2):
        ring = all_links[4 * d:][:4][::1 - 2 * d]
        for x in range(4):
            (_, _, own), (fwd, _, own_up), (fwd_up, fwd2, _) = ring[x], ring[x - 1], ring[x - 2]
            parts.append([n & LOW for n in (own, fwd, own_up, fwd_up, fwd2)])
    for o, size in enumerate(SIZES):
        longest = zero
        for own, fwd, own_up, fwd_up, fwd2 in parts:
            wait, wait_up = jnp.where(fwd > 0, 2 * size, 0), jnp.where(fwd_up > 0, 2 * size, 0)
            total = jnp.maximum(own, wait) + fwd
            late = jnp.maximum(own_up, wait_up) + 2 * size
            longest = jnp.maximum(longest, jnp.where(fwd2 > 0, jnp.maximum(total, late) + fwd2, total))
        trips = (jnp.maximum((longest + size - 1) // size, cross) + TURN - 1) // TURN
        price = trips * (TURN * size + 7)
        better = price < best
        best, pick, turns, chunk = [jnp.where(better, n, o) for n, o in (
            (price, best), (o, pick), (trips * TURN, turns), (size, chunk))]
    tab[ROUNDS] = turns
    tab[PICK] = pick
    tab[SHARE] = jnp.minimum(SL // jnp.maximum(turns - TURN, 1) + 1, A)

    x0 = gray(me >> 1)
    left, right, opposite = (x0 - 1) & 3, (x0 + 1) & 3, (x0 + 2) & 3
    shift = []
    for lid, d, x in ((S0, 0, x0), (S1, 1, x0), (R0, 0, left), (R1, 1, right)):
        own, fwd, fwd2, start, _, start2 = link(d, x, chunk)
        here, up = back(d, x, 0), back(d, x, 1)
        base = zero + lid * WIDE
        wide = 2 * (three[here] >> 16)
        pad = base + 2 * (own >> 16)
        pad2 = pad + 2 + 2 * (fwd >> 16)
        tab[pad] = start - (own & LOW)
        tab[pad2] = start2 - start - (fwd & LOW)
        last = pad2 + 2 + 2 * (fwd2 >> 16)
        tab[last] = zero + END
        for a in (pad, pad2, last):
            tab[a + 1] = zero + NONE * HALF
        hop3, hop2 = three[here], two[here]
        segs = ((base, zero), (base + wide, hop3 & LOW), (base + wide + 2 * (hop2 >> 16), (hop3 + hop2) & LOW),
                (pad + 2, start), (pad + 2 + 2 * (three[up] >> 16), start + (three[up] & LOW)), (pad2 + 2, start2))
        for k, (where, pos) in enumerate(segs):
            addr[SEGS * lid + k] = where
            at[SEGS * lid + k] = pos
        shift.append(((hop3 + hop2) & LOW) - start)
    addr[IDLE] = zero + DUMP
    at[IDLE] = zero

    def append(seg, hit, nb, code):
        seg = jnp.where(hit, seg, IDLE)
        a, p = addr[seg], at[seg]
        tab[a] = nb
        tab[a + 1] = code
        addr[seg] = a + jnp.where(hit, 2, 0)
        at[seg] = p + nb
        return p + nb

    def source(s, c):
        i = (me >> 1) * 2 * SL + s
        kind = kindv[i]
        seg = jnp.where(kind > 3, SEGS + 6, 3) - kind
        append(seg, kind > 0, nbv[i], ((s >> 5) << 16) + (s & 31) * BL)
        return c

    lax.fori_loop(0, 2 * SL, source, 0, unroll=4)

    def visit(i, hit, seg, goes_on, seg_on, ahead):
        nb = nbv[i]
        dst = dest_ref[i]
        code = jnp.where(goes_on, FWD * HALF + at[seg] + ahead, (((dst >> 5) & 1) << 16) + (dst & 31) * BL)
        end = append(seg, hit, nb, code)
        append(seg_on, goes_on, nb, code)
        mine = hit & ((dst >> 5) == me) & jnp.logical_not(goes_on)
        tab[RDY + jnp.where(mine, dst & 31, SL)] = end

    for d, x in ((0, left), (1, right)):
        def beside(s, c):
            i = gray(x) * 2 * SL + s
            kind = kindv[i]
            h = kind - 3 * d
            along = (h > 0) & (h <= 3)
            about = kind == 6 - 3 * d
            seg = jnp.where(along, SEGS * (R0 + d) + 3 - h, SEGS * (R1 - d) + 5)
            visit(i, along | about, seg, along & (h > 1), SEGS * d + 6 - h, 0)
            return c

        lax.fori_loop(0, 2 * SL, beside, 0, unroll=2)

    def across(s, c):
        i = gray(opposite) * 2 * SL + s
        kind = kindv[i]
        d = jnp.where(kind > 3, 1, 0)
        h = kind - 3 * d
        seg = SEGS * (R0 + d) + jnp.where(h == 3, 3, 4)
        visit(i, h > 1, seg, h == 3, SEGS * d + 5, jnp.where(d == 0, shift[R0], shift[R1]))
        return c

    lax.fori_loop(0, 2 * SL, across, 0, unroll=2)

    for lid, sender, receiver in ((XS, me, me ^ 1), (XR, me ^ 1, me)):
        def cross_list(s, c):
            a, pos = c
            i = sender * SL + s
            nb = nbv[i]
            dst = dest_ref[i]
            hit = (dst >> 5) == receiver
            tab[a] = nb
            tab[a + 1] = (s if lid == XS else dst & 31) * BL
            pos = pos + jnp.where(hit, nb, 0)
            if lid == XR:
                tab[RDX + jnp.where(hit, dst & 31, SL)] = pos
            return a + jnp.where(hit, 2, 0), pos

        a, _ = lax.fori_loop(0, SL, cross_list, (zero + lid * WIDE, zero), unroll=2)
        tab[a] = zero + END
        tab[a + 1] = zero + NONE * HALF


class Mover:
    def __init__(self, tab, st_in, st, size):
        self.tab, self.st, self.size = tab, st, size
        self.core = tab[CORE]

        def cp(i, _):
            st[i] = st_in[i]
            return 0

        lax.fori_loop(0, STATE, cp, 0)

    def walk(self, lid, use, n, fn):
        tab, st = self.tab, self.st
        base = lid * WIDE

        def body(c):
            p, item, off, cnt = c
            width = tab[base + 2 * item]
            code = tab[base + 2 * item + 1]
            take = jnp.minimum(n - p, width - off)
            cnt = cnt + fn(p, take, code >> 16, (code & LOW) + off)
            off = off + take
            adv = off >= width
            return p + take, jnp.where(adv, item + 1, item), jnp.where(adv, 0, off), cnt

        c0 = (jnp.int32(0), st[2 * use], st[2 * use + 1], jnp.int32(0))
        _, item, off, cnt = lax.while_loop(lambda c: c[0] < n, body, c0)
        st[2 * use] = item
        st[2 * use + 1] = off
        return cnt

    @staticmethod
    def drain(cnt, ref, sem):
        @pl.when(cnt > 0)
        def _():
            part = ref.at[pl.ds(0, cnt)]
            pltpu.make_async_copy(part, part, sem).wait()

    def partial(self, d, kc, vc, buf, sem):
        core = self.core

        def fn(p, take, kind, idx):
            mine = kind == core

            @pl.when(mine & (core == 0))
            def _():
                pltpu.make_async_copy(vc.at[pl.ds(idx, take)], buf.at[pl.ds(p, take)], sem).start()

            @pl.when(mine & (core == 1))
            def _():
                pltpu.make_async_copy(kc.at[pl.ds(idx, take)], buf.at[pl.ds(p, take)], sem).start()

            return jnp.where(mine, take, 0)

        return self.walk(S0 + d, U_PART + d, self.size, fn)

    def merge(self, d, kc, vc, pre, fwd, buf, sem):
        core = self.core

        def fn(p, take, kind, idx):
            mine = kind == core

            @pl.when(mine & (core == 0))
            def _():
                pltpu.make_async_copy(kc.at[pl.ds(idx, take)], buf.at[pl.ds(p, take)], sem).start()

            @pl.when(mine & (core == 1))
            def _():
                pltpu.make_async_copy(vc.at[pl.ds(idx, take)], buf.at[pl.ds(p, take)], sem).start()

            @pl.when(kind == 1 - core)
            def _():
                pltpu.make_async_copy(pre.at[d, pl.ds(p, take)], buf.at[pl.ds(p, take)], sem).start()

            if fwd is not None:
                @pl.when(kind == FWD)
                def _():
                    pltpu.make_async_copy(fwd.at[pl.ds(idx, take)], buf.at[pl.ds(p, take)], sem).start()
            return jnp.where(kind < NONE, take, 0)

        return self.walk(S0 + d, U_MERGE + d, self.size, fn)

    def cross_send(self, kc, vc, buf, sem):
        def fn(p, take, kind, idx):
            @pl.when(kind == 0)
            def _():
                pltpu.make_async_copy(kc.at[pl.ds(idx, take)], buf.at[0, pl.ds(p, take)], sem).start()
                pltpu.make_async_copy(vc.at[pl.ds(idx, take)], buf.at[1, pl.ds(p, take)], sem).start()

            return jnp.where(kind == 0, 2 * take, 0)

        return self.walk(XS, U_XS, NX, fn)

    def cross_recv(self, n, ko, vo, buf, sem):
        def fn(p, take, kind, idx):
            @pl.when(kind == 0)
            def _():
                pltpu.make_async_copy(buf.at[0, pl.ds(p, take)], ko.at[pl.ds(idx, take)], sem).start()
                pltpu.make_async_copy(buf.at[1, pl.ds(p, take)], vo.at[pl.ds(idx, take)], sem).start()

            return jnp.where(kind == 0, 2 * take, 0)

        return self.walk(XR, U_XR, n, fn)

    def unpack(self, d, use, n, flip, ko, vo, fwd, buf, sem):
        core = self.core
        plane = 1 - core if flip else core

        def fn(p, take, kind, idx):
            mine = kind == core

            @pl.when(mine & (plane == 0))
            def _():
                pltpu.make_async_copy(buf.at[pl.ds(p, take)], ko.at[pl.ds(idx, take)], sem).start()

            @pl.when(mine & (plane == 1))
            def _():
                pltpu.make_async_copy(buf.at[pl.ds(p, take)], vo.at[pl.ds(idx, take)], sem).start()

            cnt = jnp.where(mine, take, 0)
            if fwd is not None:
                @pl.when(kind == FWD)
                def _():
                    pltpu.make_async_copy(buf.at[pl.ds(p, take)], fwd.at[pl.ds(idx, take)], sem).start()

                cnt = cnt + jnp.where(kind == FWD, take, 0)
            return cnt

        return self.walk(R0 + d, use + d, n, fn)


def open_kernel(NB, tab, st_in, kc, vc, st, part, sem):
    mv = Mover(tab, st_in, st, NB)
    mv.drain(sum(mv.partial(d, kc, vc, part.at[d], sem) for d in range(2)), kc, sem)


def open_merge_kernel(NB, tab, st_in, kc, vc, pre, st, send0, send1, sem):
    mv = Mover(tab, st_in, st, NB)
    mv.drain(sum(mv.merge(d, kc, vc, pre, None, buf, sem) for d, buf in enumerate((send0, send1))), kc, sem)


def stages(r, NB):
    return [jnp.where(r >= back, n, 0) for back, n in ((1, NB), (2, NB), (1, NX))]


def round_kernel(NB, tab, st_in, kc, vc, pre, rc0, rc1, po0, po1, dxr, f0i, f1i, koi, voi,
                 st, send0, send1, part, dxs, f0, f1, ko, vo, in_sem, out_sem, post_sem):
    mv = Mover(tab, st_in, st, NB)
    r = st_in[STEP]
    st[STEP] = r + 1
    n1, n2, nx = stages(r, NB)
    links = ((0, rc0, po0, f0, send0), (1, rc1, po1, f1, send1))
    mv.drain(sum(mv.unpack(d, U_OWN, n1, False, ko, vo, fwd, rc, out_sem) for d, rc, _, fwd, _ in links), kc, out_sem)
    cnt = sum(mv.merge(d, kc, vc, pre, fwd, send, in_sem) for d, _, _, fwd, send in links)
    late = sum(mv.unpack(d, U_POST, n2, True, ko, vo, None, po, post_sem) for d, _, po, _, _ in links)
    cnt += sum(mv.partial(d, kc, vc, part.at[d], in_sem) for d in range(2)) + mv.cross_send(kc, vc, dxs, in_sem)
    late += mv.cross_recv(nx, ko, vo, dxr, post_sem)
    mv.drain(cnt, kc, in_sem)
    mv.drain(late, kc, post_sem)


def close_kernel(NB, last, tab, st_in, *refs):
    if last:
        (po0, po1, koi, voi, st, ko, vo, sem) = refs
    else:
        (rc0, rc1, po0, po1, dxr, koi, voi, st, ko, vo, sem) = refs
    mv = Mover(tab, st_in, st, NB)
    r = st_in[STEP]
    st[STEP] = r + 1
    n1, n2, nx = stages(r, NB)
    cnt = sum(mv.unpack(d, U_POST, n2, True, ko, vo, None, po, sem) for d, po in enumerate((po0, po1)))
    if not last:
        cnt += sum(mv.unpack(d, U_OWN, n1, False, ko, vo, None, rc, sem) for d, rc in enumerate((rc0, rc1)))
        cnt += mv.cross_recv(nx, ko, vo, dxr, sem)
    mv.drain(cnt, ko, sem)


def attn_kernel(NB, last, tab, st_in, q, kn, vn, kc, vc, koi, voi, aoi, st, ko, vo, ao,
                kb, vb, ob, sel, lsem, wsem):
    def cp(i, _):
        st[i] = st_in[i]
        return 0

    lax.fori_loop(0, STATE, cp, 0)
    share = SL if last else tab[SHARE]
    link_end = jnp.maximum((st_in[STEP] - 2) * NB, 0)
    swap_end = jnp.maximum((st_in[STEP] - 1) * NX, 0)

    def load(a, j):
        s = tab[SRC + j]

        @pl.when(s >= 0)
        def _():
            pltpu.make_async_copy(kc.at[pl.ds(s * BL, BL)], kb.at[a], lsem.at[a]).start()
            pltpu.make_async_copy(vc.at[pl.ds(s * BL, BL)], vb.at[a], lsem.at[a]).start()

        @pl.when(s < 0)
        def _():
            pltpu.make_async_copy(ko.at[pl.ds(j * BL, BL)], kb.at[a], lsem.at[a]).start()
            pltpu.make_async_copy(vo.at[pl.ds(j * BL, BL)], vb.at[a], lsem.at[a]).start()

    def compute(a, j):
        pltpu.make_async_copy(kb.at[a], kb.at[a], lsem.at[a]).wait()
        pltpu.make_async_copy(vb.at[a], vb.at[a], lsem.at[a]).wait()
        m = tab[MLEN + j]
        b0 = m >> SHIFT
        row = lax.broadcasted_iota(i32, BLOCK, 0) >> 3
        for buf, new in ((kb, kn), (vb, vn)):
            x = buf[a, b0].astype(f32)
            fresh = jnp.concatenate([new[j].astype(f32)] * BP, axis=0)
            t = b0 * BP + row
            buf[a, b0] = jnp.where(t < m, x, jnp.where(t == m, fresh, 0.0)).astype(bf16)

        def wipe(b, _):
            kb[a, b] = jnp.zeros(BLOCK, bf16)
            vb[a, b] = jnp.zeros(BLOCK, bf16)
            return 0

        lax.fori_loop(b0 + 1, BL, wipe, 0)
        kf = kb[a].reshape(-1, 128)
        vf = vb[a].reshape(-1, 128)
        sc = lax.dot_general(q[j], kf, (((1,), (1,)), ((), ())), preferred_element_type=f32) * (128 ** -0.5)
        col = lax.broadcasted_iota(i32, sc.shape, 1)
        head = lax.broadcasted_iota(i32, sc.shape, 0) // 3
        ok = ((col & 7) == head) & ((col >> 3) <= m)
        sc = jnp.where(ok, sc, -1e30)
        top = jnp.max(sc, axis=1, keepdims=True)
        w = jnp.exp(sc - top)
        tot = jnp.sum(w, axis=1, keepdims=True)
        acc = lax.dot_general(w.astype(bf16), vf, (((1,), (0,)), ((), ())), preferred_element_type=f32)
        ob[a] = (acc / tot).astype(bf16)
        for src, dst in writes(a, j):
            pltpu.make_async_copy(src, dst, wsem.at[a]).start()

    def writes(a, j):
        bw = jnp.where(tab[SRC + j] >= 0, 0, tab[MLEN + j] >> SHIFT)
        tail, home = pl.ds(bw, BL - bw), pl.ds(j * BL + bw, BL - bw)
        return (kb.at[a, tail], ko.at[home]), (vb.at[a, tail], vo.at[home]), (ob.at[a], ao.at[j])

    def settle(k):
        a, j = k & (A - 1), sel[k]
        for src, dst in writes(a, j):
            pltpu.make_async_copy(src, dst, wsem.at[a]).wait()

    def pick(j, n):
        hit = (st[DONE + j] == 0) & (tab[RDY + j] <= link_end) & (tab[RDX + j] <= swap_end) & (n < share)
        sel[n] = j
        st[DONE + j] = jnp.where(hit, 1, st[DONE + j])
        return n + jnp.where(hit, 1, 0)

    n = lax.fori_loop(0, SL, pick, jnp.int32(0))

    def early(k, c):
        load(k, sel[k])
        return c

    lax.fori_loop(0, jnp.minimum(n, A - 1), early, 0)

    def step(k, c):
        compute(k & (A - 1), sel[k])
        later = k + A - 1

        @pl.when(later < n)
        def _():
            @pl.when(k >= 1)
            def _():
                settle(k - 1)

            load(later & (A - 1), sel[later])

        return c

    lax.fori_loop(0, n, step, 0)

    def wind_up(k, c):
        settle(k)
        return c

    lax.fori_loop(jnp.maximum(n - A, 0), n, wind_up, 0)


SMEM = pl.BlockSpec(memory_space=pltpu.SMEM)
VMEM = pl.BlockSpec(memory_space=pltpu.VMEM)
ANY = pl.BlockSpec(memory_space=pl.ANY)
BLOCK = (8 * BP, 128)


def sds(shape, dtype=bf16):
    return jax.ShapeDtypeStruct(shape, dtype)


def dma(n):
    return pltpu.SemaphoreType.DMA((n,))


def buf(*lead):
    return pltpu.VMEM(lead + BLOCK, bf16)


def cost(us):
    return pl.CostEstimate(flops=us * FLOPS, bytes_accessed=us * FLOPS, transcendentals=0)


ST = sds((STATE,), i32)
DMA = [pltpu.SemaphoreType.DMA]
TAGS = ('ra', 'rb')


def solution(mesh):
    group = mesh.shape['dp']
    ring = [0, 1, 3, 2]
    cw = [(ring[k] * 2 + c, ring[(k + 1) % 4] * 2 + c) for k in range(4) for c in range(2)]
    ccw = [(b, a) for a, b in cw]
    swap = [(d, d ^ 1) for d in range(group)]

    def local(query, k_cache, v_cache, cache_lens, dest_slot, k_new, v_new):
        kc = k_cache.reshape((SL * BL,) + BLOCK)
        vc = v_cache.reshape((SL * BL,) + BLOCK)
        lens_all = pl.pallas_call(
            lens_kernel, out_shape=sds((8, 1, SL), i32), in_specs=[VMEM], out_specs=VMEM,
            scratch_shapes=[pltpu.SemaphoreType.DMA, dma(8), dma(8)],
            compiler_params=pltpu.CompilerParams(collective_id=0, has_side_effects=True),
            name='lens')(cache_lens.reshape(1, SL))
        me = jnp.full((1,), lax.axis_index('dp'), i32)
        tab, lens_out = pl.pallas_call(
            plan_kernel, out_shape=(sds((TAB,), i32), sds((SL,), i32)), in_specs=[SMEM] * 3, out_specs=(SMEM, SMEM),
            scratch_shapes=[pltpu.SMEM((8 * SL + 1,), i32)] * 4 + [pltpu.SMEM((IDLE + 1,), i32)] * 6,
            name='plan')(me, dest_slot, lens_all)

        def run(NB):
            def nothing(*refs):
                pass

            chunk, both, cross = sds((NB,) + BLOCK), sds((2, NB) + BLOCK), sds((2, NX) + BLOCK)
            cache, store = sds((SL * BL,) + BLOCK), sds((4 * SL * BL,) + BLOCK)
            ko, vo, ao, f0, f1, rc0, rc1, po0, po1, dxr = pl.pallas_call(
                nothing, out_shape=(cache, cache, sds((SL, 24, 128)), store, store, chunk, chunk, chunk, chunk, cross),
                out_specs=(ANY,) * 10, name='blank')()

            st = jnp.zeros((STATE,), i32)
            caches = [SMEM, SMEM, ANY, ANY]

            def opened(st):
                return pl.pallas_call(
                    functools.partial(open_kernel, NB), out_shape=(ST, both), in_specs=caches, out_specs=(SMEM, VMEM),
                    scratch_shapes=DMA, name='open')(tab, st, kc, vc)

            st, part = opened(st)
            pre = lax.ppermute(part, 'dp', swap)
            st, part = opened(st)
            pre1 = lax.ppermute(part, 'dp', swap)
            st, s0, s1 = pl.pallas_call(
                functools.partial(open_merge_kernel, NB), out_shape=(ST, chunk, chunk), in_specs=caches + [VMEM],
                out_specs=(SMEM, VMEM, VMEM), scratch_shapes=DMA,
                name='open_merge')(tab, st, kc, vc, pre)
            pre = pre1

            def attend(st, ko, vo, ao, last):
                return pl.pallas_call(
                    functools.partial(attn_kernel, NB, last),
                    out_shape=(ST, cache, cache, sds((SL, 24, 128))),
                    in_specs=[SMEM, SMEM, VMEM, VMEM, VMEM, ANY, ANY, ANY, ANY, ANY], out_specs=(SMEM, ANY, ANY, ANY),
                    input_output_aliases={7: 1, 8: 2, 9: 3},
                    scratch_shapes=[buf(A, BL), buf(A, BL), pltpu.VMEM((A, 24, 128), bf16), pltpu.SMEM((SL + 1,), i32),
                                    dma(A), dma(A)],
                    cost_estimate=cost(6), name='attend')(tab, st, query, k_new, v_new, kc, vc, ko, vo, ao)

            def one_round(tag, c):
                st, s0, s1, pre, rc0, rc1, po0, po1, dxr, f0, f1, ko, vo, ao = c
                nrc0 = lax.ppermute(s0, 'dp', cw)
                nrc1 = lax.ppermute(s1, 'dp', ccw)
                npo0 = lax.ppermute(rc0, 'dp', swap)
                npo1 = lax.ppermute(rc1, 'dp', swap)
                st, s0, s1, part, dxs, f0, f1, ko, vo = pl.pallas_call(
                    functools.partial(round_kernel, NB), out_shape=(ST, chunk, chunk, both, cross, store, store, cache, cache),
                    in_specs=caches + [VMEM] * 6 + [ANY] * 4, out_specs=(SMEM,) + (VMEM,) * 4 + (ANY,) * 4,
                    input_output_aliases={10: 5, 11: 6, 12: 7, 13: 8},
                    scratch_shapes=DMA * 3,
                    cost_estimate=cost(10), name='round')(tab, st, kc, vc, pre, rc0, rc1, po0, po1, dxr, f0, f1, ko, vo)
                npre = lax.ppermute(part, 'dp', swap)
                ndxr = lax.ppermute(dxs, 'dp', swap)
                st, ko, vo, ao = attend(st, ko, vo, ao, False)
                if tag != TAGS[-1]:
                    s0, s1, npo0, npo1 = lax.optimization_barrier((s0, s1, npo0, npo1))
                return st, s0, s1, npre, nrc0, nrc1, npo0, npo1, ndxr, f0, f1, ko, vo, ao

            rounds = tab[ROUNDS]

            def body(c):
                return (c[0] + TURN,) + functools.reduce(lambda c, tag: one_round(tag, c), TAGS, c[1:])

            c = lax.while_loop(lambda c: c[0] < rounds, body,
                           (jnp.int32(0), st, s0, s1, pre, rc0, rc1, po0, po1, dxr, f0, f1, ko, vo, ao))
            _, st, _, _, _, rc0, rc1, po0, po1, dxr, _, _, ko, vo, ao = c

            def close(last, st, ko, vo, *ins):
                n = len(ins)
                return pl.pallas_call(
                    functools.partial(close_kernel, NB, last), out_shape=(ST, cache, cache),
                    in_specs=[SMEM, SMEM] + [VMEM] * n + [ANY] * 2, out_specs=(SMEM, ANY, ANY),
                    input_output_aliases={n + 2: 1, n + 3: 2},
                    scratch_shapes=DMA,
                    name='close_last' if last else 'close')(tab, st, *ins, ko, vo)

            lpo0 = lax.ppermute(rc0, 'dp', swap)
            lpo1 = lax.ppermute(rc1, 'dp', swap)
            st, ko, vo = close(False, st, ko, vo, rc0, rc1, po0, po1, dxr)
            st, ko, vo = close(True, st, ko, vo, lpo0, lpo1)
            st, ko, vo, ao = attend(st, ko, vo, ao, True)
            return ao, ko, vo

        ao, ko, vo = lax.switch(tab[PICK], [functools.partial(run, size) for size in SIZES])
        return ao, ko.reshape(k_cache.shape), vo.reshape(v_cache.shape), lens_out

    row_spec = P('dp')
    return jax.shard_map(local, mesh=mesh, in_specs=(row_spec, row_spec, row_spec, row_spec, P(), row_spec, row_spec),
                         out_specs=(row_spec, row_spec, row_spec, row_spec), check_vma=False)
```

```python
import functools

import jax
import jax.numpy as jnp
from jax import lax
from jax.experimental import pallas as pl
from jax.experimental.pallas import tpu as pltpu
from jax.sharding import PartitionSpec as P


BP, SHIFT = 8, 3
SIZES = range(84, 56, -4)
NX = 32
A = 4
SL = 32
BL = 64
WIDE = 400
S0, S1, R0, R1, XS, XR, FREE = range(7)
RDY, RDX, MLEN, SRC, ROUNDS = range(FREE * WIDE, FREE * WIDE + 200, 40)
CORE, _, SHARE, DUMP = range(ROUNDS + 1, ROUNDS + 5)
TAB = ROUNDS + 8
FWD, NONE = 2, 3
TURN = 2
SEGS = 6
IDLE = 4 * SEGS
HALF = 1 << 16
FLOPS = 4000000
LOW = HALF - 1
U_PART, U_MERGE, U_OWN, U_POST, U_XS, U_XR = 0, 2, 4, 6, 8, 9
STEP, DONE, STATE = 24, 32, 64
END = HALF * HALF // 4
bf16 = jnp.bfloat16
f32 = jnp.float32
i32 = jnp.int32


def gray(c):
    return c ^ (c >> 1)


def lens_kernel(x, o, bsem, ssem, rsem):
    me = lax.axis_index('dp')
    barrier = pltpu.get_barrier_semaphore()
    for k in range(1, 8):
        pl.semaphore_signal(barrier, inc=1, device_id=(lax.rem(me + k, 8),), device_id_type=pl.DeviceIdType.MESH)
    pl.semaphore_wait(barrier, 7)
    here = pltpu.make_async_copy(x, o.at[me], bsem)
    here.start()
    sends = []
    for k in range(1, 8):
        c = pltpu.make_async_remote_copy(src_ref=x, dst_ref=o.at[me], send_sem=ssem.at[k], recv_sem=rsem.at[k],
                                         device_id=(lax.rem(me + k, 8),), device_id_type=pl.DeviceIdType.MESH)
        c.start()
        sends.append(c)
    here.wait()
    for c in sends:
        c.wait()


def plan_kernel(me_ref, dest_ref, len_ref, tab, lens_out, state, rounds_out, pick_out, nbv, kindv, todo, near, load, one, two, three, cur):
    me = me_ref[0]
    zero = me - me
    for i in range(17):
        for ref in (one, two, three):
            ref[i] = zero
    tab[CORE] = me & 1
    for j in range(SL):
        tab[RDY + j] = zero
        tab[RDX + j] = zero

    def first(i, c):
        size = len_ref[i >> 5, 0, i & 31]
        d = dest_ref[i]
        nb = (size + (BP - 1)) >> SHIFT
        ra = gray(i >> 6)
        delta = (gray(d >> 6) - ra) & 3
        nbv[i] = nb
        beside = (delta & 1) == 1
        ccw = delta == 3
        kindv[i] = jnp.where(beside, jnp.where(ccw, 4, 1), 0)
        todo[c[0]] = i
        near[c[1]] = i
        cross = (delta == 0) & ((i >> 5) != (d >> 5))
        slot = jnp.where(beside, jnp.where(ccw, 4, 0) + ra, jnp.where(cross, 9 + (i >> 5), 8))
        one[slot] = one[slot] + nb + HALF
        mine = jnp.where((d >> 5) == me, d & 31, SL)
        tab[MLEN + mine] = size
        tab[SRC + mine] = jnp.where((i >> 5) == me, i & 31, -1)
        return c[0] + jnp.where(delta == 2, 1, 0), c[1] + jnp.where(beside, 1, 0)

    far, side = lax.fori_loop(0, 8 * SL, first, (zero, zero), unroll=8)
    for i in range(8):
        load[i] = one[i] & LOW

    def lens(j, c):
        lens_out[j] = tab[MLEN + j] + 1
        return c

    lax.fori_loop(0, SL, lens, 0, unroll=8)

    def hops(x):
        return (x, (x + 1) & 3, (x + 2) & 3), (4 + x, 4 + ((x - 1) & 3), 4 + ((x + 2) & 3))

    def choose(n, c):
        i = todo[n]
        nb = nbv[i]
        (a1, a2, _), (b1, b2, _) = hops(gray(i >> 6))
        la1, la2, lb1, lb2 = load[a1], load[a2], load[b1], load[b2]
        la, lb = jnp.maximum(la1, la2), jnp.maximum(lb1, lb2)
        cw = (la < lb) | ((la == lb) & (la1 + la2 <= lb1 + lb2))
        x1, x2 = jnp.where(cw, a1, b1), jnp.where(cw, a2, b2)
        load[x1] = load[x1] + nb
        load[x2] = load[x2] + nb
        two[x1] = two[x1] + nb + HALF
        kindv[i] = jnp.where(cw, 2, 5)
        return c

    lax.fori_loop(0, far, choose, 0)

    def largest():
        return functools.reduce(jnp.maximum, [load[x] for x in range(8)])

    cur[0] = largest()

    def detour(n, c):
        i = near[n]
        nb = nbv[i]
        cws, ccws = hops(gray(i >> 6))
        cw = kindv[i] == 1
        a = jnp.where(cw, cws[0], ccws[0])
        b = [jnp.where(cw, y, x) for x, y in zip(cws, ccws)]
        lb = [load[x] for x in b]
        la = load[a]

        @pl.when((la - nb >= functools.reduce(jnp.maximum, lb) + nb) & (la * 10 >= cur[0] * 9))
        def _():
            load[a] = la - nb
            one[a] = one[a] - nb - HALF
            for x, l in zip(b, lb):
                load[x] = l + nb
            three[b[0]] = three[b[0]] + nb + HALF
            kindv[i] = jnp.where(cw, 6, 3)
            cur[0] = largest()

        return c

    lax.fori_loop(0, side, detour, 0)

    def again(n, c):
        i = todo[n]
        nb = nbv[i]
        cws, ccws = hops(gray(i >> 6))
        cw = kindv[i] == 2
        a = [jnp.where(cw, x, y) for x, y in zip(cws[:2], ccws)]
        b = [jnp.where(cw, y, x) for x, y in zip(cws[:2], ccws)]
        la, lb = [load[x] for x in a], [load[x] for x in b]

        @pl.when(jnp.maximum(*lb) + nb < jnp.maximum(*la))
        def _():
            for x, l in zip(a + b, [l - nb for l in la] + [l + nb for l in lb]):
                load[x] = l
            two[a[0]] = two[a[0]] - nb - HALF
            two[b[0]] = two[b[0]] + nb + HALF
            kindv[i] = jnp.where(cw, 5, 2)

        return c

    lax.fori_loop(0, far, again, 0)

    def back(d, x, n):
        return 4 * d + ((x + (2 * d - 1) * n) & 3)

    def own_of(d, x):
        x = back(d, x, 0)
        return one[x] + two[x] + three[x]

    def link(d, x, size):
        up, up2 = back(d, x, 1), back(d, x, 2)
        own = own_of(d, x)
        fwd, fwd2 = two[up] + three[up], three[up2]
        start = jnp.maximum(own & LOW, jnp.where(fwd > 0, 2 * size, 0))
        own_up = own_of(d, up & 3)
        start_up = jnp.maximum(own_up & LOW, jnp.where(two[up2] + three[up2] > 0, 2 * size, 0))
        start2 = jnp.maximum(start + (fwd & LOW), jnp.where(fwd2 > 0, start_up + 2 * size, 0))
        return own, fwd, fwd2, start, start_up, start2

    cross = zero
    for d in range(8):
        cross = jnp.maximum(cross, ((one[9 + d] & LOW) + NX - 1) // NX)
    best, pick, turns, chunk = zero + END, zero, zero, zero
    all_links = [(two[x] + three[x], three[x], one[x] + two[x] + three[x]) for x in range(8)]
    parts = []
    for d in range(2):
        ring = all_links[4 * d:][:4][::1 - 2 * d]
        for x in range(4):
            (_, _, own), (fwd, _, own_up), (fwd_up, fwd2, _) = ring[x], ring[x - 1], ring[x - 2]
            parts.append([n & LOW for n in (own, fwd, own_up, fwd_up, fwd2)])
    for o, size in enumerate(SIZES):
        longest = zero
        for own, fwd, own_up, fwd_up, fwd2 in parts:
            wait, wait_up = jnp.where(fwd > 0, 2 * size, 0), jnp.where(fwd_up > 0, 2 * size, 0)
            total = jnp.maximum(own, wait) + fwd
            late = jnp.maximum(own_up, wait_up) + 2 * size
            longest = jnp.maximum(longest, jnp.where(fwd2 > 0, jnp.maximum(total, late) + fwd2, total))
        trips = (jnp.maximum((longest + size - 1) // size, cross) + TURN - 1) // TURN
        price = trips * (TURN * size + 7)
        better = price < best
        best, pick, turns, chunk = [jnp.where(better, n, o) for n, o in (
            (price, best), (o, pick), (trips * TURN, turns), (size, chunk))]
    rounds_out[0] = turns
    pick_out[0] = pick
    for i in range(STATE):
        state[i] = zero
    tab[SHARE] = jnp.minimum(SL // jnp.maximum(turns - TURN, 1) + 1, A)

    x0 = gray(me >> 1)
    left, right, opposite = (x0 - 1) & 3, (x0 + 1) & 3, (x0 + 2) & 3
    shift = []
    for lid, d, x in ((S0, 0, x0), (S1, 1, x0), (R0, 0, left), (R1, 1, right)):
        own, fwd, fwd2, start, _, start2 = link(d, x, chunk)
        here, up = back(d, x, 0), back(d, x, 1)
        base = zero + lid * WIDE
        wide = 2 * (three[here] >> 16)
        pad = base + 2 * (own >> 16)
        pad2 = pad + 2 + 2 * (fwd >> 16)
        tab[pad] = start - (own & LOW)
        tab[pad2] = start2 - start - (fwd & LOW)
        last = pad2 + 2 + 2 * (fwd2 >> 16)
        tab[last] = zero + END
        for a in (pad, pad2, last):
            tab[a + 1] = zero + NONE * HALF
        hop3, hop2 = three[here], two[here]
        segs = ((base, zero), (base + wide, hop3 & LOW), (base + wide + 2 * (hop2 >> 16), (hop3 + hop2) & LOW),
                (pad + 2, start), (pad + 2 + 2 * (three[up] >> 16), start + (three[up] & LOW)), (pad2 + 2, start2))
        for k, (where, pos) in enumerate(segs):
            cur[SEGS * lid + k] = where * HALF + pos
        shift.append(((hop3 + hop2) & LOW) - start)
    cur[IDLE] = zero + DUMP * HALF

    def append(seg, hit, nb, code_at):
        seg = jnp.where(hit, seg, IDLE)
        c = cur[seg]
        a, p = c >> 16, c & LOW
        code = code_at(p)
        tab[a] = nb
        tab[a + 1] = code
        cur[seg] = c + jnp.where(hit, 2 * HALF + nb, 0)
        return p + nb, code

    def source(s, c):
        i = (me >> 1) * 2 * SL + s
        kind = kindv[i]
        seg = jnp.where(kind > 3, SEGS + 6, 3) - kind
        append(seg, kind > 0, nbv[i], lambda p: ((s >> 5) << 16) + (s & 31) * BL)
        return c

    lax.fori_loop(0, 2 * SL, source, 0, unroll=4)

    def visit(i, hit, seg, goes_on, seg_on, ahead):
        nb = nbv[i]
        dst = dest_ref[i]
        home = (((dst >> 5) & 1) << 16) + (dst & 31) * BL
        end, code = append(seg, hit, nb, lambda p: jnp.where(goes_on, FWD * HALF + p + ahead, home))
        append(seg_on, goes_on, nb, lambda p: code)
        mine = hit & ((dst >> 5) == me) & jnp.logical_not(goes_on)
        tab[RDY + jnp.where(mine, dst & 31, SL)] = end

    for d, x in ((0, left), (1, right)):
        def beside(s, c):
            i = gray(x) * 2 * SL + s
            kind = kindv[i]
            h = kind - 3 * d
            along = (h > 0) & (h <= 3)
            about = kind == 6 - 3 * d
            seg = jnp.where(along, SEGS * (R0 + d) + 3 - h, SEGS * (R1 - d) + 5)
            visit(i, along | about, seg, along & (h > 1), SEGS * d + 6 - h, 0)
            return c

        lax.fori_loop(0, 2 * SL, beside, 0, unroll=2)

    def across(s, c):
        i = gray(opposite) * 2 * SL + s
        kind = kindv[i]
        d = jnp.where(kind > 3, 1, 0)
        h = kind - 3 * d
        seg = SEGS * (R0 + d) + jnp.where(h == 3, 3, 4)
        visit(i, h > 1, seg, h == 3, SEGS * d + 5, jnp.where(d == 0, shift[R0], shift[R1]))
        return c

    lax.fori_loop(0, 2 * SL, across, 0, unroll=2)

    for lid, sender, receiver in ((XS, me, me ^ 1), (XR, me ^ 1, me)):
        def cross_list(s, c):
            a, pos = c
            i = sender * SL + s
            nb = nbv[i]
            dst = dest_ref[i]
            hit = (dst >> 5) == receiver
            tab[a] = nb
            tab[a + 1] = (s if lid == XS else dst & 31) * BL
            pos = pos + jnp.where(hit, nb, 0)
            if lid == XR:
                tab[RDX + jnp.where(hit, dst & 31, SL)] = pos
            return a + jnp.where(hit, 2, 0), pos

        a, _ = lax.fori_loop(0, SL, cross_list, (zero + lid * WIDE, zero), unroll=2)
        tab[a] = zero + END
        tab[a + 1] = zero + NONE * HALF


class Mover:
    def __init__(self, tab, st_in, st, size):
        self.tab, self.st, self.size = tab, st, size
        self.core = tab[CORE]

        def cp(i, _):
            st[i] = st_in[i]
            return 0

        lax.fori_loop(0, STATE, cp, 0)

    def walk(self, lid, use, n, fn):
        tab, st = self.tab, self.st
        base = lid * WIDE

        def body(c):
            p, item, off, cnt = c
            width = tab[base + 2 * item]
            code = tab[base + 2 * item + 1]
            take = jnp.minimum(n - p, width - off)
            cnt = cnt + fn(p, take, code >> 16, (code & LOW) + off)
            off = off + take
            adv = off >= width
            return p + take, jnp.where(adv, item + 1, item), jnp.where(adv, 0, off), cnt

        c0 = (jnp.int32(0), st[2 * use], st[2 * use + 1], jnp.int32(0))
        _, item, off, cnt = lax.while_loop(lambda c: c[0] < n, body, c0)
        st[2 * use] = item
        st[2 * use + 1] = off
        return cnt

    @staticmethod
    def drain(cnt, ref, sem):
        @pl.when(cnt > 0)
        def _():
            part = ref.at[pl.ds(0, cnt)]
            pltpu.make_async_copy(part, part, sem).wait()

    def partial(self, d, kc, vc, buf, sem):
        core = self.core

        def fn(p, take, kind, idx):
            mine = kind == core

            @pl.when(mine & (core == 0))
            def _():
                pltpu.make_async_copy(vc.at[pl.ds(idx, take)], buf.at[pl.ds(p, take)], sem).start()

            @pl.when(mine & (core == 1))
            def _():
                pltpu.make_async_copy(kc.at[pl.ds(idx, take)], buf.at[pl.ds(p, take)], sem).start()

            return jnp.where(mine, take, 0)

        return self.walk(S0 + d, U_PART + d, self.size, fn)

    def merge(self, d, kc, vc, pre, fwd, buf, sem):
        core = self.core

        def fn(p, take, kind, idx):
            mine = kind == core

            @pl.when(mine & (core == 0))
            def _():
                pltpu.make_async_copy(kc.at[pl.ds(idx, take)], buf.at[pl.ds(p, take)], sem).start()

            @pl.when(mine & (core == 1))
            def _():
                pltpu.make_async_copy(vc.at[pl.ds(idx, take)], buf.at[pl.ds(p, take)], sem).start()

            @pl.when(kind == 1 - core)
            def _():
                pltpu.make_async_copy(pre.at[d, pl.ds(p, take)], buf.at[pl.ds(p, take)], sem).start()

            if fwd is not None:
                @pl.when(kind == FWD)
                def _():
                    pltpu.make_async_copy(fwd.at[pl.ds(idx, take)], buf.at[pl.ds(p, take)], sem).start()
            return jnp.where(kind < NONE, take, 0)

        return self.walk(S0 + d, U_MERGE + d, self.size, fn)

    def cross_send(self, kc, vc, buf, sem):
        def fn(p, take, kind, idx):
            @pl.when(kind == 0)
            def _():
                pltpu.make_async_copy(kc.at[pl.ds(idx, take)], buf.at[0, pl.ds(p, take)], sem).start()
                pltpu.make_async_copy(vc.at[pl.ds(idx, take)], buf.at[1, pl.ds(p, take)], sem).start()

            return jnp.where(kind == 0, 2 * take, 0)

        return self.walk(XS, U_XS, NX, fn)

    def cross_recv(self, n, ko, vo, buf, sem):
        def fn(p, take, kind, idx):
            @pl.when(kind == 0)
            def _():
                pltpu.make_async_copy(buf.at[0, pl.ds(p, take)], ko.at[pl.ds(idx, take)], sem).start()
                pltpu.make_async_copy(buf.at[1, pl.ds(p, take)], vo.at[pl.ds(idx, take)], sem).start()

            return jnp.where(kind == 0, 2 * take, 0)

        return self.walk(XR, U_XR, n, fn)

    def unpack(self, d, use, n, flip, ko, vo, fwd, buf, sem):
        core = self.core
        plane = 1 - core if flip else core

        def fn(p, take, kind, idx):
            mine = kind == core

            @pl.when(mine & (plane == 0))
            def _():
                pltpu.make_async_copy(buf.at[pl.ds(p, take)], ko.at[pl.ds(idx, take)], sem).start()

            @pl.when(mine & (plane == 1))
            def _():
                pltpu.make_async_copy(buf.at[pl.ds(p, take)], vo.at[pl.ds(idx, take)], sem).start()

            cnt = jnp.where(mine, take, 0)
            if fwd is not None:
                @pl.when(kind == FWD)
                def _():
                    pltpu.make_async_copy(buf.at[pl.ds(p, take)], fwd.at[pl.ds(idx, take)], sem).start()

                cnt = cnt + jnp.where(kind == FWD, take, 0)
            return cnt

        return self.walk(R0 + d, use + d, n, fn)


def open_kernel(NB, tab, st_in, kc, vc, st, part, sem):
    mv = Mover(tab, st_in, st, NB)
    mv.drain(sum(mv.partial(d, kc, vc, part.at[d], sem) for d in range(2)), kc, sem)


def open_merge_kernel(NB, tab, st_in, kc, vc, pre, st, send0, send1, sem):
    mv = Mover(tab, st_in, st, NB)
    mv.drain(sum(mv.merge(d, kc, vc, pre, None, buf, sem) for d, buf in enumerate((send0, send1))), kc, sem)


def stages(r, NB):
    return [jnp.where(r >= back, n, 0) for back, n in ((1, NB), (2, NB), (1, NX))]


def round_kernel(NB, tab, st_in, kc, vc, pre, rc0, rc1, po0, po1, dxr, f0i, f1i, koi, voi,
                 st, send0, send1, part, dxs, f0, f1, ko, vo, in_sem, out_sem, post_sem):
    mv = Mover(tab, st_in, st, NB)
    r = st_in[STEP]
    st[STEP] = r + 1
    n1, n2, nx = stages(r, NB)
    links = ((0, rc0, po0, f0, send0), (1, rc1, po1, f1, send1))
    mv.drain(sum(mv.unpack(d, U_OWN, n1, False, ko, vo, fwd, rc, out_sem) for d, rc, _, fwd, _ in links), kc, out_sem)
    cnt = sum(mv.merge(d, kc, vc, pre, fwd, send, in_sem) for d, _, _, fwd, send in links)
    late = sum(mv.unpack(d, U_POST, n2, True, ko, vo, None, po, post_sem) for d, _, po, _, _ in links)
    cnt += sum(mv.partial(d, kc, vc, part.at[d], in_sem) for d in range(2)) + mv.cross_send(kc, vc, dxs, in_sem)
    late += mv.cross_recv(nx, ko, vo, dxr, post_sem)
    mv.drain(cnt, kc, in_sem)
    mv.drain(late, kc, post_sem)


def close_kernel(NB, last, tab, st_in, *refs):
    if last:
        (po0, po1, koi, voi, st, ko, vo, sem) = refs
    else:
        (rc0, rc1, po0, po1, dxr, koi, voi, st, ko, vo, sem) = refs
    mv = Mover(tab, st_in, st, NB)
    r = st_in[STEP]
    st[STEP] = r + 1
    n1, n2, nx = stages(r, NB)
    cnt = sum(mv.unpack(d, U_POST, n2, True, ko, vo, None, po, sem) for d, po in enumerate((po0, po1)))
    if not last:
        cnt += sum(mv.unpack(d, U_OWN, n1, False, ko, vo, None, rc, sem) for d, rc in enumerate((rc0, rc1)))
        cnt += mv.cross_recv(nx, ko, vo, dxr, sem)
    mv.drain(cnt, ko, sem)


def attn_kernel(NB, last, tab, st_in, q, kn, vn, kc, vc, koi, voi, aoi, st, ko, vo, ao,
                kb, vb, ob, scores, sel, lsem, wsem):
    def cp(i, _):
        st[i] = st_in[i]
        return 0

    lax.fori_loop(0, STATE, cp, 0)
    share = SL if last else tab[SHARE]
    link_end = jnp.maximum((st_in[STEP] - 2) * NB, 0)
    swap_end = jnp.maximum((st_in[STEP] - 1) * NX, 0)

    def load(a, j):
        s = tab[SRC + j]

        @pl.when(s >= 0)
        def _():
            pltpu.make_async_copy(kc.at[pl.ds(s * BL, BL)], kb.at[a], lsem.at[a]).start()
            pltpu.make_async_copy(vc.at[pl.ds(s * BL, BL)], vb.at[a], lsem.at[a]).start()

        @pl.when(s < 0)
        def _():
            pltpu.make_async_copy(ko.at[pl.ds(j * BL, BL)], kb.at[a], lsem.at[a]).start()
            pltpu.make_async_copy(vo.at[pl.ds(j * BL, BL)], vb.at[a], lsem.at[a]).start()

    def compute(a, j):
        pltpu.make_async_copy(kb.at[a], kb.at[a], lsem.at[a]).wait()
        pltpu.make_async_copy(vb.at[a], vb.at[a], lsem.at[a]).wait()
        m = tab[MLEN + j]
        b0 = m >> SHIFT
        row = lax.broadcasted_iota(i32, BLOCK, 0) >> 3
        for buf, new in ((kb, kn), (vb, vn)):
            x = buf[a, b0].astype(f32)
            fresh = jnp.concatenate([new[j].astype(f32)] * BP, axis=0)
            t = b0 * BP + row
            buf[a, b0] = jnp.where(t < m, x, jnp.where(t == m, fresh, 0.0)).astype(bf16)

        def wipe(b, _):
            kb[a, b] = jnp.zeros(BLOCK, bf16)
            vb[a, b] = jnp.zeros(BLOCK, bf16)
            return 0

        lax.fori_loop(b0 + 1, BL, wipe, 0)
        pieces = (m >> 7) + 1
        span = 128 // BP

        def rows(buf, c):
            return buf[a, pl.ds(c * span, span)].reshape(-1, 128)

        def score(c, top):
            sc = lax.dot_general(q[j], rows(kb, c), (((1,), (1,)), ((), ())), preferred_element_type=f32) * (128 ** -0.5)
            col = lax.broadcasted_iota(i32, sc.shape, 1)
            head = lax.broadcasted_iota(i32, sc.shape, 0) // 3
            ok = ((col & 7) == head) & ((col >> 3) <= m - c * 128)
            sc = jnp.where(ok, sc, -1e30)
            scores[c] = sc
            return jnp.maximum(top, jnp.max(sc, axis=1, keepdims=True))

        top = lax.fori_loop(0, pieces, score, jnp.full((24, 1), -1e30, f32))

        def weigh(c, carry):
            tot, acc = carry
            w = jnp.exp(scores[c] - top)
            acc = acc + lax.dot_general(w.astype(bf16), rows(vb, c), (((1,), (0,)), ((), ())), preferred_element_type=f32)
            return tot + jnp.sum(w, axis=1, keepdims=True), acc

        tot, acc = lax.fori_loop(0, pieces, weigh, (jnp.zeros((24, 1), f32), jnp.zeros((24, 128), f32)))
        ob[a] = (acc / tot).astype(bf16)
        for src, dst in writes(a, j):
            pltpu.make_async_copy(src, dst, wsem.at[a]).start()

    def writes(a, j):
        bw = jnp.where(tab[SRC + j] >= 0, 0, tab[MLEN + j] >> SHIFT)
        tail, home = pl.ds(bw, BL - bw), pl.ds(j * BL + bw, BL - bw)
        return (kb.at[a, tail], ko.at[home]), (vb.at[a, tail], vo.at[home]), (ob.at[a], ao.at[j])

    def settle(k):
        a, j = k & (A - 1), sel[k]
        for src, dst in writes(a, j):
            pltpu.make_async_copy(src, dst, wsem.at[a]).wait()

    def pick(j, n):
        hit = (st[DONE + j] == 0) & (tab[RDY + j] <= link_end) & (tab[RDX + j] <= swap_end) & (n < share)
        sel[n] = j
        st[DONE + j] = jnp.where(hit, 1, st[DONE + j])
        return n + jnp.where(hit, 1, 0)

    n = lax.fori_loop(0, SL, pick, jnp.int32(0))

    def early(k, c):
        load(k, sel[k])
        return c

    lax.fori_loop(0, jnp.minimum(n, A - 1), early, 0)

    def step(k, c):
        compute(k & (A - 1), sel[k])
        later = k + A - 1

        @pl.when(later < n)
        def _():
            @pl.when(k >= 1)
            def _():
                settle(k - 1)

            load(later & (A - 1), sel[later])

        return c

    lax.fori_loop(0, n, step, 0)

    def wind_up(k, c):
        settle(k)
        return c

    lax.fori_loop(jnp.maximum(n - A, 0), n, wind_up, 0)


SMEM = pl.BlockSpec(memory_space=pltpu.SMEM)
VMEM = pl.BlockSpec(memory_space=pltpu.VMEM)
ANY = pl.BlockSpec(memory_space=pl.ANY)
BLOCK = (8 * BP, 128)


def sds(shape, dtype=bf16):
    return jax.ShapeDtypeStruct(shape, dtype)


def dma(n):
    return pltpu.SemaphoreType.DMA((n,))


def buf(*lead):
    return pltpu.VMEM(lead + BLOCK, bf16)


def cost(us):
    return pl.CostEstimate(flops=us * FLOPS, bytes_accessed=us * FLOPS, transcendentals=0)


ST = sds((STATE,), i32)
DMA = [pltpu.SemaphoreType.DMA]
TAGS = ('ra', 'rb')


def solution(mesh):
    group = mesh.shape['dp']
    ring = [0, 1, 3, 2]
    cw = [(ring[k] * 2 + c, ring[(k + 1) % 4] * 2 + c) for k in range(4) for c in range(2)]
    ccw = [(b, a) for a, b in cw]
    swap = [(d, d ^ 1) for d in range(group)]

    def local(query, k_cache, v_cache, cache_lens, dest_slot, k_new, v_new):
        kc = k_cache.reshape((SL * BL,) + BLOCK)
        vc = v_cache.reshape((SL * BL,) + BLOCK)
        lens_all = pl.pallas_call(
            lens_kernel, out_shape=sds((8, 1, SL), i32), in_specs=[VMEM], out_specs=VMEM,
            scratch_shapes=[pltpu.SemaphoreType.DMA, dma(8), dma(8)],
            compiler_params=pltpu.CompilerParams(collective_id=0, has_side_effects=True),
            name='lens')(cache_lens.reshape(1, SL))
        me = jnp.full((1,), lax.axis_index('dp'), i32)
        tab, lens_out, state, rounds, pick = pl.pallas_call(
            plan_kernel, out_shape=[sds((n,), i32) for n in (TAB, SL, STATE, 1, 1)], in_specs=[SMEM] * 3, out_specs=[SMEM] * 5,
            scratch_shapes=[pltpu.SMEM((8 * SL + 1,), i32)] * 4 + [pltpu.SMEM((IDLE + 1,), i32)] * 5,
            name='plan')(me, dest_slot, lens_all)

        def run(NB):
            def nothing(*refs):
                pass

            chunk, both, cross = sds((NB,) + BLOCK), sds((2, NB) + BLOCK), sds((2, NX) + BLOCK)
            cache, store = sds((SL * BL,) + BLOCK), sds((4 * SL * BL,) + BLOCK)
            ko, vo, ao, f0, f1, rc0, rc1, po0, po1, dxr = pl.pallas_call(
                nothing, out_shape=(cache, cache, sds((SL, 24, 128)), store, store, chunk, chunk, chunk, chunk, cross),
                out_specs=(ANY,) * 10, name='blank')()

            st = state
            caches = [SMEM, SMEM, ANY, ANY]

            def opened(st):
                return pl.pallas_call(
                    functools.partial(open_kernel, NB), out_shape=(ST, both), in_specs=caches, out_specs=(SMEM, VMEM),
                    scratch_shapes=DMA, name='open')(tab, st, kc, vc)

            st, part = opened(st)
            pre = lax.ppermute(part, 'dp', swap)
            st, part = opened(st)
            pre1 = lax.ppermute(part, 'dp', swap)
            st, s0, s1 = pl.pallas_call(
                functools.partial(open_merge_kernel, NB), out_shape=(ST, chunk, chunk), in_specs=caches + [VMEM],
                out_specs=(SMEM, VMEM, VMEM), scratch_shapes=DMA,
                name='open_merge')(tab, st, kc, vc, pre)
            pre = pre1

            def attend(st, ko, vo, ao, last):
                return pl.pallas_call(
                    functools.partial(attn_kernel, NB, last),
                    out_shape=(ST, cache, cache, sds((SL, 24, 128))),
                    in_specs=[SMEM, SMEM, VMEM, VMEM, VMEM, ANY, ANY, ANY, ANY, ANY], out_specs=(SMEM, ANY, ANY, ANY),
                    input_output_aliases={7: 1, 8: 2, 9: 3},
                    scratch_shapes=[buf(A, BL), buf(A, BL), pltpu.VMEM((A, 24, 128), bf16),
                                    pltpu.VMEM((4, 24, 1024), f32), pltpu.SMEM((SL + 1,), i32),
                                    dma(A), dma(A)],
                    cost_estimate=cost(6), name='attend')(tab, st, query, k_new, v_new, kc, vc, ko, vo, ao)

            def one_round(tag, c):
                st, s0, s1, pre, rc0, rc1, po0, po1, dxr, f0, f1, ko, vo, ao = c
                nrc0 = lax.ppermute(s0, 'dp', cw)
                nrc1 = lax.ppermute(s1, 'dp', ccw)
                npo0 = lax.ppermute(rc0, 'dp', swap)
                npo1 = lax.ppermute(rc1, 'dp', swap)
                st, s0, s1, part, dxs, f0, f1, ko, vo = pl.pallas_call(
                    functools.partial(round_kernel, NB), out_shape=(ST, chunk, chunk, both, cross, store, store, cache, cache),
                    in_specs=caches + [VMEM] * 6 + [ANY] * 4, out_specs=(SMEM,) + (VMEM,) * 4 + (ANY,) * 4,
                    input_output_aliases={10: 5, 11: 6, 12: 7, 13: 8},
                    scratch_shapes=DMA * 3,
                    cost_estimate=cost(10), name='round')(tab, st, kc, vc, pre, rc0, rc1, po0, po1, dxr, f0, f1, ko, vo)
                npre = lax.ppermute(part, 'dp', swap)
                ndxr = lax.ppermute(dxs, 'dp', swap)
                st, ko, vo, ao = attend(st, ko, vo, ao, False)
                if tag != TAGS[-1]:
                    s0, s1, npo0, npo1 = lax.optimization_barrier((s0, s1, npo0, npo1))
                return st, s0, s1, npre, nrc0, nrc1, npo0, npo1, ndxr, f0, f1, ko, vo, ao

            turns = rounds[0]

            def body(c):
                return (c[0] + TURN,) + functools.reduce(lambda c, tag: one_round(tag, c), TAGS, c[1:])

            c = lax.while_loop(lambda c: c[0] < turns, body,
                           (jnp.int32(0), st, s0, s1, pre, rc0, rc1, po0, po1, dxr, f0, f1, ko, vo, ao))
            _, st, _, _, _, rc0, rc1, po0, po1, dxr, _, _, ko, vo, ao = c

            def close(last, st, ko, vo, *ins):
                n = len(ins)
                return pl.pallas_call(
                    functools.partial(close_kernel, NB, last), out_shape=(ST, cache, cache),
                    in_specs=[SMEM, SMEM] + [VMEM] * n + [ANY] * 2, out_specs=(SMEM, ANY, ANY),
                    input_output_aliases={n + 2: 1, n + 3: 2},
                    scratch_shapes=DMA,
                    name='close_last' if last else 'close')(tab, st, *ins, ko, vo)

            lpo0 = lax.ppermute(rc0, 'dp', swap)
            lpo1 = lax.ppermute(rc1, 'dp', swap)
            st, ko, vo = close(False, st, ko, vo, rc0, rc1, po0, po1, dxr)
            st, ko, vo = close(True, st, ko, vo, lpo0, lpo1)
            st, ko, vo, ao = attend(st, ko, vo, ao, True)
            return ao, ko, vo

        ao, ko, vo = lax.switch(pick[0], [functools.partial(run, size) for size in SIZES])
        return ao, ko.reshape(k_cache.shape), vo.reshape(v_cache.shape), lens_out

    row_spec = P('dp')
    return jax.shard_map(local, mesh=mesh, in_specs=(row_spec, row_spec, row_spec, row_spec, P(), row_spec, row_spec),
                         out_specs=(row_spec, row_spec, row_spec, row_spec), check_vma=False)
```

```python
import functools

import jax
import jax.numpy as jnp
from jax import lax
from jax.experimental import pallas as pl
from jax.experimental.pallas import tpu as pltpu
from jax.sharding import PartitionSpec as P


BP, SHIFT = 8, 3
SIZES = range(88, 60, -4)
NX = 32
A = 4
SL = 32
BL = 64
WIDE = 400
S0, S1, R0, R1, XS, XR, FREE = range(7)
RDY, RDX, MLEN, SRC, ROUNDS = range(FREE * WIDE, FREE * WIDE + 200, 40)
CORE, _, SHARE, DUMP = range(ROUNDS + 1, ROUNDS + 5)
TAB = ROUNDS + 8
FWD, NONE = 2, 3
TURN = 2
SEGS = 6
IDLE = 4 * SEGS
HALF = 1 << 16
FLOPS = 4000000
LOW = HALF - 1
U_PART, U_MERGE, U_OWN, U_POST, U_XS, U_XR = 0, 2, 4, 6, 8, 9
STEP, DONE, STATE = 24, 32, 64
END = HALF * HALF // 4
bf16 = jnp.bfloat16
f32 = jnp.float32
i32 = jnp.int32


def gray(c):
    return c ^ (c >> 1)


def lens_kernel(x, o, bsem, ssem, rsem):
    me = lax.axis_index('dp')
    barrier = pltpu.get_barrier_semaphore()
    for k in range(1, 8):
        pl.semaphore_signal(barrier, inc=1, device_id=(lax.rem(me + k, 8),), device_id_type=pl.DeviceIdType.MESH)
    pl.semaphore_wait(barrier, 7)
    here = pltpu.make_async_copy(x, o.at[me], bsem)
    here.start()
    sends = []
    for k in range(1, 8):
        c = pltpu.make_async_remote_copy(src_ref=x, dst_ref=o.at[me], send_sem=ssem.at[k], recv_sem=rsem.at[k],
                                         device_id=(lax.rem(me + k, 8),), device_id_type=pl.DeviceIdType.MESH)
        c.start()
        sends.append(c)
    here.wait()
    for c in sends:
        c.wait()


def plan_kernel(me_ref, dest_ref, len_ref, tab, lens_out, state, rounds_out, pick_out, nbv, kindv, todo, near, load, one, two, three, cur):
    me = me_ref[0]
    zero = me - me
    for i in range(17):
        for ref in (one, two, three):
            ref[i] = zero
    tab[CORE] = me & 1
    for j in range(SL):
        tab[RDY + j] = zero
        tab[RDX + j] = zero

    def first(i, c):
        size = len_ref[i >> 5, 0, i & 31]
        d = dest_ref[i]
        nb = (size + (BP - 1)) >> SHIFT
        ra = gray(i >> 6)
        delta = (gray(d >> 6) - ra) & 3
        nbv[i] = nb
        beside = (delta & 1) == 1
        ccw = delta == 3
        kindv[i] = jnp.where(beside, jnp.where(ccw, 4, 1), 0)
        todo[c[0]] = i
        near[c[1]] = i
        cross = (delta == 0) & ((i >> 5) != (d >> 5))
        slot = jnp.where(beside, jnp.where(ccw, 4, 0) + ra, jnp.where(cross, 9 + (i >> 5), 8))
        one[slot] = one[slot] + nb + HALF
        mine = jnp.where((d >> 5) == me, d & 31, SL)
        tab[MLEN + mine] = size
        tab[SRC + mine] = jnp.where((i >> 5) == me, i & 31, -1)
        return c[0] + jnp.where(delta == 2, 1, 0), c[1] + jnp.where(beside, 1, 0)

    far, side = lax.fori_loop(0, 8 * SL, first, (zero, zero), unroll=8)
    for i in range(8):
        load[i] = one[i] & LOW

    def lens(j, c):
        lens_out[j] = tab[MLEN + j] + 1
        return c

    lax.fori_loop(0, SL, lens, 0, unroll=8)

    def hops(x):
        return (x, (x + 1) & 3, (x + 2) & 3), (4 + x, 4 + ((x - 1) & 3), 4 + ((x + 2) & 3))

    def choose(n, c):
        i = todo[n]
        nb = nbv[i]
        (a1, a2, _), (b1, b2, _) = hops(gray(i >> 6))
        la1, la2, lb1, lb2 = load[a1], load[a2], load[b1], load[b2]
        la, lb = jnp.maximum(la1, la2), jnp.maximum(lb1, lb2)
        cw = (la < lb) | ((la == lb) & (la1 + la2 <= lb1 + lb2))
        x1, x2 = jnp.where(cw, a1, b1), jnp.where(cw, a2, b2)
        load[x1] = load[x1] + nb
        load[x2] = load[x2] + nb
        two[x1] = two[x1] + nb + HALF
        kindv[i] = jnp.where(cw, 2, 5)
        return c

    lax.fori_loop(0, far, choose, 0)

    def largest():
        return functools.reduce(jnp.maximum, [load[x] for x in range(8)])

    cur[0] = largest()

    def detour(n, c):
        i = near[n]
        nb = nbv[i]
        cws, ccws = hops(gray(i >> 6))
        cw = kindv[i] == 1
        a = jnp.where(cw, cws[0], ccws[0])
        b = [jnp.where(cw, y, x) for x, y in zip(cws, ccws)]
        lb = [load[x] for x in b]
        la = load[a]

        @pl.when((la - nb >= functools.reduce(jnp.maximum, lb) + nb) & (la * 10 >= cur[0] * 9))
        def _():
            load[a] = la - nb
            one[a] = one[a] - nb - HALF
            for x, l in zip(b, lb):
                load[x] = l + nb
            three[b[0]] = three[b[0]] + nb + HALF
            kindv[i] = jnp.where(cw, 6, 3)
            cur[0] = largest()

        return c

    lax.fori_loop(0, side, detour, 0)

    def again(n, c):
        i = todo[n]
        nb = nbv[i]
        cws, ccws = hops(gray(i >> 6))
        cw = kindv[i] == 2
        a = [jnp.where(cw, x, y) for x, y in zip(cws[:2], ccws)]
        b = [jnp.where(cw, y, x) for x, y in zip(cws[:2], ccws)]
        la, lb = [load[x] for x in a], [load[x] for x in b]

        @pl.when(jnp.maximum(*lb) + nb < jnp.maximum(*la))
        def _():
            for x, l in zip(a + b, [l - nb for l in la] + [l + nb for l in lb]):
                load[x] = l
            two[a[0]] = two[a[0]] - nb - HALF
            two[b[0]] = two[b[0]] + nb + HALF
            kindv[i] = jnp.where(cw, 5, 2)

        return c

    lax.fori_loop(0, far, again, 0)

    def back(d, x, n):
        return 4 * d + ((x + (2 * d - 1) * n) & 3)

    def own_of(d, x):
        x = back(d, x, 0)
        return one[x] + two[x] + three[x]

    def link(d, x, size):
        up, up2 = back(d, x, 1), back(d, x, 2)
        own = own_of(d, x)
        fwd, fwd2 = two[up] + three[up], three[up2]
        start = jnp.maximum(own & LOW, jnp.where(fwd > 0, 2 * size, 0))
        own_up = own_of(d, up & 3)
        start_up = jnp.maximum(own_up & LOW, jnp.where(two[up2] + three[up2] > 0, 2 * size, 0))
        start2 = jnp.maximum(start + (fwd & LOW), jnp.where(fwd2 > 0, start_up + 2 * size, 0))
        return own, fwd, fwd2, start, start_up, start2

    cross = zero
    for d in range(8):
        cross = jnp.maximum(cross, ((one[9 + d] & LOW) + NX - 1) // NX)
    best, pick, turns, chunk = zero + END, zero, zero, zero
    all_links = [(two[x] + three[x], three[x], one[x] + two[x] + three[x]) for x in range(8)]
    parts = []
    for d in range(2):
        ring = all_links[4 * d:][:4][::1 - 2 * d]
        for x in range(4):
            (_, _, own), (fwd, _, own_up), (fwd_up, fwd2, _) = ring[x], ring[x - 1], ring[x - 2]
            parts.append([n & LOW for n in (own, fwd, own_up, fwd_up, fwd2)])
    for o, size in enumerate(SIZES):
        longest = zero
        for own, fwd, own_up, fwd_up, fwd2 in parts:
            wait, wait_up = jnp.where(fwd > 0, 2 * size, 0), jnp.where(fwd_up > 0, 2 * size, 0)
            total = jnp.maximum(own, wait) + fwd
            late = jnp.maximum(own_up, wait_up) + 2 * size
            longest = jnp.maximum(longest, jnp.where(fwd2 > 0, jnp.maximum(total, late) + fwd2, total))
        trips = (jnp.maximum((longest + size - 1) // size, cross) + TURN - 1) // TURN
        price = trips * (TURN * size + 7)
        better = price < best
        best, pick, turns, chunk = [jnp.where(better, n, o) for n, o in (
            (price, best), (o, pick), (trips * TURN, turns), (size, chunk))]
    rounds_out[0] = turns
    pick_out[0] = pick
    for i in range(STATE):
        state[i] = zero
    tab[SHARE] = jnp.minimum(SL // jnp.maximum(turns - TURN, 1) + 1, A)

    x0 = gray(me >> 1)
    left, right, opposite = (x0 - 1) & 3, (x0 + 1) & 3, (x0 + 2) & 3
    shift = []
    for lid, d, x in ((S0, 0, x0), (S1, 1, x0), (R0, 0, left), (R1, 1, right)):
        own, fwd, fwd2, start, _, start2 = link(d, x, chunk)
        here, up = back(d, x, 0), back(d, x, 1)
        base = zero + lid * WIDE
        wide = 2 * (three[here] >> 16)
        pad = base + 2 * (own >> 16)
        pad2 = pad + 2 + 2 * (fwd >> 16)
        tab[pad] = start - (own & LOW)
        tab[pad2] = start2 - start - (fwd & LOW)
        last = pad2 + 2 + 2 * (fwd2 >> 16)
        tab[last] = zero + END
        for a in (pad, pad2, last):
            tab[a + 1] = zero + NONE * HALF
        hop3, hop2 = three[here], two[here]
        segs = ((base, zero), (base + wide, hop3 & LOW), (base + wide + 2 * (hop2 >> 16), (hop3 + hop2) & LOW),
                (pad + 2, start), (pad + 2 + 2 * (three[up] >> 16), start + (three[up] & LOW)), (pad2 + 2, start2))
        for k, (where, pos) in enumerate(segs):
            cur[SEGS * lid + k] = where * HALF + pos
        shift.append(((hop3 + hop2) & LOW) - start)
    cur[IDLE] = zero + DUMP * HALF

    def append(seg, hit, nb, code_at):
        seg = jnp.where(hit, seg, IDLE)
        c = cur[seg]
        a, p = c >> 16, c & LOW
        code = code_at(p)
        tab[a] = nb
        tab[a + 1] = code
        cur[seg] = c + jnp.where(hit, 2 * HALF + nb, 0)
        return p + nb, code

    def source(s, c):
        i = (me >> 1) * 2 * SL + s
        kind = kindv[i]
        seg = jnp.where(kind > 3, SEGS + 6, 3) - kind
        append(seg, kind > 0, nbv[i], lambda p: ((s >> 5) << 16) + (s & 31) * BL)
        return c

    lax.fori_loop(0, 2 * SL, source, 0, unroll=4)

    def visit(i, hit, seg, goes_on, seg_on, ahead):
        nb = nbv[i]
        dst = dest_ref[i]
        home = (((dst >> 5) & 1) << 16) + (dst & 31) * BL
        end, code = append(seg, hit, nb, lambda p: jnp.where(goes_on, FWD * HALF + p + ahead, home))
        append(seg_on, goes_on, nb, lambda p: code)
        mine = hit & ((dst >> 5) == me) & jnp.logical_not(goes_on)
        tab[RDY + jnp.where(mine, dst & 31, SL)] = end

    for d, x in ((0, left), (1, right)):
        def beside(s, c):
            i = gray(x) * 2 * SL + s
            kind = kindv[i]
            h = kind - 3 * d
            along = (h > 0) & (h <= 3)
            about = kind == 6 - 3 * d
            seg = jnp.where(along, SEGS * (R0 + d) + 3 - h, SEGS * (R1 - d) + 5)
            visit(i, along | about, seg, along & (h > 1), SEGS * d + 6 - h, 0)
            return c

        lax.fori_loop(0, 2 * SL, beside, 0, unroll=2)

    def across(s, c):
        i = gray(opposite) * 2 * SL + s
        kind = kindv[i]
        d = jnp.where(kind > 3, 1, 0)
        h = kind - 3 * d
        seg = SEGS * (R0 + d) + jnp.where(h == 3, 3, 4)
        visit(i, h > 1, seg, h == 3, SEGS * d + 5, jnp.where(d == 0, shift[R0], shift[R1]))
        return c

    lax.fori_loop(0, 2 * SL, across, 0, unroll=2)

    for lid, sender, receiver in ((XS, me, me ^ 1), (XR, me ^ 1, me)):
        def cross_list(s, c):
            a, pos = c
            i = sender * SL + s
            nb = nbv[i]
            dst = dest_ref[i]
            hit = (dst >> 5) == receiver
            tab[a] = nb
            tab[a + 1] = (s if lid == XS else dst & 31) * BL
            pos = pos + jnp.where(hit, nb, 0)
            if lid == XR:
                tab[RDX + jnp.where(hit, dst & 31, SL)] = pos
            return a + jnp.where(hit, 2, 0), pos

        a, _ = lax.fori_loop(0, SL, cross_list, (zero + lid * WIDE, zero), unroll=2)
        tab[a] = zero + END
        tab[a + 1] = zero + NONE * HALF


class Mover:
    def __init__(self, tab, st_in, st, size):
        self.tab, self.st, self.size = tab, st, size
        self.core = tab[CORE]

        def cp(i, _):
            st[i] = st_in[i]
            return 0

        lax.fori_loop(0, STATE, cp, 0)

    def walk(self, lid, use, n, fn):
        tab, st = self.tab, self.st
        base = lid * WIDE

        def body(c):
            p, item, off, cnt = c
            width = tab[base + 2 * item]
            code = tab[base + 2 * item + 1]
            take = jnp.minimum(n - p, width - off)
            cnt = cnt + fn(p, take, code >> 16, (code & LOW) + off)
            off = off + take
            adv = off >= width
            return p + take, jnp.where(adv, item + 1, item), jnp.where(adv, 0, off), cnt

        c0 = (jnp.int32(0), st[2 * use], st[2 * use + 1], jnp.int32(0))
        _, item, off, cnt = lax.while_loop(lambda c: c[0] < n, body, c0)
        st[2 * use] = item
        st[2 * use + 1] = off
        return cnt

    @staticmethod
    def drain(cnt, ref, sem):
        @pl.when(cnt > 0)
        def _():
            part = ref.at[pl.ds(0, cnt)]
            pltpu.make_async_copy(part, part, sem).wait()

    def partial(self, d, kc, vc, buf, sem):
        core = self.core

        def fn(p, take, kind, idx):
            mine = kind == core

            @pl.when(mine & (core == 0))
            def _():
                pltpu.make_async_copy(vc.at[pl.ds(idx, take)], buf.at[pl.ds(p, take)], sem).start()

            @pl.when(mine & (core == 1))
            def _():
                pltpu.make_async_copy(kc.at[pl.ds(idx, take)], buf.at[pl.ds(p, take)], sem).start()

            return jnp.where(mine, take, 0)

        return self.walk(S0 + d, U_PART + d, self.size, fn)

    def merge(self, d, kc, vc, pre, fwd, buf, sem):
        core = self.core

        def fn(p, take, kind, idx):
            mine = kind == core

            @pl.when(mine & (core == 0))
            def _():
                pltpu.make_async_copy(kc.at[pl.ds(idx, take)], buf.at[pl.ds(p, take)], sem).start()

            @pl.when(mine & (core == 1))
            def _():
                pltpu.make_async_copy(vc.at[pl.ds(idx, take)], buf.at[pl.ds(p, take)], sem).start()

            @pl.when(kind == 1 - core)
            def _():
                pltpu.make_async_copy(pre.at[d, pl.ds(p, take)], buf.at[pl.ds(p, take)], sem).start()

            if fwd is not None:
                @pl.when(kind == FWD)
                def _():
                    pltpu.make_async_copy(fwd.at[pl.ds(idx, take)], buf.at[pl.ds(p, take)], sem).start()
            return jnp.where(kind < NONE, take, 0)

        return self.walk(S0 + d, U_MERGE + d, self.size, fn)

    def cross_send(self, kc, vc, buf, sem):
        def fn(p, take, kind, idx):
            @pl.when(kind == 0)
            def _():
                pltpu.make_async_copy(kc.at[pl.ds(idx, take)], buf.at[0, pl.ds(p, take)], sem).start()
                pltpu.make_async_copy(vc.at[pl.ds(idx, take)], buf.at[1, pl.ds(p, take)], sem).start()

            return jnp.where(kind == 0, 2 * take, 0)

        return self.walk(XS, U_XS, NX, fn)

    def cross_recv(self, n, ko, vo, buf, sem):
        def fn(p, take, kind, idx):
            @pl.when(kind == 0)
            def _():
                pltpu.make_async_copy(buf.at[0, pl.ds(p, take)], ko.at[pl.ds(idx, take)], sem).start()
                pltpu.make_async_copy(buf.at[1, pl.ds(p, take)], vo.at[pl.ds(idx, take)], sem).start()

            return jnp.where(kind == 0, 2 * take, 0)

        return self.walk(XR, U_XR, n, fn)

    def unpack(self, d, use, n, flip, ko, vo, fwd, buf, sem):
        core = self.core
        plane = 1 - core if flip else core

        def fn(p, take, kind, idx):
            mine = kind == core

            @pl.when(mine & (plane == 0))
            def _():
                pltpu.make_async_copy(buf.at[pl.ds(p, take)], ko.at[pl.ds(idx, take)], sem).start()

            @pl.when(mine & (plane == 1))
            def _():
                pltpu.make_async_copy(buf.at[pl.ds(p, take)], vo.at[pl.ds(idx, take)], sem).start()

            cnt = jnp.where(mine, take, 0)
            if fwd is not None:
                @pl.when(kind == FWD)
                def _():
                    pltpu.make_async_copy(buf.at[pl.ds(p, take)], fwd.at[pl.ds(idx, take)], sem).start()

                cnt = cnt + jnp.where(kind == FWD, take, 0)
            return cnt

        return self.walk(R0 + d, use + d, n, fn)


def open_kernel(NB, tab, st_in, kc, vc, st, part, sem):
    mv = Mover(tab, st_in, st, NB)
    mv.drain(sum(mv.partial(d, kc, vc, part.at[d], sem) for d in range(2)), kc, sem)


def open_merge_kernel(NB, tab, st_in, kc, vc, pre, st, send0, send1, sem):
    mv = Mover(tab, st_in, st, NB)
    mv.drain(sum(mv.merge(d, kc, vc, pre, None, buf, sem) for d, buf in enumerate((send0, send1))), kc, sem)


def stages(r, NB):
    return [jnp.where(r >= back, n, 0) for back, n in ((1, NB), (2, NB), (1, NX))]


def round_kernel(NB, tab, st_in, kc, vc, pre, rc0, rc1, po0, po1, dxr, f0i, f1i, koi, voi,
                 st, send0, send1, part, dxs, f0, f1, ko, vo, in_sem, out_sem, post_sem):
    mv = Mover(tab, st_in, st, NB)
    r = st_in[STEP]
    st[STEP] = r + 1
    n1, n2, nx = stages(r, NB)
    links = ((0, rc0, po0, f0, send0), (1, rc1, po1, f1, send1))
    mv.drain(sum(mv.unpack(d, U_OWN, n1, False, ko, vo, fwd, rc, out_sem) for d, rc, _, fwd, _ in links), kc, out_sem)
    cnt = sum(mv.merge(d, kc, vc, pre, fwd, send, in_sem) for d, _, _, fwd, send in links)
    late = sum(mv.unpack(d, U_POST, n2, True, ko, vo, None, po, post_sem) for d, _, po, _, _ in links)
    cnt += sum(mv.partial(d, kc, vc, part.at[d], in_sem) for d in range(2)) + mv.cross_send(kc, vc, dxs, in_sem)
    late += mv.cross_recv(nx, ko, vo, dxr, post_sem)
    mv.drain(cnt, kc, in_sem)
    mv.drain(late, kc, post_sem)


def close_kernel(NB, last, tab, st_in, *refs):
    if last:
        (po0, po1, koi, voi, st, ko, vo, sem) = refs
    else:
        (rc0, rc1, po0, po1, dxr, koi, voi, st, ko, vo, sem) = refs
    mv = Mover(tab, st_in, st, NB)
    r = st_in[STEP]
    st[STEP] = r + 1
    n1, n2, nx = stages(r, NB)
    cnt = sum(mv.unpack(d, U_POST, n2, True, ko, vo, None, po, sem) for d, po in enumerate((po0, po1)))
    if not last:
        cnt += sum(mv.unpack(d, U_OWN, n1, False, ko, vo, None, rc, sem) for d, rc in enumerate((rc0, rc1)))
        cnt += mv.cross_recv(nx, ko, vo, dxr, sem)
    mv.drain(cnt, ko, sem)


def attn_kernel(NB, last, tab, st_in, q, kn, vn, kc, vc, koi, voi, aoi, st, ko, vo, ao,
                kb, vb, ob, sel, lsem, wsem):
    def cp(i, _):
        st[i] = st_in[i]
        return 0

    lax.fori_loop(0, STATE, cp, 0)
    share = SL if last else tab[SHARE]
    link_end = jnp.maximum((st_in[STEP] - 2) * NB, 0)
    swap_end = jnp.maximum((st_in[STEP] - 1) * NX, 0)

    def load(a, j):
        s = tab[SRC + j]

        @pl.when(s >= 0)
        def _():
            pltpu.make_async_copy(kc.at[pl.ds(s * BL, BL)], kb.at[a], lsem.at[a]).start()
            pltpu.make_async_copy(vc.at[pl.ds(s * BL, BL)], vb.at[a], lsem.at[a]).start()

        @pl.when(s < 0)
        def _():
            pltpu.make_async_copy(ko.at[pl.ds(j * BL, BL)], kb.at[a], lsem.at[a]).start()
            pltpu.make_async_copy(vo.at[pl.ds(j * BL, BL)], vb.at[a], lsem.at[a]).start()

    def compute(a, j):
        pltpu.make_async_copy(kb.at[a], kb.at[a], lsem.at[a]).wait()
        pltpu.make_async_copy(vb.at[a], vb.at[a], lsem.at[a]).wait()
        m = tab[MLEN + j]
        b0 = m >> SHIFT
        row = lax.broadcasted_iota(i32, BLOCK, 0) >> 3
        for buf, new in ((kb, kn), (vb, vn)):
            x = buf[a, b0].astype(f32)
            fresh = jnp.concatenate([new[j].astype(f32)] * BP, axis=0)
            t = b0 * BP + row
            buf[a, b0] = jnp.where(t < m, x, jnp.where(t == m, fresh, 0.0)).astype(bf16)

        def wipe(b, _):
            kb[a, b] = jnp.zeros(BLOCK, bf16)
            vb[a, b] = jnp.zeros(BLOCK, bf16)
            return 0

        lax.fori_loop(b0 + 1, BL, wipe, 0)
        kf = kb[a].reshape(-1, 128)
        vf = vb[a].reshape(-1, 128)
        sc = lax.dot_general(q[j], kf, (((1,), (1,)), ((), ())), preferred_element_type=f32) * (128 ** -0.5)
        col = lax.broadcasted_iota(i32, sc.shape, 1)
        head = lax.broadcasted_iota(i32, sc.shape, 0) // 3
        ok = ((col & 7) == head) & ((col >> 3) <= m)
        sc = jnp.where(ok, sc, -1e30)
        top = jnp.max(sc, axis=1, keepdims=True)
        w = jnp.exp(sc - top)
        tot = jnp.sum(w, axis=1, keepdims=True)
        acc = lax.dot_general(w.astype(bf16), vf, (((1,), (0,)), ((), ())), preferred_element_type=f32)
        ob[a] = (acc / tot).astype(bf16)
        for src, dst in writes(a, j):
            pltpu.make_async_copy(src, dst, wsem.at[a]).start()

    def writes(a, j):
        bw = jnp.where(tab[SRC + j] >= 0, 0, tab[MLEN + j] >> SHIFT)
        tail, home = pl.ds(bw, BL - bw), pl.ds(j * BL + bw, BL - bw)
        return (kb.at[a, tail], ko.at[home]), (vb.at[a, tail], vo.at[home]), (ob.at[a], ao.at[j])

    def settle(k):
        a, j = k & (A - 1), sel[k]
        for src, dst in writes(a, j):
            pltpu.make_async_copy(src, dst, wsem.at[a]).wait()

    def pick(j, n):
        hit = (st[DONE + j] == 0) & (tab[RDY + j] <= link_end) & (tab[RDX + j] <= swap_end) & (n < share)
        sel[n] = j
        st[DONE + j] = jnp.where(hit, 1, st[DONE + j])
        return n + jnp.where(hit, 1, 0)

    n = lax.fori_loop(0, SL, pick, jnp.int32(0))

    def early(k, c):
        load(k, sel[k])
        return c

    lax.fori_loop(0, jnp.minimum(n, A - 1), early, 0)

    def step(k, c):
        compute(k & (A - 1), sel[k])
        later = k + A - 1

        @pl.when(later < n)
        def _():
            @pl.when(k >= 1)
            def _():
                settle(k - 1)

            load(later & (A - 1), sel[later])

        return c

    lax.fori_loop(0, n, step, 0)

    def wind_up(k, c):
        settle(k)
        return c

    lax.fori_loop(jnp.maximum(n - A, 0), n, wind_up, 0)


SMEM = pl.BlockSpec(memory_space=pltpu.SMEM)
VMEM = pl.BlockSpec(memory_space=pltpu.VMEM)
ANY = pl.BlockSpec(memory_space=pl.ANY)
BLOCK = (8 * BP, 128)


def sds(shape, dtype=bf16):
    return jax.ShapeDtypeStruct(shape, dtype)


def dma(n):
    return pltpu.SemaphoreType.DMA((n,))


def buf(*lead):
    return pltpu.VMEM(lead + BLOCK, bf16)


def cost(us):
    return pl.CostEstimate(flops=us * FLOPS, bytes_accessed=us * FLOPS, transcendentals=0)


ST = sds((STATE,), i32)
DMA = [pltpu.SemaphoreType.DMA]
TAGS = ('ra', 'rb')


def solution(mesh):
    group = mesh.shape['dp']
    ring = [0, 1, 3, 2]
    cw = [(ring[k] * 2 + c, ring[(k + 1) % 4] * 2 + c) for k in range(4) for c in range(2)]
    ccw = [(b, a) for a, b in cw]
    swap = [(d, d ^ 1) for d in range(group)]

    def local(query, k_cache, v_cache, cache_lens, dest_slot, k_new, v_new):
        kc = k_cache.reshape((SL * BL,) + BLOCK)
        vc = v_cache.reshape((SL * BL,) + BLOCK)
        lens_all = pl.pallas_call(
            lens_kernel, out_shape=sds((8, 1, SL), i32), in_specs=[VMEM], out_specs=VMEM,
            scratch_shapes=[pltpu.SemaphoreType.DMA, dma(8), dma(8)],
            compiler_params=pltpu.CompilerParams(collective_id=0, has_side_effects=True),
            name='lens')(cache_lens.reshape(1, SL))
        me = jnp.full((1,), lax.axis_index('dp'), i32)
        tab, lens_out, state, rounds, pick = pl.pallas_call(
            plan_kernel, out_shape=[sds((n,), i32) for n in (TAB, SL, STATE, 1, 1)], in_specs=[SMEM] * 3, out_specs=[SMEM] * 5,
            scratch_shapes=[pltpu.SMEM((8 * SL + 1,), i32)] * 4 + [pltpu.SMEM((IDLE + 1,), i32)] * 5,
            name='plan')(me, dest_slot, lens_all)

        def run(NB):
            def nothing(*refs):
                pass

            chunk, both, cross = sds((NB,) + BLOCK), sds((2, NB) + BLOCK), sds((2, NX) + BLOCK)
            cache, store = sds((SL * BL,) + BLOCK), sds((4 * SL * BL,) + BLOCK)
            ko, vo, ao, f0, f1, rc0, rc1, po0, po1, dxr = pl.pallas_call(
                nothing, out_shape=(cache, cache, sds((SL, 24, 128)), store, store, chunk, chunk, chunk, chunk, cross),
                out_specs=(ANY,) * 10, name='blank')()

            st = state
            caches = [SMEM, SMEM, ANY, ANY]

            def opened(st):
                return pl.pallas_call(
                    functools.partial(open_kernel, NB), out_shape=(ST, both), in_specs=caches, out_specs=(SMEM, VMEM),
                    scratch_shapes=DMA, name='open')(tab, st, kc, vc)

            st, part = opened(st)
            pre = lax.ppermute(part, 'dp', swap)
            st, part = opened(st)
            pre1 = lax.ppermute(part, 'dp', swap)
            st, s0, s1 = pl.pallas_call(
                functools.partial(open_merge_kernel, NB), out_shape=(ST, chunk, chunk), in_specs=caches + [VMEM],
                out_specs=(SMEM, VMEM, VMEM), scratch_shapes=DMA,
                name='open_merge')(tab, st, kc, vc, pre)
            pre = pre1

            def attend(st, ko, vo, ao, last):
                return pl.pallas_call(
                    functools.partial(attn_kernel, NB, last),
                    out_shape=(ST, cache, cache, sds((SL, 24, 128))),
                    in_specs=[SMEM, SMEM, VMEM, VMEM, VMEM, ANY, ANY, ANY, ANY, ANY], out_specs=(SMEM, ANY, ANY, ANY),
                    input_output_aliases={7: 1, 8: 2, 9: 3},
                    scratch_shapes=[buf(A, BL), buf(A, BL), pltpu.VMEM((A, 24, 128), bf16), pltpu.SMEM((SL + 1,), i32),
                                    dma(A), dma(A)],
                    cost_estimate=cost(6), name='attend')(tab, st, query, k_new, v_new, kc, vc, ko, vo, ao)

            def one_round(tag, c):
                st, s0, s1, pre, rc0, rc1, po0, po1, dxr, f0, f1, ko, vo, ao = c
                nrc0 = lax.ppermute(s0, 'dp', cw)
                nrc1 = lax.ppermute(s1, 'dp', ccw)
                npo0 = lax.ppermute(rc0, 'dp', swap)
                npo1 = lax.ppermute(rc1, 'dp', swap)
                st, s0, s1, part, dxs, f0, f1, ko, vo = pl.pallas_call(
                    functools.partial(round_kernel, NB), out_shape=(ST, chunk, chunk, both, cross, store, store, cache, cache),
                    in_specs=caches + [VMEM] * 6 + [ANY] * 4, out_specs=(SMEM,) + (VMEM,) * 4 + (ANY,) * 4,
                    input_output_aliases={10: 5, 11: 6, 12: 7, 13: 8},
                    scratch_shapes=DMA * 3,
                    cost_estimate=cost(10), name='round')(tab, st, kc, vc, pre, rc0, rc1, po0, po1, dxr, f0, f1, ko, vo)
                npre = lax.ppermute(part, 'dp', swap)
                ndxr = lax.ppermute(dxs, 'dp', swap)
                st, ko, vo, ao = attend(st, ko, vo, ao, False)
                if tag != TAGS[-1]:
                    s0, s1, npo0, npo1 = lax.optimization_barrier((s0, s1, npo0, npo1))
                return st, s0, s1, npre, nrc0, nrc1, npo0, npo1, ndxr, f0, f1, ko, vo, ao

            turns = rounds[0]

            def body(c):
                return (c[0] + TURN,) + functools.reduce(lambda c, tag: one_round(tag, c), TAGS, c[1:])

            c = lax.while_loop(lambda c: c[0] < turns, body,
                           (jnp.int32(0), st, s0, s1, pre, rc0, rc1, po0, po1, dxr, f0, f1, ko, vo, ao))
            _, st, _, _, _, rc0, rc1, po0, po1, dxr, _, _, ko, vo, ao = c

            def close(last, st, ko, vo, *ins):
                n = len(ins)
                return pl.pallas_call(
                    functools.partial(close_kernel, NB, last), out_shape=(ST, cache, cache),
                    in_specs=[SMEM, SMEM] + [VMEM] * n + [ANY] * 2, out_specs=(SMEM, ANY, ANY),
                    input_output_aliases={n + 2: 1, n + 3: 2},
                    scratch_shapes=DMA,
                    name='close_last' if last else 'close')(tab, st, *ins, ko, vo)

            lpo0 = lax.ppermute(rc0, 'dp', swap)
            lpo1 = lax.ppermute(rc1, 'dp', swap)
            st, ko, vo = close(False, st, ko, vo, rc0, rc1, po0, po1, dxr)
            st, ko, vo = close(True, st, ko, vo, lpo0, lpo1)
            st, ko, vo, ao = attend(st, ko, vo, ao, True)
            return ao, ko, vo

        ao, ko, vo = lax.switch(pick[0], [functools.partial(run, size) for size in SIZES])
        return ao, ko.reshape(k_cache.shape), vo.reshape(v_cache.shape), lens_out

    row_spec = P('dp')
    return jax.shard_map(local, mesh=mesh, in_specs=(row_spec, row_spec, row_spec, row_spec, P(), row_spec, row_spec),
                         out_specs=(row_spec, row_spec, row_spec, row_spec), check_vma=False)
```
